32 devices in a mesh: data: 32 (over z, y, x, core).
Axes of the slice: x: 2, y: 2, z: 4, core: 2. Of those that a mesh axis runs over, the one named last changes fastest.
Arguments:
- grad_qkv: bfloat16 [32, 1, 3551232], P('data')
- weight_qkv: float32 [1, 3551232], P(None, 'data')
- mom_qkv: float32 [1, 3551232], P(None, 'data')
- var_qkv: float32 [1, 3551232], P(None, 'data')
- grad_proj: bfloat16 [32, 1, 1183744], P('data')
- weight_proj: float32 [1, 1183744], P(None, 'data')
- mom_proj: float32 [1, 1183744], P(None, 'data')
- var_proj: float32 [1, 1183744], P(None, 'data')
- grad_fc_in: bfloat16 [32, 1, 4734976], P('data')
- weight_fc_in: float32 [1, 4734976], P(None, 'data')
- mom_fc_in: float32 [1, 4734976], P(None, 'data')
- var_fc_in: float32 [1, 4734976], P(None, 'data')
- grad_fc_out: bfloat16 [32, 1, 4734976], P('data')
- weight_fc_out: float32 [1, 4734976], P(None, 'data')
- mom_fc_out: float32 [1, 4734976], P(None, 'data')
- var_fc_out: float32 [1, 4734976], P(None, 'data')
Outputs:
- output 1: bfloat16 [1, 3551232], replicated
- output 2: float32 [1, 3551232], P(None, 'data')
- output 3: float32 [1, 3551232], P(None, 'data')
- output 4: float32 [1, 3551232], P(None, 'data')
- output 5: bfloat16 [1, 1183744], replicated
- output 6: float32 [1, 1183744], P(None, 'data')
- output 7: float32 [1, 1183744], P(None, 'data')
- output 8: float32 [1, 1183744], P(None, 'data')
- output 9: bfloat16 [1, 4734976], replicated
- output 10: float32 [1, 4734976], P(None, 'data')
- output 11: float32 [1, 4734976], P(None, 'data')
- output 12: float32 [1, 4734976], P(None, 'data')
- output 13: bfloat16 [1, 4734976], replicated
- output 14: float32 [1, 4734976], P(None, 'data')
- output 15: float32 [1, 4734976], P(None, 'data')
- output 16: float32 [1, 4734976], P(None, 'data')
All inputs are finite; a program needn't handle non-finite values.
Results may differ from the reference program's by a relative error of at most 0.001.
Values are sent between devices in bfloat16 or wider.
A program may use at most 1 GiB of HBM per device.

```python
import jax
import jax.numpy as jnp

D = 1088
FF = 4352
LAYERS = 1
DATA = 32
STEP = 10

LEARN_RATE = 0.1
BETA_ONE = 0.9
BETA_TWO = 0.999
EPSILON = 1e-6
WEIGHT_DECAY = 0.01
TENSOR_SHAPES = ((D, 3 * D), (D, D), (D, FF), (FF, D))
KIND_NAMES = ("qkv", "proj", "fc_in", "fc_out")


def draw_tensor(rng_key, fan_in, fan_out):
    size_flat = fan_in * fan_out
    sub_keys = jax.random.split(rng_key, 8)
    position = jnp.arange(size_flat, dtype=jnp.float32) / size_flat - 0.5
    sign_flip = 2.0 * jax.random.randint(sub_keys[0], (LAYERS, 1), 0, 2).astype(jnp.float32) - 1.0
    ramp_slope = sign_flip * jax.random.uniform(sub_keys[1], (LAYERS, 1), minval=1.0, maxval=2.0)
    weight_scale = fan_in ** -0.5 * jnp.exp(jax.random.uniform(sub_keys[2], (LAYERS, 1), minval=-1.0, maxval=1.0))
    grad_scale = 10.0 * jnp.exp(jax.random.uniform(sub_keys[3], (LAYERS, 1), minval=-1.0, maxval=1.0))
    weight = weight_scale * jnp.exp(ramp_slope * position) * jax.random.normal(sub_keys[4], (LAYERS, size_flat))
    local_grad = grad_scale * DATA ** 0.5 * jax.random.normal(sub_keys[5], (DATA, LAYERS, size_flat))
    first_mom = 0.05 * grad_scale * jax.random.normal(sub_keys[6], (LAYERS, size_flat))
    second_mom = 0.0005 * grad_scale * grad_scale * jax.random.uniform(sub_keys[7], (LAYERS, size_flat), minval=0.5, maxval=1.5)
    return local_grad.astype(jnp.bfloat16), weight, first_mom, second_mom


def setup_inputs(seed: int = 0) -> dict:
    root_key = jax.random.key(seed)
    arrays = {}
    for kind_pos in range(4):
        fan_in, fan_out = TENSOR_SHAPES[kind_pos]
        drawn_set = draw_tensor(jax.random.fold_in(root_key, kind_pos), fan_in, fan_out)
        arrays["grad_" + KIND_NAMES[kind_pos]] = drawn_set[0]
        arrays["weight_" + KIND_NAMES[kind_pos]] = drawn_set[1]
        arrays["mom_" + KIND_NAMES[kind_pos]] = drawn_set[2]
        arrays["var_" + KIND_NAMES[kind_pos]] = drawn_set[3]
    return arrays


def lamb_tensor(local_grad, weight, first_mom, second_mom):
    grad_mean = jnp.sum(local_grad, axis=0, dtype=jnp.float32) / local_grad.shape[0]
    new_first = BETA_ONE * first_mom + (1.0 - BETA_ONE) * grad_mean
    new_second = BETA_TWO * second_mom + (1.0 - BETA_TWO) * grad_mean * grad_mean
    direction = (new_first / (1.0 - BETA_ONE ** STEP)) / (jnp.sqrt(new_second / (1.0 - BETA_TWO ** STEP)) + EPSILON) + WEIGHT_DECAY * weight
    weight_norm = jnp.sqrt(jnp.sum(weight * weight, axis=1, keepdims=True))
    update_norm = jnp.sqrt(jnp.sum(direction * direction, axis=1, keepdims=True))
    new_weight = weight - LEARN_RATE * (weight_norm / update_norm) * direction
    return new_weight.astype(jnp.bfloat16), new_weight, new_first, new_second


def reference(grad_qkv, weight_qkv, mom_qkv, var_qkv, grad_proj, weight_proj, mom_proj, var_proj, grad_fc_in, weight_fc_in, mom_fc_in, var_fc_in, grad_fc_out, weight_fc_out, mom_fc_out, var_fc_out):
    copy_qkv, new_weight_qkv, new_mom_qkv, new_var_qkv = lamb_tensor(grad_qkv, weight_qkv, mom_qkv, var_qkv)
    copy_proj, new_weight_proj, new_mom_proj, new_var_proj = lamb_tensor(grad_proj, weight_proj, mom_proj, var_proj)
    copy_fc_in, new_weight_fc_in, new_mom_fc_in, new_var_fc_in = lamb_tensor(grad_fc_in, weight_fc_in, mom_fc_in, var_fc_in)
    copy_fc_out, new_weight_fc_out, new_mom_fc_out, new_var_fc_out = lamb_tensor(grad_fc_out, weight_fc_out, mom_fc_out, var_fc_out)
    return (copy_qkv, new_weight_qkv, new_mom_qkv, new_var_qkv, copy_proj, new_weight_proj, new_mom_proj, new_var_proj, copy_fc_in, new_weight_fc_in, new_mom_fc_in, new_var_fc_in, copy_fc_out, new_weight_fc_out, new_mom_fc_out, new_var_fc_out)
```

```python
import functools

import jax
import jax.numpy as jnp
from jax import lax
from jax.experimental import pallas as pl
from jax.experimental.pallas import tpu as pltpu
from jax.sharding import PartitionSpec as P

STEP = 10
LEARN_RATE = 0.1
BETA_ONE = 0.9
BETA_TWO = 0.999
EPSILON = 1e-6
WEIGHT_DECAY = 0.01

LANES = 128
ROWS = (867, 289, 1156, 1156)
PADDED = (880, 304, 1168, 1168)
STARTS = (0, 880, 1184, 2352)
TOTAL = 3520
UNITS = (
    (0, 0, 448, 0), (0, 448, 432, 1),
    (1, 0, 144, 0), (1, 144, 160, 1),
    (2, 0, 592, 0), (2, 592, 576, 1),
    (3, 0, 576, 0), (3, 576, 592, 1),
)
MAX_ROWS = 592
TILE = 48
MESH = pl.DeviceIdType.MESH
F32 = jnp.float32
BF16 = jnp.bfloat16


def pack_kernel(g0, g1, g2, g3, out):
    for t, ref in enumerate((g0, g1, g2, g3)):
        pad = jnp.zeros((PADDED[t] - ROWS[t], LANES), BF16)
        out[0, pl.ds(STARTS[t], PADDED[t]), :] = jnp.concatenate([ref[...].reshape(ROWS[t], LANES), pad], axis=0)


def pack(grads):
    specs = [pl.BlockSpec((1, r * LANES), lambda i: (0, i)) for r in ROWS]
    return pl.pallas_call(
        pack_kernel,
        grid=(32,),
        in_specs=specs,
        out_specs=pl.BlockSpec((1, TOTAL, LANES), lambda i: (i, 0, 0)),
        out_shape=jax.ShapeDtypeStruct((32, TOTAL, LANES), BF16),
        name="pack",
    )(*grads)


def unpack_kernel(full, w, m, v, c0, c1, c2, c3, *outs):
    for t, ref in enumerate((c0, c1, c2, c3)):
        ref[...] = full[0, pl.ds(STARTS[t], ROWS[t]), :].reshape(1, ROWS[t] * LANES)

    @pl.when(pl.program_id(0) == 0)
    def _():
        for s, src in enumerate((w, m, v)):
            for t in range(4):
                outs[4 * s + t][...] = src[pl.ds(STARTS[t], ROWS[t]), :].reshape(1, ROWS[t] * LANES)


def unpack(full, w, m, v):
    state = pl.BlockSpec((TOTAL, LANES), lambda i: (0, 0))
    return pl.pallas_call(
        unpack_kernel,
        grid=(32,),
        in_specs=[pl.BlockSpec((1, TOTAL, LANES), lambda i: (i, 0, 0)), state, state, state],
        out_specs=[pl.BlockSpec((1, r * LANES), lambda i: (0, i)) for r in ROWS]
        + [pl.BlockSpec((1, r * LANES), lambda i: (0, 0)) for r in ROWS] * 3,
        out_shape=[jax.ShapeDtypeStruct((1, 32 * r * LANES), BF16) for r in ROWS]
        + [jax.ShapeDtypeStruct((1, r * LANES), F32) for r in ROWS] * 3,
        name="unpack",
    )(full, w, m, v)


def comm_kernel(*refs):
    grads = refs[0]
    state_in = refs[1:13]
    full, new_w, new_m, new_v = refs[13:17]
    state = refs[17:29]
    (rx, r2, r3, rz, t2, lx, ns, nr, state_sem, lx_sem, p_send, p_recv, c_send, c_recv, q_send, q_recv,
     z_send, z_recv, n_send, n_recv, out_sem, own_sem, gz_send, gz_recv, gq_send, gq_recv, gp_send, gp_recv,
     gc_send, gc_recv) = refs[29:]

    me = lax.axis_index("data")
    c = me % 2
    x = (me // 2) % 2
    y = (me // 4) % 2
    z = me // 8

    def dev(zz, yy, xx, cc):
        return (((zz * 2 + yy) * 2 + xx) * 2 + cc,)

    core_peer = dev(z, y, x, 1 - c)
    x_peer = dev(z, y, 1 - x, c)
    y_peer = dev(z, 1 - y, x, c)
    z_peer = [dev((z + k) % 4, y, x, c) for k in (1, 2, 3)]

    barrier = pltpu.get_barrier_semaphore()
    for peer in [core_peer, x_peer, y_peer] + z_peer:
        pl.semaphore_signal(barrier, inc=1, device_id=peer, device_id_type=MESH)
    pl.semaphore_wait(barrier, 6)

    def remote(src, dst, ssem, rsem, peer):
        return pltpu.make_async_remote_copy(src_ref=src, dst_ref=dst, send_sem=ssem, recv_sem=rsem, device_id=peer, device_id_type=MESH)

    def rows_of(u):
        t, first, h, colour = UNITS[u]
        return pl.ds(STARTS[t] + first, h)

    def grad_slab(u, mine):
        rows = rows_of(u)
        if UNITS[u][3] == 0:
            return grads.at[:, :, x if mine else 1 - x, :, rows, :]
        return grads.at[:, y if mine else 1 - y, :, :, rows, :]

    def p_peer(u):
        return x_peer if UNITS[u][3] == 0 else y_peer

    def q_peer(u):
        return y_peer if UNITS[u][3] == 0 else x_peer

    def q_me(u):
        return y if UNITS[u][3] == 0 else x

    n_units = len(UNITS)
    p_copy = [remote(grad_slab(u, False), rx.at[:, :, :, rows_of(u), :], p_send.at[u], p_recv.at[u], p_peer(u)) for u in range(n_units)]
    lx_copy = [pltpu.make_async_copy(grad_slab(u, True), lx.at[u % 2, :, :, :, pl.ds(0, UNITS[u][2]), :], lx_sem.at[u % 2]) for u in range(n_units)]
    c_copy = [remote(t2.at[u % 2, :, :, pl.ds(0, UNITS[u][2]), :], r2.at[:, :, rows_of(u), :], c_send.at[u], c_recv.at[u], core_peer) for u in range(n_units)]
    q_copy = [remote(r2.at[:, 1 - q_me(u), rows_of(u), :], r3.at[:, rows_of(u), :], q_send.at[u], q_recv.at[u], q_peer(u)) for u in range(n_units)]
    z_copy = [[remote(r3.at[(z + k) % 4, rows_of(u), :], rz.at[k - 1, rows_of(u), :], z_send.at[u, k - 1], z_recv.at[u, k - 1], z_peer[k - 1]) for k in (1, 2, 3)] for u in range(n_units)]

    for u in range(n_units):
        p_copy[u].start()
    state_copy = [pltpu.make_async_copy(state_in[i], state[i], state_sem.at[i]) for i in range(12)]
    for cp in state_copy:
        cp.start()
    lx_copy[0].start()
    lx_copy[1].start()
    ns[...] = jnp.zeros_like(ns)

    def base(u):
        return STARTS[UNITS[u][0]] + UNITS[u][1]

    def core_step(u):
        lx_copy[u].wait()
        p_copy[u].wait_recv()
        if u >= 2:
            c_copy[u - 2].wait_send()

        def body(i, carry):
            r = pl.multiple_of(i * 16, 16)
            a = lx[u % 2, :, :, 1 - c, pl.ds(r, 16), :].astype(F32)
            b = rx[:, :, 1 - c, pl.ds(base(u) + r, 16), :].astype(F32)
            t2[u % 2, :, :, pl.ds(r, 16), :] = a + b
            return carry

        lax.fori_loop(0, UNITS[u][2] // 16, body, 0)
        c_copy[u].start()

    def q_step(u):
        c_copy[u].wait_recv()

        def body(i, carry):
            r = pl.multiple_of(i * 16, 16)
            a = lx[u % 2, :, :, c, pl.ds(r, 16), :].astype(F32)
            b = rx[:, :, c, pl.ds(base(u) + r, 16), :].astype(F32)
            r2[:, :, pl.ds(base(u) + r, 16), :] = r2[:, :, pl.ds(base(u) + r, 16), :] + (a + b)
            return carry

        lax.fori_loop(0, UNITS[u][2] // 16, body, 0)
        q_copy[u].start()
        if u + 2 < n_units:
            lx_copy[u + 2].start()

    def z_step(u):
        q_copy[u].wait_recv()

        def body(i, carry):
            r = pl.multiple_of(base(u) + i * 16, 16)
            r3[:, pl.ds(r, 16), :] = r3[:, pl.ds(r, 16), :] + r2[:, q_me(u), pl.ds(r, 16), :]
            return carry

        lax.fori_loop(0, UNITS[u][2] // 16, body, 0)
        for cp in z_copy[u]:
            cp.start()

    def lamb_step(u):
        t, first, h, colour = UNITS[u]
        for cp in z_copy[u]:
            cp.wait_recv()
        if u % 2 == 0:
            for i in (t, 4 + t, 8 + t):
                state_copy[i].wait()
        valid = min(h, ROWS[t] - first)
        q = q_me(u)

        def tile(r, n):
            rows = pl.ds(base(u) + r, n)
            flat = pl.ds((first + r) * LANES if isinstance(r, int) else pl.multiple_of((first + r) * LANES, LANES), n * LANES)
            w = state[t][:, flat].reshape(n, LANES)
            m = state[4 + t][:, flat].reshape(n, LANES)
            v = state[8 + t][:, flat].reshape(n, LANES)
            g = (((r3[z, rows, :] + rz[0, rows, :]) + rz[1, rows, :]) + rz[2, rows, :]) / 32.0
            nm = BETA_ONE * m + (1.0 - BETA_ONE) * g
            nv = BETA_TWO * v + (1.0 - BETA_TWO) * g * g
            u_dir = (nm / (1.0 - BETA_ONE ** STEP)) / (jnp.sqrt(nv / (1.0 - BETA_TWO ** STEP)) + EPSILON) + WEIGHT_DECAY * w
            r2[0, q, rows, :] = nm
            r2[1, q, rows, :] = nv
            rz[0, rows, :] = u_dir
            return w * w, u_dir * u_dir

        def body(i, carry):
            ww, uu = tile(pl.multiple_of(i * TILE, 16), TILE)
            return (carry[0] + jnp.sum(ww.reshape(TILE // 8, 8, LANES), axis=0), carry[1] + jnp.sum(uu.reshape(TILE // 8, 8, LANES), axis=0))

        zero = jnp.zeros((8, LANES), F32)
        acc_w, acc_u = lax.fori_loop(0, valid // TILE, body, (zero, zero))
        sum_w = jnp.sum(acc_w, axis=0, keepdims=True)
        sum_u = jnp.sum(acc_u, axis=0, keepdims=True)
        if valid % TILE:
            ww, uu = tile(valid - valid % TILE, valid % TILE)
            sum_w = sum_w + jnp.sum(ww, axis=0, keepdims=True)
            sum_u = sum_u + jnp.sum(uu, axis=0, keepdims=True)
        ns[pl.ds(2 * t, 1), :] = ns[pl.ds(2 * t, 1), :] + sum_w
        ns[pl.ds(2 * t + 1, 1), :] = ns[pl.ds(2 * t + 1, 1), :] + sum_u
        out_m[u].start()
        out_v[u].start()

    out_m = [pltpu.make_async_copy(r2.at[0, q_me(u), rows_of(u), :], new_m.at[rows_of(u), :], out_sem.at[0, u]) for u in range(n_units)]
    out_v = [pltpu.make_async_copy(r2.at[1, q_me(u), rows_of(u), :], new_v.at[rows_of(u), :], out_sem.at[1, u]) for u in range(n_units)]
    out_w = [pltpu.make_async_copy(rz.at[1, rows_of(u), :], new_w.at[rows_of(u), :], out_sem.at[2, u]) for u in range(n_units)]
    own_copy = [pltpu.make_async_copy(rx.at[0, 0, 0, rows_of(u), :], full.at[z, y, x, c, rows_of(u), :], own_sem.at[u]) for u in range(n_units)]

    for s in range(n_units + 3):
        if s < n_units:
            core_step(s)
        if 0 <= s - 1 < n_units:
            q_step(s - 1)
        if 0 <= s - 2 < n_units:
            z_step(s - 2)
        if 0 <= s - 3 < n_units:
            lamb_step(s - 3)

    for i, peer in enumerate((core_peer, x_peer, y_peer)):
        cp = remote(ns, nr.at[i], n_send.at[i], n_recv.at[i], peer)
        cp.start()
        cp.wait()
        ns[...] = ns[...] + nr[i]
    z_norm = [remote(ns, nr.at[3 + z], n_send.at[2 + k], n_recv.at[2 + k], z_peer[k - 1]) for k in (1, 2, 3)]
    for cp in z_norm:
        cp.start()
    nr[3 + z] = ns[...]
    for k in (1, 2, 3):
        remote(ns, nr.at[3 + (z + 4 - k) % 4], n_send.at[2 + k], n_recv.at[2 + k], z_peer[k - 1]).wait_recv()
    for cp in z_norm:
        cp.wait_send()
    total = (nr[3] + nr[4]) + (nr[5] + nr[6])
    norms = jnp.sqrt(jnp.sum(total, axis=1, keepdims=True))

    def weight_step(u):
        t, first, h, colour = UNITS[u]
        valid = min(h, ROWS[t] - first)
        scale = LEARN_RATE * (norms[2 * t:2 * t + 1] / norms[2 * t + 1:2 * t + 2])

        def tile(r, n):
            rows = pl.ds(base(u) + r, n)
            flat = pl.ds((first + r) * LANES if isinstance(r, int) else pl.multiple_of((first + r) * LANES, LANES), n * LANES)
            w = state[t][:, flat].reshape(n, LANES)
            nw = w - scale * rz[0, rows, :]
            rz[1, rows, :] = nw
            rx[0, 0, 0, rows, :] = nw.astype(BF16)

        def body(i, carry):
            tile(pl.multiple_of(i * TILE, 16), TILE)
            return carry

        lax.fori_loop(0, valid // TILE, body, 0)
        if valid % TILE:
            tile(valid - valid % TILE, valid % TILE)
        own_copy[u].start()
        out_w[u].start()

    def slab(u, zz, yy, xx, cc):
        return full.at[zz, yy, xx, cc, rows_of(u), :]

    def gathered_q(u):
        return full.at[:, y, x, c, rows_of(u), :]

    def gathered_p(u):
        if UNITS[u][3] == 0:
            return full.at[:, :, x, c, rows_of(u), :]
        return full.at[:, y, :, c, rows_of(u), :]

    def gathered_c(u):
        return full.at[:, :, :, c, rows_of(u), :]

    gz = [[remote(slab(u, z, y, x, c), slab(u, z, y, x, c), gz_send.at[u, k - 1], gz_recv.at[u, k - 1], z_peer[k - 1]) for k in (1, 2, 3)] for u in range(n_units)]
    gq = [remote(gathered_q(u), gathered_q(u), gq_send.at[u], gq_recv.at[u], q_peer(u)) for u in range(n_units)]
    gp = [remote(gathered_p(u), gathered_p(u), gp_send.at[u], gp_recv.at[u], p_peer(u)) for u in range(n_units)]
    gc = [remote(gathered_c(u), gathered_c(u), gc_send.at[u], gc_recv.at[u], core_peer) for u in range(n_units)]

    for s in range(n_units + 4):
        if s < n_units:
            weight_step(s)
            own_copy[s].wait()
            for cp in gz[s]:
                cp.start()
        if 0 <= s - 1 < n_units:
            for cp in gz[s - 1]:
                cp.wait_recv()
            gq[s - 1].start()
        if 0 <= s - 2 < n_units:
            gq[s - 2].wait_recv()
            gp[s - 2].start()
        if 0 <= s - 3 < n_units:
            gp[s - 3].wait_recv()
            gc[s - 3].start()
        if 0 <= s - 4 < n_units:
            gc[s - 4].wait_recv()

    for u in range(n_units):
        p_copy[u].wait_send()
        if u >= n_units - 2:
            c_copy[u].wait_send()
        q_copy[u].wait_send()
        for cp in z_copy[u] + gz[u]:
            cp.wait_send()
        gq[u].wait_send()
        gp[u].wait_send()
        gc[u].wait_send()
        out_m[u].wait()
        out_v[u].wait()
        out_w[u].wait()


def comm(grads, state):
    n_units = len(UNITS)
    any_spec = pl.BlockSpec(memory_space=pl.ANY)
    dma = pltpu.SemaphoreType.DMA
    return pl.pallas_call(
        comm_kernel,
        in_specs=[any_spec] * 13,
        out_specs=[any_spec] * 4,
        out_shape=[jax.ShapeDtypeStruct((4, 2, 2, 2, TOTAL, LANES), BF16)] + [jax.ShapeDtypeStruct((TOTAL, LANES), F32)] * 3,
        scratch_shapes=[pltpu.VMEM((1, r * LANES), F32) for r in ROWS] * 3
        + [
            pltpu.VMEM((4, 2, 2, TOTAL, LANES), BF16),
            pltpu.VMEM((4, 2, TOTAL, LANES), F32),
            pltpu.VMEM((4, TOTAL, LANES), F32),
            pltpu.VMEM((3, TOTAL, LANES), F32),
            pltpu.VMEM((2, 4, 2, MAX_ROWS, LANES), F32),
            pltpu.VMEM((2, 4, 2, 2, MAX_ROWS, LANES), BF16),
            pltpu.VMEM((8, LANES), F32),
            pltpu.VMEM((7, 8, LANES), F32),
            dma((12,)), dma((2,)),
            dma((n_units,)), dma((n_units,)), dma((n_units,)), dma((n_units,)), dma((n_units,)), dma((n_units,)),
            dma((n_units, 3)), dma((n_units, 3)), dma((6,)), dma((6,)), dma((3, n_units)), dma((n_units,)),
            dma((n_units, 3)), dma((n_units, 3)), dma((n_units,)), dma((n_units,)), dma((n_units,)), dma((n_units,)),
            dma((n_units,)), dma((n_units,)),
        ],
        compiler_params=pltpu.CompilerParams(collective_id=0, has_side_effects=True, vmem_limit_bytes=64 * 1024 * 1024 - 128 * 1024),
        name="lamb_comm",
    )(grads, *state)


def solution(mesh):
    grad_spec = P("data", None, None)
    shard_spec = P(None, "data")
    full_spec = P(None, None)

    def device_step(*blocks):
        grads = pack([blocks[4 * t].reshape(1, -1) for t in range(4)])
        state = [blocks[4 * t + s] for s in (1, 2, 3) for t in range(4)]
        full, w, m, v = comm(grads.reshape(4, 2, 2, 2, TOTAL, LANES), state)
        outs = unpack(full.reshape(32, TOTAL, LANES), w, m, v)
        results = []
        for t in range(4):
            results.extend((outs[t], outs[4 + t], outs[8 + t], outs[12 + t]))
        return tuple(results)

    return jax.shard_map(device_step, mesh=mesh, in_specs=(grad_spec, shard_spec, shard_spec, shard_spec) * 4, out_specs=(full_spec, shard_spec, shard_spec, shard_spec) * 4, check_vma=False)
```

```python
import functools

import jax
import jax.numpy as jnp
from jax import lax
from jax.experimental import pallas as pl
from jax.experimental.pallas import tpu as pltpu
from jax.sharding import PartitionSpec as P

STEP = 10
LEARN_RATE = 0.1
BETA_ONE = 0.9
BETA_TWO = 0.999
EPSILON = 1e-6
WEIGHT_DECAY = 0.01

LANES = 128
ROWS = (867, 289, 1156, 1156)
PADDED = (880, 304, 1168, 1168)
STARTS = (0, 880, 1184, 2352)
TOTAL = 3520
STEPS = (
    ((2, 0, 304), (2, 304, 288)),
    ((2, 592, 288), (2, 880, 288)),
    ((3, 0, 288), (3, 288, 304)),
    ((3, 592, 288), (3, 880, 288)),
    ((0, 0, 224), (0, 224, 224)),
    ((0, 448, 224), (0, 672, 208)),
    ((1, 0, 80), (1, 80, 80)),
    ((1, 160, 80), (1, 240, 64)),
)
UNITS = tuple(unit + (colour,) for step in STEPS for colour, unit in enumerate(step))
MAX_ROWS = 304
TILE = 48
MESH = pl.DeviceIdType.MESH
F32 = jnp.float32
BF16 = jnp.bfloat16


def unpack_kernel(full, w, m, v, c0, c1, c2, c3, *outs):
    for t, ref in enumerate((c0, c1, c2, c3)):
        ref[...] = full[0, pl.ds(STARTS[t], ROWS[t]), :].astype(F32).reshape(1, ROWS[t] * LANES).astype(BF16)

    @pl.when(pl.program_id(0) == 0)
    def _():
        for s, src in enumerate((w, m, v)):
            for t in range(4):
                outs[4 * s + t][...] = src[pl.ds(STARTS[t], ROWS[t]), :].reshape(1, ROWS[t] * LANES)


def unpack(full, w, m, v):
    state = pl.BlockSpec((TOTAL, LANES), lambda i: (0, 0))
    return pl.pallas_call(
        unpack_kernel,
        grid=(32,),
        in_specs=[pl.BlockSpec((1, TOTAL, LANES), lambda i: (i, 0, 0)), state, state, state],
        out_specs=[pl.BlockSpec((1, r * LANES), lambda i: (0, i)) for r in ROWS]
        + [pl.BlockSpec((1, r * LANES), lambda i: (0, 0)) for r in ROWS] * 3,
        out_shape=[jax.ShapeDtypeStruct((1, 32 * r * LANES), BF16) for r in ROWS]
        + [jax.ShapeDtypeStruct((1, r * LANES), F32) for r in ROWS] * 3,
        name="unpack",
    )(full, w, m, v)


def comm_kernel(*refs):
    grads = refs[0:4]
    state_in = refs[4:16]
    full, new_w, new_m, new_v = refs[16:20]
    state = refs[20:32]
    (rx, r2, r3, rz, t2, lx, ps, stage, ns, nr, state_sem, stage_sem, p_send, p_recv, c_send, c_recv, q_send, q_recv,
     z_send, z_recv, n_send, n_recv, out_sem, own_sem, gz_send, gz_recv, gq_send, gq_recv, gp_send, gp_recv,
     gc_send, gc_recv) = refs[32:]

    me = lax.axis_index("data")
    c = me % 2
    x = (me // 2) % 2
    y = (me // 4) % 2
    z = me // 8

    def dev(zz, yy, xx, cc):
        return (((zz * 2 + yy) * 2 + xx) * 2 + cc,)

    def flip(value, by):
        return 1 - value if by else value

    core_peer = dev(z, y, x, 1 - c)
    x_peer = dev(z, y, 1 - x, c)
    y_peer = dev(z, 1 - y, x, c)
    z_peer = [dev((z + k) % 4, y, x, c) for k in (1, 2, 3)]
    plane_peer = [dev(z, flip(y, k // 4), flip(x, k // 2 % 2), flip(c, k % 2)) for k in range(1, 8)]
    plane_slot = [flip(y, k // 4) * 4 + flip(x, k // 2 % 2) * 2 + flip(c, k % 2) for k in range(8)]

    barrier = pltpu.get_barrier_semaphore()
    for peer in plane_peer + z_peer:
        pl.semaphore_signal(barrier, inc=1, device_id=peer, device_id_type=MESH)

    def remote(src, dst, ssem, rsem, peer):
        return pltpu.make_async_remote_copy(src_ref=src, dst_ref=dst, send_sem=ssem, recv_sem=rsem, device_id=peer, device_id_type=MESH)

    n_units = len(UNITS)
    n_steps = len(STEPS)
    units = range(n_units)

    def base(u):
        return STARTS[UNITS[u][0]] + UNITS[u][1]

    def rows_of(u):
        return pl.ds(base(u), UNITS[u][2])

    def valid_of(u):
        return min(UNITS[u][2], ROWS[UNITS[u][0]] - UNITS[u][1])

    def p_peer(u):
        return x_peer if UNITS[u][3] == 0 else y_peer

    def q_peer(u):
        return y_peer if UNITS[u][3] == 0 else x_peer

    def q_me(u):
        return y if UNITS[u][3] == 0 else x

    def stage_copy(u, mine):
        t, first, h, colour = UNITS[u]
        lanes = pl.ds(first * LANES, valid_of(u) * LANES)
        if colour == 0:
            src = grads[t].at[:, :, x if mine else 1 - x, :, :, lanes]
        else:
            src = grads[t].at[:, y if mine else 1 - y, :, :, :, lanes]
        return pltpu.make_async_copy(src, stage.at[colour, :, :, :, :, pl.ds(0, valid_of(u) * LANES)], stage_sem.at[colour])

    def pack(u, store):
        h, colour = UNITS[u][2:]
        valid = valid_of(u)

        def body(j, carry):
            for cc in (0, 1):
                dense = stage[colour, j // 2, j % 2, cc, :, pl.ds(0, valid * LANES)].reshape(valid, LANES)
                if valid < h:
                    dense = jnp.concatenate([dense, jnp.zeros((h - valid, LANES), BF16)], axis=0)
                store(j // 2, j % 2, cc, dense)
            return carry

        lax.fori_loop(0, 8, body, 0)

    def pack_send(u):
        h, colour = UNITS[u][2:]

        def store(zz, qq, cc, dense):
            ps[colour, (u // 2) % 2, zz, qq, cc, pl.ds(0, h), :] = dense

        pack(u, store)

    def pack_own(u):
        h, colour = UNITS[u][2:]

        def store(zz, qq, cc, dense):
            lx[colour, zz, qq, cc, pl.ds(0, h), :] = dense

        pack(u, store)

    p_copy = [remote(ps.at[u % 2, (u // 2) % 2, :, :, :, pl.ds(0, UNITS[u][2]), :], rx.at[:, :, :, rows_of(u), :], p_send.at[u], p_recv.at[u], p_peer(u)) for u in units]
    c_copy = [remote(t2.at[u % 2, :, :, pl.ds(0, UNITS[u][2]), :], r2.at[:, :, rows_of(u), :], c_send.at[u], c_recv.at[u], core_peer) for u in units]
    q_copy = [remote(r2.at[:, 1 - q_me(u), rows_of(u), :], r3.at[:, rows_of(u), :], q_send.at[u], q_recv.at[u], q_peer(u)) for u in units]
    z_copy = [[remote(r3.at[(z + k) % 4, rows_of(u), :], rz.at[k - 1, rows_of(u), :], z_send.at[u, k - 1], z_recv.at[u, k - 1], z_peer[k - 1]) for k in (1, 2, 3)] for u in units]
    out_m = [pltpu.make_async_copy(r2.at[0, q_me(u), rows_of(u), :], new_m.at[rows_of(u), :], out_sem.at[0, u]) for u in units]
    out_v = [pltpu.make_async_copy(r2.at[1, q_me(u), rows_of(u), :], new_v.at[rows_of(u), :], out_sem.at[1, u]) for u in units]
    out_w = [pltpu.make_async_copy(rz.at[1, rows_of(u), :], new_w.at[rows_of(u), :], out_sem.at[2, u]) for u in units]
    own_copy = [pltpu.make_async_copy(rx.at[0, 0, 0, rows_of(u), :], full.at[z, y, x, c, rows_of(u), :], own_sem.at[u]) for u in units]
    state_copy = [pltpu.make_async_copy(state_in[i], state[i], state_sem.at[i]) for i in range(12)]

    def core_step(u):
        with jax.named_scope(f"wait_p#u={u}"):
            p_copy[u].wait_recv()
        if u >= 2:
            c_copy[u - 2].wait_send()

        def body(i, carry):
            r = pl.multiple_of(i * 16, 16)
            a = lx[u % 2, :, :, 1 - c, pl.ds(r, 16), :].astype(F32)
            b = rx[:, :, 1 - c, pl.ds(base(u) + r, 16), :].astype(F32)
            t2[u % 2, :, :, pl.ds(r, 16), :] = a + b
            return carry

        lax.fori_loop(0, UNITS[u][2] // 16, body, 0)
        c_copy[u].start()

    def q_step(u):
        with jax.named_scope(f"wait_c#u={u}"):
            c_copy[u].wait_recv()

        def body(i, carry):
            r = pl.multiple_of(i * 16, 16)
            a = lx[u % 2, :, :, c, pl.ds(r, 16), :].astype(F32)
            b = rx[:, :, c, pl.ds(base(u) + r, 16), :].astype(F32)
            r2[:, :, pl.ds(base(u) + r, 16), :] = r2[:, :, pl.ds(base(u) + r, 16), :] + (a + b)
            return carry

        lax.fori_loop(0, UNITS[u][2] // 16, body, 0)
        q_copy[u].start()

    def z_step(u):
        with jax.named_scope(f"wait_q#u={u}"):
            q_copy[u].wait_recv()

        def body(i, carry):
            r = pl.multiple_of(base(u) + i * 16, 16)
            r3[:, pl.ds(r, 16), :] = r3[:, pl.ds(r, 16), :] + r2[:, q_me(u), pl.ds(r, 16), :]
            return carry

        lax.fori_loop(0, UNITS[u][2] // 16, body, 0)
        for cp in z_copy[u]:
            cp.start()

    def flat_rows(u, r, n):
        start = (UNITS[u][1] + r) * LANES
        return pl.ds(start if isinstance(r, int) else pl.multiple_of(start, LANES), n * LANES)

    def lamb_step(u):
        t, first, h, colour = UNITS[u]
        with jax.named_scope(f"wait_z#u={u}"):
            for cp in z_copy[u]:
                cp.wait_recv()
        if first == 0:
            for i in (t, 4 + t, 8 + t):
                state_copy[i].wait()
        valid = valid_of(u)
        q = q_me(u)

        def tile(r, n):
            rows = pl.ds(base(u) + r, n)
            flat = flat_rows(u, r, n)
            w = state[t][:, flat].reshape(n, LANES)
            m = state[4 + t][:, flat].reshape(n, LANES)
            v = state[8 + t][:, flat].reshape(n, LANES)
            g = (((r3[z, rows, :] + rz[0, rows, :]) + rz[1, rows, :]) + rz[2, rows, :]) / 32.0
            nm = BETA_ONE * m + (1.0 - BETA_ONE) * g
            nv = BETA_TWO * v + (1.0 - BETA_TWO) * g * g
            u_dir = (nm / (1.0 - BETA_ONE ** STEP)) / (jnp.sqrt(nv / (1.0 - BETA_TWO ** STEP)) + EPSILON) + WEIGHT_DECAY * w
            r2[0, q, rows, :] = nm
            r2[1, q, rows, :] = nv
            rz[0, rows, :] = u_dir
            return w * w, u_dir * u_dir

        def body(i, carry):
            ww, uu = tile(pl.multiple_of(i * TILE, 16), TILE)
            return (carry[0] + jnp.sum(ww.reshape(TILE // 8, 8, LANES), axis=0), carry[1] + jnp.sum(uu.reshape(TILE // 8, 8, LANES), axis=0))

        zero = jnp.zeros((8, LANES), F32)
        acc_w, acc_u = lax.fori_loop(0, valid // TILE, body, (zero, zero))
        sum_w = jnp.sum(acc_w, axis=0, keepdims=True)
        sum_u = jnp.sum(acc_u, axis=0, keepdims=True)
        if valid % TILE:
            ww, uu = tile(valid - valid % TILE, valid % TILE)
            sum_w = sum_w + jnp.sum(ww, axis=0, keepdims=True)
            sum_u = sum_u + jnp.sum(uu, axis=0, keepdims=True)
        ns[pl.ds(2 * t, 1), :] = ns[pl.ds(2 * t, 1), :] + sum_w
        ns[pl.ds(2 * t + 1, 1), :] = ns[pl.ds(2 * t + 1, 1), :] + sum_u
        out_m[u].start()
        out_v[u].start()

    def pair(s):
        return (2 * s, 2 * s + 1)

    for s in (0, 1):
        for u in pair(s):
            stage_copy(u, False).start()
        if s == 0:
            for cp in state_copy:
                cp.start()
            ns[...] = jnp.zeros_like(ns)
        for u in pair(s):
            stage_copy(u, False).wait()
            pack_send(u)
        if s == 0:
            pl.semaphore_wait(barrier, 10)
        for u in pair(s):
            p_copy[u].start()
    for u in pair(0):
        stage_copy(u, True).start()
    for u in pair(0):
        stage_copy(u, True).wait()
        pack_own(u)
        stage_copy(u + 4, False).start()

    for s in range(n_steps + 2):
        if s < n_steps:
            for u in pair(s):
                core_step(u)
            for u in pair(s):
                q_step(u)
            if s + 2 < n_steps:
                for u in pair(s + 2):
                    stage_copy(u, False).wait()
                    p_copy[u - 4].wait_send()
                    pack_send(u)
                    p_copy[u].start()
            if s + 1 < n_steps:
                for u in pair(s + 1):
                    stage_copy(u, True).start()
                for u in pair(s + 1):
                    stage_copy(u, True).wait()
                    pack_own(u)
                    if s + 3 < n_steps:
                        stage_copy(u + 4, False).start()
        if 0 <= s - 1 < n_steps:
            for u in pair(s - 1):
                z_step(u)
        if 0 <= s - 2 < n_steps:
            for u in pair(s - 2):
                lamb_step(u)

    with jax.named_scope("norms"):
        plane_norm = [remote(ns, nr.at[plane_slot[0]], n_send.at[k], n_recv.at[plane_slot[0]], plane_peer[k - 1]) for k in range(1, 8)]
        for cp in plane_norm:
            cp.start()
        nr[plane_slot[0]] = ns[...]
        for k in range(1, 8):
            remote(ns, nr.at[plane_slot[k]], n_send.at[k], n_recv.at[plane_slot[k]], plane_peer[k - 1]).wait_recv()
        for cp in plane_norm:
            cp.wait_send()
        ns[...] = ((nr[0] + nr[1]) + (nr[2] + nr[3])) + ((nr[4] + nr[5]) + (nr[6] + nr[7]))
        z_norm = [remote(ns, nr.at[8 + z], n_send.at[7 + k], n_recv.at[8 + z], z_peer[k - 1]) for k in (1, 2, 3)]
        for cp in z_norm:
            cp.start()
        nr[8 + z] = ns[...]
        for k in (1, 2, 3):
            zz = (z + k) % 4
            remote(ns, nr.at[8 + zz], n_send.at[7 + k], n_recv.at[8 + zz], z_peer[k - 1]).wait_recv()
        for cp in z_norm:
            cp.wait_send()
    total = (nr[8] + nr[9]) + (nr[10] + nr[11])
    norms = jnp.sqrt(jnp.sum(total, axis=1, keepdims=True))

    def gathered_q(u):
        return full.at[:, y, x, c, rows_of(u), :]

    def gathered_p(u):
        if UNITS[u][3] == 0:
            return full.at[:, :, x, c, rows_of(u), :]
        return full.at[:, y, :, c, rows_of(u), :]

    def gathered_c(u):
        return full.at[:, :, :, c, rows_of(u), :]

    gz = [[remote(rx.at[0, 0, 0, rows_of(u), :], full.at[z, y, x, c, rows_of(u), :], gz_send.at[u, k - 1], gz_recv.at[u, k - 1], z_peer[k - 1]) for k in (1, 2, 3)] for u in units]
    gq = [remote(gathered_q(u), gathered_q(u), gq_send.at[u], gq_recv.at[u], q_peer(u)) for u in units]
    gp = [remote(gathered_p(u), gathered_p(u), gp_send.at[u], gp_recv.at[u], p_peer(u)) for u in units]
    gc = [remote(gathered_c(u), gathered_c(u), gc_send.at[u], gc_recv.at[u], core_peer) for u in units]

    def weight_step(u):
        t = UNITS[u][0]
        valid = valid_of(u)
        scale = LEARN_RATE * (norms[2 * t:2 * t + 1] / norms[2 * t + 1:2 * t + 2])

        def tile(r, n):
            rows = pl.ds(base(u) + r, n)
            w = state[t][:, flat_rows(u, r, n)].reshape(n, LANES)
            nw = w - scale * rz[0, rows, :]
            rz[1, rows, :] = nw
            rx[0, 0, 0, rows, :] = nw.astype(BF16)

        def body(i, carry):
            tile(pl.multiple_of(i * TILE, 16), TILE)
            return carry

        lax.fori_loop(0, valid // TILE, body, 0)
        if valid % TILE:
            tile(valid - valid % TILE, valid % TILE)
        own_copy[u].start()
        for cp in gz[u]:
            cp.start()
        out_w[u].start()

    order = list(range(n_steps))[::-1]
    for i in (0, 1):
        for u in pair(order[i]):
            weight_step(u)
    for i in range(n_steps + 3):
        if i < n_steps:
            for u in pair(order[i]):
                own_copy[u].wait()
                with jax.named_scope(f"wait_gz#u={u}"):
                    for cp in gz[u]:
                        cp.wait_recv()
                gq[u].start()
        if i + 2 < n_steps:
            for u in pair(order[i + 2]):
                weight_step(u)
        if 0 <= i - 1 < n_steps:
            for u in pair(order[i - 1]):
                with jax.named_scope(f"wait_gq#u={u}"):
                    gq[u].wait_recv()
                gp[u].start()
        if 0 <= i - 2 < n_steps:
            for u in pair(order[i - 2]):
                with jax.named_scope(f"wait_gp#u={u}"):
                    gp[u].wait_recv()
                gc[u].start()
        if 0 <= i - 3 < n_steps:
            for u in pair(order[i - 3]):
                with jax.named_scope(f"wait_gc#u={u}"):
                    gc[u].wait_recv()

    for u in units:
        if u >= n_units - 4:
            p_copy[u].wait_send()
        if u >= n_units - 2:
            c_copy[u].wait_send()
        q_copy[u].wait_send()
        for cp in z_copy[u] + gz[u]:
            cp.wait_send()
        gq[u].wait_send()
        gp[u].wait_send()
        gc[u].wait_send()
        out_m[u].wait()
        out_v[u].wait()
        out_w[u].wait()


def comm(grads, state):
    n_units = len(UNITS)
    any_spec = pl.BlockSpec(memory_space=pl.ANY)
    dma = pltpu.SemaphoreType.DMA
    return pl.pallas_call(
        comm_kernel,
        in_specs=[any_spec] * 16,
        out_specs=[any_spec] * 4,
        out_shape=[jax.ShapeDtypeStruct((4, 2, 2, 2, TOTAL, LANES), BF16)] + [jax.ShapeDtypeStruct((TOTAL, LANES), F32)] * 3,
        scratch_shapes=[pltpu.VMEM((1, r * LANES), F32) for r in ROWS] * 3
        + [
            pltpu.VMEM((4, 2, 2, TOTAL, LANES), BF16),
            pltpu.VMEM((4, 2, TOTAL, LANES), F32),
            pltpu.VMEM((4, TOTAL, LANES), F32),
            pltpu.VMEM((3, TOTAL, LANES), F32),
            pltpu.VMEM((2, 4, 2, MAX_ROWS, LANES), F32),
            pltpu.VMEM((2, 4, 2, 2, MAX_ROWS, LANES), BF16),
            pltpu.VMEM((2, 2, 4, 2, 2, MAX_ROWS, LANES), BF16),
            pltpu.VMEM((2, 4, 2, 2, 1, MAX_ROWS * LANES), BF16),
            pltpu.VMEM((8, LANES), F32),
            pltpu.VMEM((12, 8, LANES), F32),
            dma((12,)), dma((2,)),
            dma((n_units,)), dma((n_units,)), dma((n_units,)), dma((n_units,)), dma((n_units,)), dma((n_units,)),
            dma((n_units, 3)), dma((n_units, 3)), dma((11,)), dma((12,)), dma((3, n_units)), dma((n_units,)),
            dma((n_units, 3)), dma((n_units, 3)), dma((n_units,)), dma((n_units,)), dma((n_units,)), dma((n_units,)),
            dma((n_units,)), dma((n_units,)),
        ],
        compiler_params=pltpu.CompilerParams(collective_id=0, has_side_effects=True, vmem_limit_bytes=64 * 1024 * 1024 - 128 * 1024),
        name="lamb_comm",
    )(*grads, *state)


def solution(mesh):
    grad_spec = P("data", None, None)
    shard_spec = P(None, "data")
    full_spec = P(None, None)

    def device_step(*blocks):
        grads = [blocks[4 * t].reshape(4, 2, 2, 2, 1, -1) for t in range(4)]
        state = [blocks[4 * t + s] for s in (1, 2, 3) for t in range(4)]
        full, w, m, v = comm(grads, state)
        outs = unpack(full.reshape(32, TOTAL, LANES), w, m, v)
        results = []
        for t in range(4):
            results.extend((outs[t], outs[4 + t], outs[8 + t], outs[12 + t]))
        return tuple(results)

    return jax.shard_map(device_step, mesh=mesh, in_specs=(grad_spec, shard_spec, shard_spec, shard_spec) * 4, out_specs=(full_spec, shard_spec, shard_spec, shard_spec) * 4, check_vma=False)
```

```python
import functools

import jax
import jax.numpy as jnp
from jax import lax
from jax.experimental import pallas as pl
from jax.experimental.pallas import tpu as pltpu
from jax.sharding import PartitionSpec as P

STEP = 10
LEARN_RATE = 0.1
BETA_ONE = 0.9
BETA_TWO = 0.999
EPSILON = 1e-6
WEIGHT_DECAY = 0.01

LANES = 128
ROWS = (867, 289, 1156, 1156)
PADDED = (880, 304, 1168, 1168)
STARTS = (0, 880, 1184, 2352)
TOTAL = 3520
STEPS = (
    ((2, 0, 192), (2, 192, 176)),
    ((2, 368, 176), (2, 544, 192)),
    ((3, 0, 192), (3, 192, 192)),
    ((3, 384, 192), (3, 576, 192)),
    ((3, 768, 192), (3, 960, 208)),
    ((0, 0, 224), (0, 224, 224)),
    ((0, 448, 224), (0, 672, 208)),
    ((1, 0, 80), (1, 80, 80)),
    ((1, 160, 80), (1, 240, 64)),
)
THIRD = ((2, 736, 208, 2), (2, 944, 224, 2))
UNITS = tuple(unit + (colour,) for step in STEPS for colour, unit in enumerate(step)) + THIRD
MAX_ROWS = 224
LAG = 4
TILE = 48
MESH = pl.DeviceIdType.MESH
F32 = jnp.float32
BF16 = jnp.bfloat16


def unpack_kernel(full, w, m, v, c0, c1, c2, c3, *outs):
    for t, ref in enumerate((c0, c1, c2, c3)):
        ref[...] = full[0, pl.ds(STARTS[t], ROWS[t]), :].astype(F32).reshape(1, ROWS[t] * LANES).astype(BF16)

    @pl.when(pl.program_id(0) == 0)
    def _():
        for s, src in enumerate((w, m, v)):
            for t in range(4):
                outs[4 * s + t][...] = src[pl.ds(STARTS[t], ROWS[t]), :].reshape(1, ROWS[t] * LANES)


def unpack(full, w, m, v):
    state = pl.BlockSpec((TOTAL, LANES), lambda i: (0, 0))
    return pl.pallas_call(
        unpack_kernel,
        grid=(32,),
        in_specs=[pl.BlockSpec((1, TOTAL, LANES), lambda i: (i, 0, 0)), state, state, state],
        out_specs=[pl.BlockSpec((1, r * LANES), lambda i: (0, i)) for r in ROWS]
        + [pl.BlockSpec((1, r * LANES), lambda i: (0, 0)) for r in ROWS] * 3,
        out_shape=[jax.ShapeDtypeStruct((1, 32 * r * LANES), BF16) for r in ROWS]
        + [jax.ShapeDtypeStruct((1, r * LANES), F32) for r in ROWS] * 3,
        name="unpack",
    )(full, w, m, v)


def comm_kernel(*refs):
    grads = refs[0:4]
    state_in = refs[4:16]
    full, new_w, new_m, new_v = refs[16:20]
    state = refs[20:32]
    (rx, r2, r3, rz, t2, lx, ps, stage, rx3, t23, ps3, ns, nr, state_sem, stage_sem, p_send, p_recv, c_send, c_recv, q_send, q_recv,
     z_send, z_recv, n_send, n_recv, out_sem, own_sem, gz_send, gz_recv, gq_send, gq_recv, gp_send, gp_recv,
     gc_send, gc_recv) = refs[32:]

    me = lax.axis_index("data")
    c = me % 2
    x = (me // 2) % 2
    y = (me // 4) % 2
    z = me // 8

    def dev(zz, yy, xx, cc):
        return (((zz * 2 + yy) * 2 + xx) * 2 + cc,)

    def flip(value, by):
        return 1 - value if by else value

    core_peer = dev(z, y, x, 1 - c)
    x_peer = dev(z, y, 1 - x, c)
    y_peer = dev(z, 1 - y, x, c)
    z_peer = [dev((z + k) % 4, y, x, c) for k in (1, 2, 3)]
    plane_peer = [dev(z, flip(y, k // 4), flip(x, k // 2 % 2), flip(c, k % 2)) for k in range(1, 8)]
    plane_slot = [flip(y, k // 4) * 4 + flip(x, k // 2 % 2) * 2 + flip(c, k % 2) for k in range(8)]

    barrier = pltpu.get_barrier_semaphore()
    for peer in plane_peer + z_peer:
        pl.semaphore_signal(barrier, inc=1, device_id=peer, device_id_type=MESH)

    def remote(src, dst, ssem, rsem, peer):
        return pltpu.make_async_remote_copy(src_ref=src, dst_ref=dst, send_sem=ssem, recv_sem=rsem, device_id=peer, device_id_type=MESH)

    n_units = len(UNITS)
    n_steps = len(STEPS)
    units = range(n_units)

    def base(u):
        return STARTS[UNITS[u][0]] + UNITS[u][1]

    def rows_of(u):
        return pl.ds(base(u), UNITS[u][2])

    def valid_of(u):
        return min(UNITS[u][2], ROWS[UNITS[u][0]] - UNITS[u][1])

    def p_peer(u):
        return x_peer if UNITS[u][3] == 0 else y_peer

    def q_peer(u):
        return y_peer if UNITS[u][3] == 0 else x_peer

    def q_me(u):
        return y if UNITS[u][3] == 0 else x

    third = [2 * n_steps + i for i in range(len(THIRD))]
    pair_units = range(2 * n_steps)

    def stage_copy(u, mine):
        t, first, h, colour = UNITS[u]
        lanes = pl.ds(first * LANES, valid_of(u) * LANES)
        if colour == 0:
            src = grads[t].at[:, :, x if mine else 1 - x, :, :, lanes]
        else:
            src = grads[t].at[:, y if mine else 1 - y, :, :, :, lanes]
        return pltpu.make_async_copy(src, stage.at[colour, :, :, :, :, pl.ds(0, valid_of(u) * LANES)], stage_sem.at[colour])

    def pack(u, store):
        h, colour = UNITS[u][2:]
        valid = valid_of(u)

        def body(j, carry):
            for cc in (0, 1):
                dense = stage[colour, j // 2, j % 2, cc, :, pl.ds(0, valid * LANES)].reshape(valid, LANES)
                if valid < h:
                    dense = jnp.concatenate([dense, jnp.zeros((h - valid, LANES), BF16)], axis=0)
                store(j // 2, j % 2, cc, dense)
            return carry

        lax.fori_loop(0, 8, body, 0)

    def pack_send(u):
        h, colour = UNITS[u][2:]

        def store(zz, qq, cc, dense):
            ps[colour, (u // 2) % 2, zz, qq, cc, pl.ds(0, h), :] = dense

        pack(u, store)

    def pack_own(u):
        h, colour = UNITS[u][2:]

        def store(zz, qq, cc, dense):
            lx[colour, zz, qq, cc, pl.ds(0, h), :] = dense

        pack(u, store)

    p_copy = [remote(ps.at[u % 2, (u // 2) % 2, :, :, :, pl.ds(0, UNITS[u][2]), :], rx.at[:, :, :, rows_of(u), :], p_send.at[u], p_recv.at[u], p_peer(u)) for u in pair_units]
    c_copy = [remote(t2.at[u % 2, :, :, pl.ds(0, UNITS[u][2]), :], r2.at[:, :, rows_of(u), :], c_send.at[u], c_recv.at[u], core_peer) for u in pair_units]
    q_copy = [remote(r2.at[:, 1 - q_me(u), rows_of(u), :], r3.at[:, rows_of(u), :], q_send.at[u], q_recv.at[u], q_peer(u)) for u in pair_units]
    z_copy = [[remote(r3.at[(z + k) % 4, rows_of(u), :], rz.at[k - 1, rows_of(u), :], z_send.at[u, k - 1], z_recv.at[u, k - 1], z_peer[k - 1]) for k in (1, 2, 3)] for u in pair_units]
    out_m = [pltpu.make_async_copy(r2.at[0, q_me(u), rows_of(u), :], new_m.at[rows_of(u), :], out_sem.at[0, u]) for u in units]
    out_v = [pltpu.make_async_copy(r2.at[1, q_me(u), rows_of(u), :], new_v.at[rows_of(u), :], out_sem.at[1, u]) for u in units]
    out_w = [pltpu.make_async_copy(rz.at[1, rows_of(u), :], new_w.at[rows_of(u), :], out_sem.at[2, u]) for u in units]
    own_copy = [pltpu.make_async_copy(rx.at[0, 0, 0, rows_of(u), :], full.at[z, y, x, c, rows_of(u), :], own_sem.at[u]) for u in units]
    state_copy = [pltpu.make_async_copy(state_in[i], state[i], state_sem.at[i]) for i in range(12)]

    def core_step(u):
        with jax.named_scope(f"wait_p#u={u}"):
            p_copy[u].wait_recv()
        if u >= 2:
            c_copy[u - 2].wait_send()

        def body(i, carry):
            r = pl.multiple_of(i * 16, 16)
            a = lx[u % 2, :, :, 1 - c, pl.ds(r, 16), :].astype(F32)
            b = rx[:, :, 1 - c, pl.ds(base(u) + r, 16), :].astype(F32)
            t2[u % 2, :, :, pl.ds(r, 16), :] = a + b
            return carry

        lax.fori_loop(0, UNITS[u][2] // 16, body, 0)
        c_copy[u].start()

    def q_step(u):
        with jax.named_scope(f"wait_c#u={u}"):
            c_copy[u].wait_recv()

        def body(i, carry):
            r = pl.multiple_of(i * 16, 16)
            a = lx[u % 2, :, :, c, pl.ds(r, 16), :].astype(F32)
            b = rx[:, :, c, pl.ds(base(u) + r, 16), :].astype(F32)
            r2[:, :, pl.ds(base(u) + r, 16), :] = r2[:, :, pl.ds(base(u) + r, 16), :] + (a + b)
            return carry

        lax.fori_loop(0, UNITS[u][2] // 16, body, 0)
        q_copy[u].start()

    def z_step(u):
        with jax.named_scope(f"wait_q#u={u}"):
            q_copy[u].wait_recv()

        def body(i, carry):
            r = pl.multiple_of(base(u) + i * 16, 16)
            r3[:, pl.ds(r, 16), :] = r3[:, pl.ds(r, 16), :] + r2[:, q_me(u), pl.ds(r, 16), :]
            return carry

        lax.fori_loop(0, UNITS[u][2] // 16, body, 0)
        for cp in z_copy[u]:
            cp.start()

    def third_parts(u):
        i, h = u - 2 * n_steps, UNITS[u][2]
        rows = rows_of(u)
        short = pl.ds(0, h)
        landing = [rx.at[0:2, :, :, rows, :], rx.at[2:4, :, :, rows, :], rx3.at[i, :, :, :, short, :]]
        first = [remote(ps3.at[i, (z + k) % 4, :, :, :, short, :], landing[k - 1], z_send.at[u, k - 1], z_recv.at[u, k - 1], z_peer[k - 1]) for k in (1, 2, 3)]
        core = remote(t23.at[i, :, :, short, :], r2.at[0:2, :, rows, :], c_send.at[u], c_recv.at[u], core_peer)
        along_x = remote(r2.at[0:2, 1 - x, rows, :], r3.at[0:2, rows, :], q_send.at[u], q_recv.at[u], x_peer)
        along_y = remote(r3.at[1 - y, rows, :], rz.at[0, rows, :], p_send.at[u], p_recv.at[u], y_peer)
        return first, core, along_x, along_y

    third_copy = {u: third_parts(u) for u in third}

    def third_stage(u):
        t, first, h, colour = UNITS[u]
        valid = valid_of(u)
        lanes = pl.ds(first * LANES, valid * LANES)
        copies = [pltpu.make_async_copy(grads[t].at[:, :, :, cc, :, lanes], stage.at[cc, :, :, :, :, pl.ds(0, valid * LANES)], stage_sem.at[cc]) for cc in (0, 1)]
        for cp in copies:
            cp.start()
        for cp in copies:
            cp.wait()

        def body(j, carry):
            for xx in (0, 1):
                for cc in (0, 1):
                    dense = stage[cc, j // 2, j % 2, xx, :, pl.ds(0, valid * LANES)].reshape(valid, LANES)
                    if valid < h:
                        dense = jnp.concatenate([dense, jnp.zeros((h - valid, LANES), BF16)], axis=0)
                    ps3[u - 2 * n_steps, j // 2, j % 2, xx, cc, pl.ds(0, h), :] = dense
            return carry

        lax.fori_loop(0, 8, body, 0)
        for cp in third_copy[u][0]:
            cp.start()

    def third_sum(u, r, cc):
        i = u - 2 * n_steps
        near = pl.ds(base(u) + r, 16)
        own = ps3[i, z, :, :, cc, pl.ds(r, 16), :].astype(F32) + rx[0:2, :, cc, near, :].astype(F32)
        return own + (rx[2:4, :, cc, near, :].astype(F32) + rx3[i, :, :, cc, pl.ds(r, 16), :].astype(F32))

    def third_core_step(u):
        with jax.named_scope(f"wait_third_z#u={u}"):
            for cp in third_copy[u][0]:
                cp.wait_recv()

        def body(i, carry):
            r = pl.multiple_of(i * 16, 16)
            t23[u - 2 * n_steps, :, :, pl.ds(r, 16), :] = third_sum(u, r, 1 - c)
            return carry

        lax.fori_loop(0, UNITS[u][2] // 16, body, 0)
        third_copy[u][1].start()

    def third_x_step(u):
        third_copy[u][1].wait_recv()

        def body(i, carry):
            r = pl.multiple_of(i * 16, 16)
            near = pl.ds(base(u) + r, 16)
            r2[0:2, :, near, :] = r2[0:2, :, near, :] + third_sum(u, r, c)
            return carry

        lax.fori_loop(0, UNITS[u][2] // 16, body, 0)
        third_copy[u][2].start()

    def third_y_step(u):
        with jax.named_scope(f"wait_third_x#u={u}"):
            third_copy[u][2].wait_recv()

        def body(i, carry):
            near = pl.ds(pl.multiple_of(base(u) + i * 16, 16), 16)
            r3[0:2, near, :] = r3[0:2, near, :] + r2[0:2, x, near, :]
            return carry

        lax.fori_loop(0, UNITS[u][2] // 16, body, 0)
        third_copy[u][3].start()

    def flat_rows(u, r, n):
        start = (UNITS[u][1] + r) * LANES
        return pl.ds(start if isinstance(r, int) else pl.multiple_of(start, LANES), n * LANES)

    def lamb_step(u):
        t, first, h, colour = UNITS[u]
        with jax.named_scope(f"wait_z#u={u}"):
            if colour == 2:
                third_copy[u][3].wait_recv()
            else:
                for cp in z_copy[u]:
                    cp.wait_recv()
        if first == 0:
            for i in (t, 4 + t, 8 + t):
                state_copy[i].wait()
        valid = valid_of(u)
        q = q_me(u)

        def tile(r, n):
            rows = pl.ds(base(u) + r, n)
            flat = flat_rows(u, r, n)
            w = state[t][:, flat].reshape(n, LANES)
            m = state[4 + t][:, flat].reshape(n, LANES)
            v = state[8 + t][:, flat].reshape(n, LANES)
            if colour == 2:
                g = (r3[y, rows, :] + rz[0, rows, :]) / 32.0
            else:
                g = (((r3[z, rows, :] + rz[0, rows, :]) + rz[1, rows, :]) + rz[2, rows, :]) / 32.0
            nm = BETA_ONE * m + (1.0 - BETA_ONE) * g
            nv = BETA_TWO * v + (1.0 - BETA_TWO) * g * g
            u_dir = (nm / (1.0 - BETA_ONE ** STEP)) / (jnp.sqrt(nv / (1.0 - BETA_TWO ** STEP)) + EPSILON) + WEIGHT_DECAY * w
            r2[0, q, rows, :] = nm
            r2[1, q, rows, :] = nv
            rz[0, rows, :] = u_dir
            return w * w, u_dir * u_dir

        def body(i, carry):
            ww, uu = tile(pl.multiple_of(i * TILE, 16), TILE)
            return (carry[0] + jnp.sum(ww.reshape(TILE // 8, 8, LANES), axis=0), carry[1] + jnp.sum(uu.reshape(TILE // 8, 8, LANES), axis=0))

        zero = jnp.zeros((8, LANES), F32)
        acc_w, acc_u = lax.fori_loop(0, valid // TILE, body, (zero, zero))
        sum_w = jnp.sum(acc_w, axis=0, keepdims=True)
        sum_u = jnp.sum(acc_u, axis=0, keepdims=True)
        if valid % TILE:
            ww, uu = tile(valid - valid % TILE, valid % TILE)
            sum_w = sum_w + jnp.sum(ww, axis=0, keepdims=True)
            sum_u = sum_u + jnp.sum(uu, axis=0, keepdims=True)
        ns[pl.ds(2 * t, 1), :] = ns[pl.ds(2 * t, 1), :] + sum_w
        ns[pl.ds(2 * t + 1, 1), :] = ns[pl.ds(2 * t + 1, 1), :] + sum_u
        out_m[u].start()
        out_v[u].start()

    def pair(s):
        return (2 * s, 2 * s + 1)

    for s in (0, 1):
        for u in pair(s):
            stage_copy(u, False).start()
        if s == 0:
            for cp in state_copy:
                cp.start()
            ns[...] = jnp.zeros_like(ns)
        for u in pair(s):
            stage_copy(u, False).wait()
            pack_send(u)
        if s == 0:
            pl.semaphore_wait(barrier, 10)
        for u in pair(s):
            p_copy[u].start()
        third_stage(third[s])
    for u in pair(0):
        stage_copy(u, True).start()
    for u in pair(0):
        stage_copy(u, True).wait()
        pack_own(u)
        stage_copy(u + 4, False).start()

    for s in range(n_steps + LAG):
        if s < n_steps:
            for u in pair(s):
                core_step(u)
            for u in pair(s):
                q_step(u)
            if s == 4:
                for u in third:
                    third_core_step(u)
            if s == n_steps - 2:
                third_x_step(third[0])
            if s == n_steps - 1:
                third_x_step(third[1])
                third_y_step(third[0])
            if s + 2 < n_steps:
                for u in pair(s + 2):
                    stage_copy(u, False).wait()
                    p_copy[u - 4].wait_send()
                    pack_send(u)
                    p_copy[u].start()
            if s + 1 < n_steps:
                for u in pair(s + 1):
                    stage_copy(u, True).start()
                for u in pair(s + 1):
                    stage_copy(u, True).wait()
                    pack_own(u)
                    if s + 3 < n_steps:
                        stage_copy(u + 4, False).start()
        if 0 <= s - 1 < n_steps:
            for u in pair(s - 1):
                z_step(u)
        if s == n_steps:
            third_y_step(third[1])
        if 0 <= s - LAG < n_steps:
            for u in pair(s - LAG):
                lamb_step(u)
    for u in third:
        lamb_step(u)

    with jax.named_scope("norms"):
        plane_norm = [remote(ns, nr.at[plane_slot[0]], n_send.at[k], n_recv.at[plane_slot[0]], plane_peer[k - 1]) for k in range(1, 8)]
        for cp in plane_norm:
            cp.start()
        nr[plane_slot[0]] = ns[...]
        for k in range(1, 8):
            remote(ns, nr.at[plane_slot[k]], n_send.at[k], n_recv.at[plane_slot[k]], plane_peer[k - 1]).wait_recv()
        for cp in plane_norm:
            cp.wait_send()
        ns[...] = ((nr[0] + nr[1]) + (nr[2] + nr[3])) + ((nr[4] + nr[5]) + (nr[6] + nr[7]))
        z_norm = [remote(ns, nr.at[8 + z], n_send.at[7 + k], n_recv.at[8 + z], z_peer[k - 1]) for k in (1, 2, 3)]
        for cp in z_norm:
            cp.start()
        nr[8 + z] = ns[...]
        for k in (1, 2, 3):
            zz = (z + k) % 4
            remote(ns, nr.at[8 + zz], n_send.at[7 + k], n_recv.at[8 + zz], z_peer[k - 1]).wait_recv()
        for cp in z_norm:
            cp.wait_send()
    total = (nr[8] + nr[9]) + (nr[10] + nr[11])
    norms = jnp.sqrt(jnp.sum(total, axis=1, keepdims=True))

    def gathered_q(u):
        if UNITS[u][3] == 2:
            return full.at[z, y, x, c, rows_of(u), :]
        return full.at[:, y, x, c, rows_of(u), :]

    def gathered_p(u):
        if UNITS[u][3] == 0:
            return full.at[:, :, x, c, rows_of(u), :]
        if UNITS[u][3] == 2:
            return full.at[z, :, x, c, rows_of(u), :]
        return full.at[:, y, :, c, rows_of(u), :]

    def gathered_c(u):
        return full.at[:, :, :, c, rows_of(u), :]

    def gather_z(u, k):
        src = rx.at[0, 0, 0, rows_of(u), :]
        dst = full.at[z, y, x, c, rows_of(u), :]
        if UNITS[u][3] == 2:
            src = dst = full.at[z, :, :, c, rows_of(u), :]
        return remote(src, dst, gz_send.at[u, k - 1], gz_recv.at[u, k - 1], z_peer[k - 1])

    gz = [[gather_z(u, k) for k in (1, 2, 3)] for u in units]
    gq = [remote(gathered_q(u), gathered_q(u), gq_send.at[u], gq_recv.at[u], y_peer if UNITS[u][3] == 2 else q_peer(u)) for u in units]
    gp = [remote(gathered_p(u), gathered_p(u), gp_send.at[u], gp_recv.at[u], x_peer if UNITS[u][3] == 2 else p_peer(u)) for u in units]
    gc = [remote(gathered_c(u), gathered_c(u), gc_send.at[u], gc_recv.at[u], core_peer) for u in units]

    def weight_step(u):
        t = UNITS[u][0]
        valid = valid_of(u)
        scale = LEARN_RATE * (norms[2 * t:2 * t + 1] / norms[2 * t + 1:2 * t + 2])

        def tile(r, n):
            rows = pl.ds(base(u) + r, n)
            w = state[t][:, flat_rows(u, r, n)].reshape(n, LANES)
            nw = w - scale * rz[0, rows, :]
            rz[1, rows, :] = nw
            rx[0, 0, 0, rows, :] = nw.astype(BF16)

        def body(i, carry):
            tile(pl.multiple_of(i * TILE, 16), TILE)
            return carry

        lax.fori_loop(0, valid // TILE, body, 0)
        if valid % TILE:
            tile(valid - valid % TILE, valid % TILE)
        own_copy[u].start()
        out_w[u].start()
        if UNITS[u][3] == 2:
            own_copy[u].wait()
            gq[u].start()
        else:
            for cp in gz[u]:
                cp.start()

    def third_gather_z(u):
        with jax.named_scope(f"wait_third_gx#u={u}"):
            gp[u].wait_recv()
        for cp in gz[u]:
            cp.start()

    def third_gather_core(u):
        with jax.named_scope(f"wait_third_gz#u={u}"):
            for cp in gz[u]:
                cp.wait_recv()
        gc[u].start()

    order = list(range(n_steps))[::-1]
    for u in pair(order[0]):
        weight_step(u)
    for u in third:
        weight_step(u)
    for u in pair(order[1]):
        weight_step(u)
    for i in range(n_steps + 3):
        if i < n_steps:
            for u in pair(order[i]):
                own_copy[u].wait()
                with jax.named_scope(f"wait_gz#u={u}"):
                    for cp in gz[u]:
                        cp.wait_recv()
                gq[u].start()
        if i == 0:
            for u in third:
                gq[u].wait_recv()
                gp[u].start()
        if i + 2 < n_steps:
            for u in pair(order[i + 2]):
                weight_step(u)
        if i == 3:
            third_gather_z(third[0])
        if i == n_steps - 3:
            third_gather_z(third[1])
        if 0 <= i - 1 < n_steps:
            for u in pair(order[i - 1]):
                with jax.named_scope(f"wait_gq#u={u}"):
                    gq[u].wait_recv()
                gp[u].start()
        if i == n_steps - 1:
            third_gather_core(third[0])
        if 0 <= i - 2 < n_steps:
            for u in pair(order[i - 2]):
                with jax.named_scope(f"wait_gp#u={u}"):
                    gp[u].wait_recv()
                gc[u].start()
        if i == n_steps + 1:
            third_gather_core(third[1])
        if 0 <= i - 3 < n_steps:
            for u in pair(order[i - 3]):
                with jax.named_scope(f"wait_gc#u={u}"):
                    gc[u].wait_recv()
    for u in third:
        gc[u].wait_recv()

    for u in pair_units:
        if u >= 2 * n_steps - 4:
            p_copy[u].wait_send()
        if u >= 2 * n_steps - 2:
            c_copy[u].wait_send()
        q_copy[u].wait_send()
        for cp in z_copy[u]:
            cp.wait_send()
    for u in third:
        for cp in third_copy[u][0] + list(third_copy[u][1:]):
            cp.wait_send()
    for u in units:
        for cp in gz[u]:
            cp.wait_send()
        gq[u].wait_send()
        gp[u].wait_send()
        gc[u].wait_send()
        out_m[u].wait()
        out_v[u].wait()
        out_w[u].wait()


def comm(grads, state):
    n_units = len(UNITS)
    any_spec = pl.BlockSpec(memory_space=pl.ANY)
    dma = pltpu.SemaphoreType.DMA
    return pl.pallas_call(
        comm_kernel,
        in_specs=[any_spec] * 16,
        out_specs=[any_spec] * 4,
        out_shape=[jax.ShapeDtypeStruct((4, 2, 2, 2, TOTAL, LANES), BF16)] + [jax.ShapeDtypeStruct((TOTAL, LANES), F32)] * 3,
        scratch_shapes=[pltpu.VMEM((1, r * LANES), F32) for r in ROWS] * 3
        + [
            pltpu.VMEM((4, 2, 2, TOTAL, LANES), BF16),
            pltpu.VMEM((4, 2, TOTAL, LANES), F32),
            pltpu.VMEM((4, TOTAL, LANES), F32),
            pltpu.VMEM((3, TOTAL, LANES), F32),
            pltpu.VMEM((2, 4, 2, MAX_ROWS, LANES), F32),
            pltpu.VMEM((2, 4, 2, 2, MAX_ROWS, LANES), BF16),
            pltpu.VMEM((2, 2, 4, 2, 2, MAX_ROWS, LANES), BF16),
            pltpu.VMEM((2, 4, 2, 2, 1, MAX_ROWS * LANES), BF16),
            pltpu.VMEM((2, 2, 2, 2, MAX_ROWS, LANES), BF16),
            pltpu.VMEM((2, 2, 2, MAX_ROWS, LANES), F32),
            pltpu.VMEM((2, 4, 2, 2, 2, MAX_ROWS, LANES), BF16),
            pltpu.VMEM((8, LANES), F32),
            pltpu.VMEM((12, 8, LANES), F32),
            dma((12,)), dma((2,)),
            dma((n_units,)), dma((n_units,)), dma((n_units,)), dma((n_units,)), dma((n_units,)), dma((n_units,)),
            dma((n_units, 3)), dma((n_units, 3)), dma((11,)), dma((12,)), dma((3, n_units)), dma((n_units,)),
            dma((n_units, 3)), dma((n_units, 3)), dma((n_units,)), dma((n_units,)), dma((n_units,)), dma((n_units,)),
            dma((n_units,)), dma((n_units,)),
        ],
        compiler_params=pltpu.CompilerParams(collective_id=0, has_side_effects=True, vmem_limit_bytes=64 * 1024 * 1024 - 128 * 1024),
        name="lamb_comm",
    )(*grads, *state)


def solution(mesh):
    grad_spec = P("data", None, None)
    shard_spec = P(None, "data")
    full_spec = P(None, None)

    def device_step(*blocks):
        grads = [blocks[4 * t].reshape(4, 2, 2, 2, 1, -1) for t in range(4)]
        state = [blocks[4 * t + s] for s in (1, 2, 3) for t in range(4)]
        full, w, m, v = comm(grads, state)
        outs = unpack(full.reshape(32, TOTAL, LANES), w, m, v)
        results = []
        for t in range(4):
            results.extend((outs[t], outs[4 + t], outs[8 + t], outs[12 + t]))
        return tuple(results)

    return jax.shard_map(device_step, mesh=mesh, in_specs=(grad_spec, shard_spec, shard_spec, shard_spec) * 4, out_specs=(full_spec, shard_spec, shard_spec, shard_spec) * 4, check_vma=False)
```

```python
import functools

import jax
import jax.numpy as jnp
from jax import lax
from jax.experimental import pallas as pl
from jax.experimental.pallas import tpu as pltpu
from jax.sharding import PartitionSpec as P

STEP = 10
LEARN_RATE = 0.1
BETA_ONE = 0.9
BETA_TWO = 0.999
EPSILON = 1e-6
WEIGHT_DECAY = 0.01

LANES = 128
ROWS = (867, 289, 1156, 1156)
PADDED = (880, 304, 1168, 1168)
STARTS = (0, 880, 1184, 2352)
TOTAL = 3520
PLAN = (
    (2, ((192, 176), (176, 192))),
    (3, ((192, 192), (192, 192), (192, 208))),
    (0, ((224, 224), (224, 208))),
    (1, ((80, 80), (80, 64))),
)
THIRD_ROWS = (208, 224)


def plan_units():
    units, third = [], []
    for t, pairs in PLAN:
        first = 0
        for rows_pair in pairs:
            for colour, rows in enumerate(rows_pair):
                units.append((t, first, rows, colour))
                first += rows
        if not third:
            for rows in THIRD_ROWS:
                third.append((t, first, rows, len(rows_pair)))
                first += rows
    return tuple(units), tuple(third)


PAIRED, THIRD = plan_units()
UNITS = PAIRED + THIRD
MAX_ROWS = 224
LAG = 4
TILE = 48
SUB = 16
HOPS = (1, 2, 3)
BOTH = (0, 1)
MESH = pl.DeviceIdType.MESH
F32 = jnp.float32
BF16 = jnp.bfloat16


def unpack_kernel(full, w, m, v, c0, c1, c2, c3, *outs):
    for t, ref in enumerate((c0, c1, c2, c3)):
        dense = full[0, pl.ds(STARTS[t], (ROWS[t] + SUB - 1) // SUB * SUB), :]
        ref[0, :] = dense.reshape(-1)[:ROWS[t] * LANES]

    @pl.when(pl.program_id(0) == 0)
    def _():
        for s, src in enumerate((w, m, v)):
            for t in range(4):
                outs[4 * s + t][...] = src[pl.ds(STARTS[t], ROWS[t]), :].reshape(1, ROWS[t] * LANES)


def unpack(full, w, m, v):
    state = pl.BlockSpec((TOTAL, LANES), lambda i: (0, 0))
    return pl.pallas_call(
        unpack_kernel,
        grid=(32,),
        in_specs=[pl.BlockSpec((1, TOTAL, LANES), lambda i: (i, 0, 0)), state, state, state],
        out_specs=[pl.BlockSpec((1, r * LANES), lambda i: (0, i)) for r in ROWS]
        + [pl.BlockSpec((1, r * LANES), lambda i: (0, 0)) for r in ROWS] * 3,
        out_shape=[jax.ShapeDtypeStruct((1, 32 * r * LANES), BF16) for r in ROWS]
        + [jax.ShapeDtypeStruct((1, r * LANES), F32) for r in ROWS] * 3,
        name="unpack",
    )(full, w, m, v)


def comm_kernel(*refs):
    grads = refs[0:4]
    state_in = refs[4:16]
    full, new_w, new_m, new_v = refs[16:20]
    state = refs[20:32]
    (rx, r2, r3, rz, t2, lx, ps, stage, rx3, t23, ps3, ns, nr, state_sem, stage_sem, p_send, p_recv, c_send, c_recv, q_send, q_recv,
     z_send, z_recv, n_send, n_recv, out_sem, own_sem, gz_send, gz_recv, gq_send, gq_recv, gp_send, gp_recv,
     gc_send, gc_recv) = refs[32:]

    me = lax.axis_index("data")
    c = me % 2
    x = (me // 2) % 2
    y = (me // 4) % 2
    z = me // 8

    def dev(zz, yy, xx, cc):
        return (((zz * 2 + yy) * 2 + xx) * 2 + cc,)

    def flip(value, by):
        return 1 - value if by else value

    core_peer = dev(z, y, x, 1 - c)
    x_peer = dev(z, y, 1 - x, c)
    y_peer = dev(z, 1 - y, x, c)
    z_peer = [dev((z + k) % 4, y, x, c) for k in HOPS]
    plane_peer = [dev(z, flip(y, k // 4), flip(x, k // 2 % 2), flip(c, k % 2)) for k in range(1, 8)]
    plane_slot = [flip(y, k // 4) * 4 + flip(x, k // 2 % 2) * 2 + flip(c, k % 2) for k in range(8)]

    barrier = pltpu.get_barrier_semaphore()
    for peer in plane_peer + z_peer:
        pl.semaphore_signal(barrier, inc=1, device_id=peer, device_id_type=MESH)

    def remote(src, dst, ssem, rsem, peer):
        return pltpu.make_async_remote_copy(src_ref=src, dst_ref=dst, send_sem=ssem, recv_sem=rsem, device_id=peer, device_id_type=MESH)

    n_units = len(UNITS)
    n_pair = len(PAIRED)
    n_steps = n_pair // 2
    units = range(n_units)

    def sweep(u, body):
        def step(i, carry):
            body(pl.multiple_of(i * SUB, SUB))
            return carry

        lax.fori_loop(0, height(u) // SUB, step, 0)

    def tensor(u):
        return UNITS[u][0]

    def height(u):
        return UNITS[u][2]

    def colour_of(u):
        return UNITS[u][3]

    def base(u):
        return STARTS[tensor(u)] + UNITS[u][1]

    def rows_of(u):
        return pl.ds(base(u), height(u))

    def valid_of(u):
        return min(height(u), ROWS[tensor(u)] - UNITS[u][1])

    def p_peer(u):
        return x_peer if colour_of(u) == 0 else y_peer

    def q_peer(u):
        return y_peer if colour_of(u) == 0 else x_peer

    def q_me(u):
        return y if colour_of(u) == 0 else x

    third = range(n_pair, n_units)
    pair_units = range(n_pair)

    def stage_copy(u, mine):
        t, first, h, colour = UNITS[u]
        lanes = pl.ds(first * LANES, valid_of(u) * LANES)
        if colour == 0:
            src = grads[t].at[:, :, x if mine else 1 - x, :, :, lanes]
        else:
            src = grads[t].at[:, y if mine else 1 - y, :, :, :, lanes]
        return pltpu.make_async_copy(src, stage.at[colour, :, :, :, :, pl.ds(0, valid_of(u) * LANES)], stage_sem.at[colour])

    def pack(u, store):
        h, colour = (height(u), colour_of(u))
        valid = valid_of(u)

        def body(j, carry):
            for cc in BOTH:
                dense = stage[colour, j // 2, j % 2, cc, :, pl.ds(0, valid * LANES)].reshape(valid, LANES)
                if valid < h:
                    dense = jnp.concatenate([dense, jnp.zeros((h - valid, LANES), BF16)], axis=0)
                store(j // 2, j % 2, cc, dense)
            return carry

        lax.fori_loop(0, 8, body, 0)

    def pack_send(u):
        h, colour = (height(u), colour_of(u))

        def store(zz, qq, cc, dense):
            ps[colour, (u // 2) % 2, zz, qq, cc, pl.ds(0, h), :] = dense

        pack(u, store)

    def pack_own(u):
        h, colour = (height(u), colour_of(u))

        def store(zz, qq, cc, dense):
            lx[colour, zz, qq, cc, pl.ds(0, h), :] = dense

        pack(u, store)

    p_copy = [remote(ps.at[u % 2, (u // 2) % 2, :, :, :, pl.ds(0, height(u)), :], rx.at[:, :, :, rows_of(u), :], p_send.at[u], p_recv.at[u], p_peer(u)) for u in pair_units]
    c_copy = [remote(t2.at[u % 2, :, :, pl.ds(0, height(u)), :], r2.at[:, :, rows_of(u), :], c_send.at[u], c_recv.at[u], core_peer) for u in pair_units]
    q_copy = [remote(r2.at[:, 1 - q_me(u), rows_of(u), :], r3.at[:, rows_of(u), :], q_send.at[u], q_recv.at[u], q_peer(u)) for u in pair_units]
    z_copy = [[remote(r3.at[(z + k) % 4, rows_of(u), :], rz.at[k - 1, rows_of(u), :], z_send.at[u, k - 1], z_recv.at[u, k - 1], z_peer[k - 1]) for k in HOPS] for u in pair_units]
    out_m = [pltpu.make_async_copy(r2.at[0, q_me(u), rows_of(u), :], new_m.at[rows_of(u), :], out_sem.at[0, u]) for u in units]
    out_v = [pltpu.make_async_copy(r2.at[1, q_me(u), rows_of(u), :], new_v.at[rows_of(u), :], out_sem.at[1, u]) for u in units]
    out_w = [pltpu.make_async_copy(rz.at[1, rows_of(u), :], new_w.at[rows_of(u), :], out_sem.at[2, u]) for u in units]
    own_copy = [pltpu.make_async_copy(rx.at[0, 0, 0, rows_of(u), :], full.at[z, y, x, c, rows_of(u), :], own_sem.at[u]) for u in units]
    state_copy = [pltpu.make_async_copy(state_in[i], state[i], state_sem.at[i]) for i in range(12)]

    def core_step(u):
        with jax.named_scope(f"wait_p#u={u}"):
            p_copy[u].wait_recv()
        if u >= 2:
            c_copy[u - 2].wait_send()

        def body(r):
            a = lx[u % 2, :, :, 1 - c, pl.ds(r, SUB), :].astype(F32)
            b = rx[:, :, 1 - c, pl.ds(base(u) + r, SUB), :].astype(F32)
            t2[u % 2, :, :, pl.ds(r, SUB), :] = a + b

        sweep(u, body)
        c_copy[u].start()

    def q_step(u):
        with jax.named_scope(f"wait_c#u={u}"):
            c_copy[u].wait_recv()

        def body(r):
            a = lx[u % 2, :, :, c, pl.ds(r, SUB), :].astype(F32)
            b = rx[:, :, c, pl.ds(base(u) + r, SUB), :].astype(F32)
            r2[:, :, pl.ds(base(u) + r, SUB), :] = r2[:, :, pl.ds(base(u) + r, SUB), :] + (a + b)

        sweep(u, body)
        q_copy[u].start()

    def z_step(u):
        with jax.named_scope(f"wait_q#u={u}"):
            q_copy[u].wait_recv()

        def body(r):
            near = pl.ds(base(u) + r, SUB)
            r3[:, near, :] = r3[:, near, :] + r2[:, q_me(u), near, :]

        sweep(u, body)
        for cp in z_copy[u]:
            cp.start()

    def third_parts(u):
        i, h = u - n_pair, height(u)
        rows = rows_of(u)
        short = pl.ds(0, h)
        landing = [rx.at[0:2, :, :, rows, :], rx.at[2:4, :, :, rows, :], rx3.at[i, :, :, :, short, :]]
        first = [remote(ps3.at[i, (z + k) % 4, :, :, :, short, :], landing[k - 1], z_send.at[u, k - 1], z_recv.at[u, k - 1], z_peer[k - 1]) for k in HOPS]
        core = remote(t23.at[i, :, :, short, :], r2.at[0:2, :, rows, :], c_send.at[u], c_recv.at[u], core_peer)
        along_x = remote(r2.at[0:2, 1 - x, rows, :], r3.at[0:2, rows, :], q_send.at[u], q_recv.at[u], x_peer)
        along_y = remote(r3.at[1 - y, rows, :], rz.at[0, rows, :], p_send.at[u], p_recv.at[u], y_peer)
        return first, core, along_x, along_y

    third_copy = {u: third_parts(u) for u in third}

    def third_stage(u):
        t, first, h, colour = UNITS[u]
        valid = valid_of(u)
        lanes = pl.ds(first * LANES, valid * LANES)
        copies = [pltpu.make_async_copy(grads[t].at[:, :, :, cc, :, lanes], stage.at[cc, :, :, :, :, pl.ds(0, valid * LANES)], stage_sem.at[cc]) for cc in BOTH]
        for cp in copies:
            cp.start()
        for cp in copies:
            cp.wait()

        def body(j, carry):
            for xx in BOTH:
                for cc in BOTH:
                    dense = stage[cc, j // 2, j % 2, xx, :, pl.ds(0, valid * LANES)].reshape(valid, LANES)
                    if valid < h:
                        dense = jnp.concatenate([dense, jnp.zeros((h - valid, LANES), BF16)], axis=0)
                    ps3[u - n_pair, j // 2, j % 2, xx, cc, pl.ds(0, h), :] = dense
            return carry

        lax.fori_loop(0, 8, body, 0)
        for cp in third_copy[u][0]:
            cp.start()

    def third_sum(u, r, cc):
        i = u - n_pair
        near = pl.ds(base(u) + r, SUB)
        own = ps3[i, z, :, :, cc, pl.ds(r, SUB), :].astype(F32) + rx[0:2, :, cc, near, :].astype(F32)
        return own + (rx[2:4, :, cc, near, :].astype(F32) + rx3[i, :, :, cc, pl.ds(r, SUB), :].astype(F32))

    def third_core_step(u):
        with jax.named_scope(f"wait_third_z#u={u}"):
            for cp in third_copy[u][0]:
                cp.wait_recv()

        def body(r):
            t23[u - n_pair, :, :, pl.ds(r, SUB), :] = third_sum(u, r, 1 - c)

        sweep(u, body)
        third_copy[u][1].start()

    def third_x_step(u):
        third_copy[u][1].wait_recv()

        def body(r):
            near = pl.ds(base(u) + r, SUB)
            r2[0:2, :, near, :] = r2[0:2, :, near, :] + third_sum(u, r, c)

        sweep(u, body)
        third_copy[u][2].start()

    def third_y_step(u):
        with jax.named_scope(f"wait_third_x#u={u}"):
            third_copy[u][2].wait_recv()

        def body(r):
            near = pl.ds(base(u) + r, SUB)
            r3[0:2, near, :] = r3[0:2, near, :] + r2[0:2, x, near, :]

        sweep(u, body)
        third_copy[u][3].start()

    def flat_rows(u, r, n):
        start = (UNITS[u][1] + r) * LANES
        return pl.ds(start if isinstance(r, int) else pl.multiple_of(start, LANES), n * LANES)

    def lamb_step(u):
        t, first, h, colour = UNITS[u]
        with jax.named_scope(f"wait_z#u={u}"):
            if colour == 2:
                third_copy[u][3].wait_recv()
            else:
                for cp in z_copy[u]:
                    cp.wait_recv()
        if first == 0:
            for i in (t, 4 + t, 8 + t):
                state_copy[i].wait()
        valid = valid_of(u)
        q = q_me(u)

        def tile(r, n):
            rows = pl.ds(base(u) + r, n)
            flat = flat_rows(u, r, n)
            w = state[t][:, flat].reshape(n, LANES)
            m = state[4 + t][:, flat].reshape(n, LANES)
            v = state[8 + t][:, flat].reshape(n, LANES)
            if colour == 2:
                g = (r3[y, rows, :] + rz[0, rows, :]) / 32.0
            else:
                g = (((r3[z, rows, :] + rz[0, rows, :]) + rz[1, rows, :]) + rz[2, rows, :]) / 32.0
            nm = BETA_ONE * m + (1.0 - BETA_ONE) * g
            nv = BETA_TWO * v + (1.0 - BETA_TWO) * g * g
            u_dir = (nm / (1.0 - BETA_ONE ** STEP)) / (jnp.sqrt(nv / (1.0 - BETA_TWO ** STEP)) + EPSILON) + WEIGHT_DECAY * w
            r2[0, q, rows, :] = nm
            r2[1, q, rows, :] = nv
            rz[0, rows, :] = u_dir
            return w * w, u_dir * u_dir

        def body(i, carry):
            ww, uu = tile(pl.multiple_of(i * TILE, SUB), TILE)
            return (carry[0] + jnp.sum(ww.reshape(TILE // 8, 8, LANES), axis=0), carry[1] + jnp.sum(uu.reshape(TILE // 8, 8, LANES), axis=0))

        zero = jnp.zeros((8, LANES), F32)
        acc_w, acc_u = lax.fori_loop(0, valid // TILE, body, (zero, zero))
        sum_w = jnp.sum(acc_w, axis=0, keepdims=True)
        sum_u = jnp.sum(acc_u, axis=0, keepdims=True)
        if valid % TILE:
            ww, uu = tile(valid - valid % TILE, valid % TILE)
            sum_w = sum_w + jnp.sum(ww, axis=0, keepdims=True)
            sum_u = sum_u + jnp.sum(uu, axis=0, keepdims=True)
        ns[pl.ds(2 * t, 1), :] = ns[pl.ds(2 * t, 1), :] + sum_w
        ns[pl.ds(2 * t + 1, 1), :] = ns[pl.ds(2 * t + 1, 1), :] + sum_u
        out_m[u].start()
        out_v[u].start()

    def pair(s):
        return (2 * s, 2 * s + 1)

    for s in BOTH:
        for u in pair(s):
            stage_copy(u, False).start()
        if s == 0:
            for cp in state_copy:
                cp.start()
            ns[...] = jnp.zeros_like(ns)
        for u in pair(s):
            stage_copy(u, False).wait()
            pack_send(u)
        if s == 0:
            pl.semaphore_wait(barrier, 10)
        for u in pair(s):
            p_copy[u].start()
        third_stage(third[s])
    for u in pair(0):
        stage_copy(u, True).start()
    for u in pair(0):
        stage_copy(u, True).wait()
        pack_own(u)
        stage_copy(u + 4, False).start()

    for s in range(n_steps + LAG):
        if s < n_steps:
            for u in pair(s):
                core_step(u)
            for u in pair(s):
                q_step(u)
            if s == 4:
                for u in third:
                    third_core_step(u)
            if s == n_steps - 2:
                third_x_step(third[0])
            if s == n_steps - 1:
                third_x_step(third[1])
                third_y_step(third[0])
            if s + 2 < n_steps:
                for u in pair(s + 2):
                    stage_copy(u, False).wait()
                    p_copy[u - 4].wait_send()
                    pack_send(u)
                    p_copy[u].start()
            if s + 1 < n_steps:
                for u in pair(s + 1):
                    stage_copy(u, True).start()
                for u in pair(s + 1):
                    stage_copy(u, True).wait()
                    pack_own(u)
                    if s + 3 < n_steps:
                        stage_copy(u + 4, False).start()
        if 0 <= s - 1 < n_steps:
            for u in pair(s - 1):
                z_step(u)
        if s == n_steps:
            third_y_step(third[1])
        if 0 <= s - LAG < n_steps:
            for u in pair(s - LAG):
                lamb_step(u)
    for u in third:
        lamb_step(u)

    with jax.named_scope("norms"):
        plane_norm = [remote(ns, nr.at[plane_slot[0]], n_send.at[k], n_recv.at[plane_slot[0]], plane_peer[k - 1]) for k in range(1, 8)]
        for cp in plane_norm:
            cp.start()
        nr[plane_slot[0]] = ns[...]
        for k in range(1, 8):
            remote(ns, nr.at[plane_slot[k]], n_send.at[k], n_recv.at[plane_slot[k]], plane_peer[k - 1]).wait_recv()
        for cp in plane_norm:
            cp.wait_send()
        ns[...] = ((nr[0] + nr[1]) + (nr[2] + nr[3])) + ((nr[4] + nr[5]) + (nr[6] + nr[7]))
        z_norm = [remote(ns, nr.at[8 + z], n_send.at[7 + k], n_recv.at[8 + z], z_peer[k - 1]) for k in HOPS]
        for cp in z_norm:
            cp.start()
        nr[8 + z] = ns[...]
        for k in HOPS:
            zz = (z + k) % 4
            remote(ns, nr.at[8 + zz], n_send.at[7 + k], n_recv.at[8 + zz], z_peer[k - 1]).wait_recv()
        for cp in z_norm:
            cp.wait_send()
    total = (nr[8] + nr[9]) + (nr[10] + nr[11])
    norms = jnp.sqrt(jnp.sum(total, axis=1, keepdims=True))

    def gathered_q(u):
        if colour_of(u) == 2:
            return full.at[z, y, x, c, rows_of(u), :]
        return full.at[:, y, x, c, rows_of(u), :]

    def gathered_p(u):
        if colour_of(u) == 0:
            return full.at[:, :, x, c, rows_of(u), :]
        if colour_of(u) == 2:
            return full.at[z, :, x, c, rows_of(u), :]
        return full.at[:, y, :, c, rows_of(u), :]

    def gathered_c(u):
        return full.at[:, :, :, c, rows_of(u), :]

    def gather_z(u, k):
        src = rx.at[0, 0, 0, rows_of(u), :]
        dst = full.at[z, y, x, c, rows_of(u), :]
        if colour_of(u) == 2:
            src = dst = full.at[z, :, :, c, rows_of(u), :]
        return remote(src, dst, gz_send.at[u, k - 1], gz_recv.at[u, k - 1], z_peer[k - 1])

    gz = [[gather_z(u, k) for k in HOPS] for u in units]
    gq = [remote(gathered_q(u), gathered_q(u), gq_send.at[u], gq_recv.at[u], y_peer if colour_of(u) == 2 else q_peer(u)) for u in units]
    gp = [remote(gathered_p(u), gathered_p(u), gp_send.at[u], gp_recv.at[u], x_peer if colour_of(u) == 2 else p_peer(u)) for u in units]
    gc = [remote(gathered_c(u), gathered_c(u), gc_send.at[u], gc_recv.at[u], core_peer) for u in units]

    def weight_step(u):
        t = tensor(u)
        valid = valid_of(u)
        scale = LEARN_RATE * (norms[2 * t:2 * t + 1] / norms[2 * t + 1:2 * t + 2])

        def tile(r, n):
            rows = pl.ds(base(u) + r, n)
            w = state[t][:, flat_rows(u, r, n)].reshape(n, LANES)
            nw = w - scale * rz[0, rows, :]
            rz[1, rows, :] = nw
            rx[0, 0, 0, rows, :] = nw.astype(BF16)

        def body(i, carry):
            tile(pl.multiple_of(i * TILE, SUB), TILE)
            return carry

        lax.fori_loop(0, valid // TILE, body, 0)
        if valid % TILE:
            tile(valid - valid % TILE, valid % TILE)
        own_copy[u].start()
        out_w[u].start()
        if colour_of(u) == 2:
            own_copy[u].wait()
            gq[u].start()
        else:
            for cp in gz[u]:
                cp.start()

    def third_gather_z(u):
        with jax.named_scope(f"wait_third_gx#u={u}"):
            gp[u].wait_recv()
        for cp in gz[u]:
            cp.start()

    def third_gather_core(u):
        with jax.named_scope(f"wait_third_gz#u={u}"):
            for cp in gz[u]:
                cp.wait_recv()
        gc[u].start()

    order = list(range(n_steps))[::-1]
    for u in pair(order[0]):
        weight_step(u)
    for u in third:
        weight_step(u)
    for u in pair(order[1]):
        weight_step(u)
    for i in range(n_steps + 3):
        if i < n_steps:
            for u in pair(order[i]):
                own_copy[u].wait()
                with jax.named_scope(f"wait_gz#u={u}"):
                    for cp in gz[u]:
                        cp.wait_recv()
                gq[u].start()
        if i == 0:
            for u in third:
                gq[u].wait_recv()
                gp[u].start()
        if i + 2 < n_steps:
            for u in pair(order[i + 2]):
                weight_step(u)
        if i == 3:
            third_gather_z(third[0])
        if i == n_steps - 3:
            third_gather_z(third[1])
        if 0 <= i - 1 < n_steps:
            for u in pair(order[i - 1]):
                with jax.named_scope(f"wait_gq#u={u}"):
                    gq[u].wait_recv()
                gp[u].start()
        if i == n_steps - 1:
            third_gather_core(third[0])
        if 0 <= i - 2 < n_steps:
            for u in pair(order[i - 2]):
                with jax.named_scope(f"wait_gp#u={u}"):
                    gp[u].wait_recv()
                gc[u].start()
        if i == n_steps + 1:
            third_gather_core(third[1])
        if 0 <= i - 3 < n_steps:
            for u in pair(order[i - 3]):
                with jax.named_scope(f"wait_gc#u={u}"):
                    gc[u].wait_recv()
    for u in third:
        gc[u].wait_recv()

    for u in pair_units:
        if u >= n_pair - 4:
            p_copy[u].wait_send()
        if u >= n_pair - 2:
            c_copy[u].wait_send()
        q_copy[u].wait_send()
        for cp in z_copy[u]:
            cp.wait_send()
    for u in third:
        for cp in third_copy[u][0] + list(third_copy[u][1:]):
            cp.wait_send()
    for u in units:
        for cp in gz[u]:
            cp.wait_send()
        gq[u].wait_send()
        gp[u].wait_send()
        gc[u].wait_send()
        out_m[u].wait()
        out_v[u].wait()
        out_w[u].wait()


def comm(grads, state):
    n_units = len(UNITS)
    any_spec = pl.BlockSpec(memory_space=pl.ANY)
    dma = pltpu.SemaphoreType.DMA
    return pl.pallas_call(
        comm_kernel,
        in_specs=[any_spec] * 16,
        out_specs=[any_spec] * 4,
        out_shape=[jax.ShapeDtypeStruct((4, 2, 2, 2, TOTAL, LANES), BF16)] + [jax.ShapeDtypeStruct((TOTAL, LANES), F32)] * 3,
        scratch_shapes=[pltpu.VMEM((1, r * LANES), F32) for r in ROWS] * 3
        + [
            pltpu.VMEM((4, 2, 2, TOTAL, LANES), BF16),
            pltpu.VMEM((4, 2, TOTAL, LANES), F32),
            pltpu.VMEM((4, TOTAL, LANES), F32),
            pltpu.VMEM((3, TOTAL, LANES), F32),
            pltpu.VMEM((2, 4, 2, MAX_ROWS, LANES), F32),
            pltpu.VMEM((2, 4, 2, 2, MAX_ROWS, LANES), BF16),
            pltpu.VMEM((2, 2, 4, 2, 2, MAX_ROWS, LANES), BF16),
            pltpu.VMEM((2, 4, 2, 2, 1, MAX_ROWS * LANES), BF16),
            pltpu.VMEM((2, 2, 2, 2, MAX_ROWS, LANES), BF16),
            pltpu.VMEM((2, 2, 2, MAX_ROWS, LANES), F32),
            pltpu.VMEM((2, 4, 2, 2, 2, MAX_ROWS, LANES), BF16),
            pltpu.VMEM((8, LANES), F32),
            pltpu.VMEM((12, 8, LANES), F32),
            dma((12,)), dma((2,)),
            dma((n_units,)), dma((n_units,)), dma((n_units,)), dma((n_units,)), dma((n_units,)), dma((n_units,)),
            dma((n_units, 3)), dma((n_units, 3)), dma((11,)), dma((12,)), dma((3, n_units)), dma((n_units,)),
            dma((n_units, 3)), dma((n_units, 3)), dma((n_units,)), dma((n_units,)), dma((n_units,)), dma((n_units,)),
            dma((n_units,)), dma((n_units,)),
        ],
        compiler_params=pltpu.CompilerParams(collective_id=0, has_side_effects=True, vmem_limit_bytes=64 * 1024 * 1024 - 128 * 1024),
        name="lamb_comm",
    )(*grads, *state)


def solution(mesh):
    grad_spec = P("data", None, None)
    shard_spec = P(None, "data")
    full_spec = P(None, None)

    def device_step(*blocks):
        grads = [blocks[4 * t].reshape(4, 2, 2, 2, 1, -1) for t in range(4)]
        state = [blocks[4 * t + s] for s in (1, 2, 3) for t in range(4)]
        full, w, m, v = comm(grads, state)
        outs = unpack(full.reshape(32, TOTAL, LANES), w, m, v)
        results = []
        for t in range(4):
            results.extend((outs[t], outs[4 + t], outs[8 + t], outs[12 + t]))
        return tuple(results)

    return jax.shard_map(device_step, mesh=mesh, in_specs=(grad_spec, shard_spec, shard_spec, shard_spec) * 4, out_specs=(full_spec, shard_spec, shard_spec, shard_spec) * 4, check_vma=False)
```

```python
import functools

import jax
import jax.numpy as jnp
from jax import lax
from jax.experimental import pallas as pl
from jax.experimental.pallas import tpu as pltpu
from jax.sharding import PartitionSpec as P

STEP = 10
LEARN_RATE = 0.1
BETA_ONE = 0.9
BETA_TWO = 0.999
EPSILON = 1e-6
WEIGHT_DECAY = 0.01

LANES = 128
SUB = 16
ROWS = (867, 289, 1156, 1156)
PADDED = (880, 304, 1168, 1168)
STARTS = (0, 880, 1184, 2352)
TOTAL = 3520
PLAN = (
    (3, ((3, 4), (6, 5), (14, 14))),
    (2, ((8, 12), (13, 14), (12, 14))),
    (0, ((8, 10), (8, 6), (7, 7), (5, 4))),
    (1, ((3, 4), (3, 3), (3, 3))),
)
THIRD_ROWS = (13, 14)
THIRD_CORE = (3, 6)
THIRD_X = (9, 11)
THIRD_Y = (11, 13)
GATHER_Z = (8, 11)
GATHER_CORE = (11, 14)


def plan_units():
    units, third = [], []
    for t, pairs in PLAN:
        first = 0
        for rows_pair in pairs:
            for colour, rows in enumerate(rows_pair):
                units.append((t, first, rows * SUB, colour))
                first += rows * SUB
        if not third:
            for rows in THIRD_ROWS:
                third.append((t, first, rows * SUB, len(rows_pair)))
                first += rows * SUB
    return tuple(units), tuple(third)


PAIRED, THIRD = plan_units()
UNITS = PAIRED + THIRD
MAX_ROWS = 224
LAG = 4
TILE = 48
SHARDS = 2
HOPS = (1, 2, 3)
BOTH = (0, 1)
MESH = pl.DeviceIdType.MESH
F32 = jnp.float32
BF16 = jnp.bfloat16


def flat(dense, t):
    return dense.reshape(-1)[:ROWS[t] * LANES]


def unpack_kernel(full, w, m, v, *outs):
    spans = [pl.ds(STARTS[t], (ROWS[t] + SUB - 1) // SUB * SUB) for t in range(4)]
    for t, span in enumerate(spans):
        for j in range(SHARDS):
            outs[t][0, pl.ds(j * ROWS[t] * LANES, ROWS[t] * LANES)] = flat(full[j, span, :], t)

    @pl.when(pl.program_id(0) == 0)
    def _():
        for s, src in enumerate((w, m, v)):
            for t, span in enumerate(spans):
                outs[4 * s + 4 + t][0, :] = flat(src[span, :], t)


def unpack(full, w, m, v):
    state = pl.BlockSpec((TOTAL, LANES), lambda i: (0, 0))
    return pl.pallas_call(
        unpack_kernel,
        grid=(32 // SHARDS,),
        in_specs=[pl.BlockSpec((SHARDS, TOTAL, LANES), lambda i: (i, 0, 0)), state, state, state],
        out_specs=[pl.BlockSpec((1, SHARDS * r * LANES), lambda i: (0, i)) for r in ROWS]
        + [pl.BlockSpec((1, r * LANES), lambda i: (0, 0)) for r in ROWS] * 3,
        out_shape=[jax.ShapeDtypeStruct((1, 32 * r * LANES), BF16) for r in ROWS]
        + [jax.ShapeDtypeStruct((1, r * LANES), F32) for r in ROWS] * 3,
        name="unpack",
    )(full, w, m, v)


def comm_kernel(*refs):
    grads = refs[0:4]
    state_in = refs[4:16]
    full, new_w, new_m, new_v = refs[16:20]
    state = refs[20:32]
    weights, first_mom, second_mom = state[:4], state[4:8], state[8:]
    (rx, r2, r3, rz, t2, lx, ps, stage, rx3, t23, ps3, ns, nr, state_sem, stage_sem, p_send, p_recv, c_send, c_recv, q_send, q_recv,
     z_send, z_recv, n_send, n_recv, out_sem, own_sem, gz_send, gz_recv, gq_send, gq_recv, gp_send, gp_recv,
     gc_send, gc_recv) = refs[32:]

    me = lax.axis_index("data")
    c = me % 2
    x = (me // 2) % 2
    y = (me // 4) % 2
    z = me // 8

    def dev(zz, yy, xx, cc):
        return (((zz * 2 + yy) * 2 + xx) * 2 + cc,)

    def flip(value, by):
        return 1 - value if by else value

    core_peer = dev(z, y, x, 1 - c)
    x_peer = dev(z, y, 1 - x, c)
    y_peer = dev(z, 1 - y, x, c)
    z_peer = {k: dev((z + k) % 4, y, x, c) for k in HOPS}
    plane_peer = [dev(z, flip(y, k // 4), flip(x, k // 2 % 2), flip(c, k % 2)) for k in range(1, 8)]
    plane_slot = [flip(y, k // 4) * 4 + flip(x, k // 2 % 2) * 2 + flip(c, k % 2) for k in range(8)]

    barrier = pltpu.get_barrier_semaphore()
    for peer in plane_peer + list(z_peer.values()):
        pl.semaphore_signal(barrier, inc=1, device_id=peer, device_id_type=MESH)

    def remote(src, dst, ssem, rsem, peer):
        return pltpu.make_async_remote_copy(src_ref=src, dst_ref=dst, send_sem=ssem, recv_sem=rsem, device_id=peer, device_id_type=MESH)

    n_units = len(UNITS)
    n_pair = len(PAIRED)
    n_steps = n_pair // 2
    units = range(n_units)

    def sweep(u, body):
        def step(i, carry):
            body(pl.multiple_of(i * SUB, SUB))
            return carry

        lax.fori_loop(0, height(u) // SUB, step, 0)

    def tensor(u):
        return UNITS[u][0]

    def height(u):
        return UNITS[u][2]

    def colour_of(u):
        return UNITS[u][3]

    def base(u):
        return STARTS[tensor(u)] + UNITS[u][1]

    def rows_of(u):
        return pl.ds(base(u), height(u))

    def valid_of(u):
        return min(height(u), ROWS[tensor(u)] - UNITS[u][1])

    def p_peer(u):
        return x_peer if colour_of(u) == 0 else y_peer

    def q_peer(u):
        return y_peer if colour_of(u) == 0 else x_peer

    def q_me(u):
        return y if colour_of(u) == 0 else x

    third = range(n_pair, n_units)
    pair_units = range(n_pair)

    def stage_copy(u, mine):
        t, first, h, colour = UNITS[u]
        lanes = pl.ds(first * LANES, valid_of(u) * LANES)
        if colour == 0:
            src = grads[t].at[:, :, x if mine else 1 - x, :, :, lanes]
        else:
            src = grads[t].at[:, y if mine else 1 - y, :, :, :, lanes]
        return pltpu.make_async_copy(src, stage.at[colour, :, :, :, :, pl.ds(0, valid_of(u) * LANES)], stage_sem.at[colour])

    def pack(u, store):
        h, colour = (height(u), colour_of(u))
        valid = valid_of(u)

        def body(j, carry):
            for cc in BOTH:
                dense = stage[colour, j // 2, j % 2, cc, :, pl.ds(0, valid * LANES)].reshape(valid, LANES)
                if valid < h:
                    dense = jnp.concatenate([dense, jnp.zeros((h - valid, LANES), BF16)], axis=0)
                store(j // 2, j % 2, cc, dense)
            return carry

        lax.fori_loop(0, 8, body, 0)

    def pack_send(u):
        h, colour = (height(u), colour_of(u))

        def store(zz, qq, cc, dense):
            ps[colour, (u // 2) % 2, zz, qq, cc, pl.ds(0, h), :] = dense

        pack(u, store)

    def pack_own(u):
        h, colour = (height(u), colour_of(u))

        def store(zz, qq, cc, dense):
            lx[colour, zz, qq, cc, pl.ds(0, h), :] = dense

        pack(u, store)

    p_copy = [remote(ps.at[u % 2, (u // 2) % 2, :, :, :, pl.ds(0, height(u)), :], rx.at[:, :, :, rows_of(u), :], p_send.at[u], p_recv.at[u], p_peer(u)) for u in pair_units]
    c_copy = [remote(t2.at[u % 2, :, :, pl.ds(0, height(u)), :], r2.at[:, :, rows_of(u), :], c_send.at[u], c_recv.at[u], core_peer) for u in pair_units]
    q_copy = [remote(r2.at[:, 1 - q_me(u), rows_of(u), :], r3.at[:, rows_of(u), :], q_send.at[u], q_recv.at[u], q_peer(u)) for u in pair_units]
    z_copy = [[remote(r3.at[(z + k) % 4, rows_of(u), :], rz.at[k - 1, rows_of(u), :], z_send.at[u, k], z_recv.at[u, k], z_peer[k]) for k in HOPS] for u in pair_units]
    out_m = [pltpu.make_async_copy(r2.at[0, q_me(u), rows_of(u), :], new_m.at[rows_of(u), :], out_sem.at[0, u]) for u in units]
    out_v = [pltpu.make_async_copy(r2.at[1, q_me(u), rows_of(u), :], new_v.at[rows_of(u), :], out_sem.at[1, u]) for u in units]
    out_w = [pltpu.make_async_copy(rz.at[1, rows_of(u), :], new_w.at[rows_of(u), :], out_sem.at[2, u]) for u in units]
    own_copy = [pltpu.make_async_copy(rx.at[0, 0, 0, rows_of(u), :], full.at[z, y, x, c, rows_of(u), :], own_sem.at[u]) for u in units]
    state_copy = [pltpu.make_async_copy(state_in[i], state[i], state_sem.at[i]) for i in range(12)]

    def core_step(u):
        with jax.named_scope(f"wait_p#u={u}"):
            p_copy[u].wait_recv()
        if u >= 2:
            c_copy[u - 2].wait_send()

        def body(r):
            a = lx[u % 2, :, :, 1 - c, pl.ds(r, SUB), :].astype(F32)
            b = rx[:, :, 1 - c, pl.ds(base(u) + r, SUB), :].astype(F32)
            t2[u % 2, :, :, pl.ds(r, SUB), :] = a + b

        sweep(u, body)
        c_copy[u].start()

    def q_step(u):
        with jax.named_scope(f"wait_c#u={u}"):
            c_copy[u].wait_recv()

        def body(r):
            a = lx[u % 2, :, :, c, pl.ds(r, SUB), :].astype(F32)
            b = rx[:, :, c, pl.ds(base(u) + r, SUB), :].astype(F32)
            r2[:, :, pl.ds(base(u) + r, SUB), :] = r2[:, :, pl.ds(base(u) + r, SUB), :] + (a + b)

        sweep(u, body)
        q_copy[u].start()

    def z_step(u):
        with jax.named_scope(f"wait_q#u={u}"):
            q_copy[u].wait_recv()

        def body(r):
            near = pl.ds(base(u) + r, SUB)
            r3[:, near, :] = r3[:, near, :] + r2[:, q_me(u), near, :]

        sweep(u, body)
        for cp in z_copy[u]:
            cp.start()

    def third_parts(u):
        i, h = u - n_pair, height(u)
        rows = rows_of(u)
        short = pl.ds(0, h)
        landing = [rx.at[0:2, :, :, rows, :], rx.at[2:4, :, :, rows, :], rx3.at[i, :, :, :, short, :]]
        first = [remote(ps3.at[i, (z + k) % 4, :, :, :, short, :], landing[k - 1], z_send.at[u, k], z_recv.at[u, k], z_peer[k]) for k in HOPS]
        core = remote(t23.at[i, :, :, short, :], r2.at[0:2, :, rows, :], c_send.at[u], c_recv.at[u], core_peer)
        along_x = remote(r2.at[0:2, 1 - x, rows, :], r3.at[0:2, rows, :], q_send.at[u], q_recv.at[u], x_peer)
        along_y = remote(r3.at[1 - y, rows, :], rz.at[0, rows, :], p_send.at[u], p_recv.at[u], y_peer)
        return first, core, along_x, along_y

    third_copy = {u: third_parts(u) for u in third}

    def third_stage(u):
        t, first, h, colour = UNITS[u]
        valid = valid_of(u)
        lanes = pl.ds(first * LANES, valid * LANES)
        copies = [pltpu.make_async_copy(grads[t].at[:, :, :, cc, :, lanes], stage.at[cc, :, :, :, :, pl.ds(0, valid * LANES)], stage_sem.at[cc]) for cc in BOTH]
        for cp in copies:
            cp.start()
        for cp in copies:
            cp.wait()

        def body(j, carry):
            for xx in BOTH:
                for cc in BOTH:
                    dense = stage[cc, j // 2, j % 2, xx, :, pl.ds(0, valid * LANES)].reshape(valid, LANES)
                    if valid < h:
                        dense = jnp.concatenate([dense, jnp.zeros((h - valid, LANES), BF16)], axis=0)
                    ps3[u - n_pair, j // 2, j % 2, xx, cc, pl.ds(0, h), :] = dense
            return carry

        lax.fori_loop(0, 8, body, 0)
        for cp in third_copy[u][0]:
            cp.start()

    def third_sum(u, r, cc):
        i = u - n_pair
        near = pl.ds(base(u) + r, SUB)
        own = ps3[i, z, :, :, cc, pl.ds(r, SUB), :].astype(F32) + rx[0:2, :, cc, near, :].astype(F32)
        return own + (rx[2:4, :, cc, near, :].astype(F32) + rx3[i, :, :, cc, pl.ds(r, SUB), :].astype(F32))

    def third_core_step(u):
        with jax.named_scope(f"wait_third_z#u={u}"):
            for cp in third_copy[u][0]:
                cp.wait_recv()

        def body(r):
            t23[u - n_pair, :, :, pl.ds(r, SUB), :] = third_sum(u, r, 1 - c)

        sweep(u, body)
        third_copy[u][1].start()

    def third_x_step(u):
        third_copy[u][1].wait_recv()

        def body(r):
            near = pl.ds(base(u) + r, SUB)
            r2[0:2, :, near, :] = r2[0:2, :, near, :] + third_sum(u, r, c)

        sweep(u, body)
        third_copy[u][2].start()

    def third_y_step(u):
        with jax.named_scope(f"wait_third_x#u={u}"):
            third_copy[u][2].wait_recv()

        def body(r):
            near = pl.ds(base(u) + r, SUB)
            r3[0:2, near, :] = r3[0:2, near, :] + r2[0:2, x, near, :]

        sweep(u, body)
        third_copy[u][3].start()

    def flat_rows(u, r, n):
        start = (UNITS[u][1] + r) * LANES
        return pl.ds(start if isinstance(r, int) else pl.multiple_of(start, LANES), n * LANES)

    def lamb_step(u):
        t, first, h, colour = UNITS[u]
        with jax.named_scope(f"wait_z#u={u}"):
            if colour == 2:
                third_copy[u][3].wait_recv()
            else:
                for cp in z_copy[u]:
                    cp.wait_recv()
        if first == 0:
            for i in (t, 4 + t, 8 + t):
                state_copy[i].wait()
        valid = valid_of(u)
        q = q_me(u)

        def tile(r, n):
            rows = pl.ds(base(u) + r, n)
            flat = flat_rows(u, r, n)
            w = weights[t][:, flat].reshape(n, LANES)
            m = first_mom[t][:, flat].reshape(n, LANES)
            v = second_mom[t][:, flat].reshape(n, LANES)
            if colour == 2:
                g = (r3[y, rows, :] + rz[0, rows, :]) / 32.0
            else:
                g = (((r3[z, rows, :] + rz[0, rows, :]) + rz[1, rows, :]) + rz[2, rows, :]) / 32.0
            nm = BETA_ONE * m + (1.0 - BETA_ONE) * g
            nv = BETA_TWO * v + (1.0 - BETA_TWO) * g * g
            u_dir = (nm / (1.0 - BETA_ONE ** STEP)) / (jnp.sqrt(nv / (1.0 - BETA_TWO ** STEP)) + EPSILON) + WEIGHT_DECAY * w
            r2[0, q, rows, :] = nm
            r2[1, q, rows, :] = nv
            rz[0, rows, :] = u_dir
            return w * w, u_dir * u_dir

        def body(i, carry):
            ww, uu = tile(pl.multiple_of(i * TILE, SUB), TILE)
            return (carry[0] + jnp.sum(ww.reshape(TILE // 8, 8, LANES), axis=0), carry[1] + jnp.sum(uu.reshape(TILE // 8, 8, LANES), axis=0))

        zero = jnp.zeros((8, LANES), F32)
        acc_w, acc_u = lax.fori_loop(0, valid // TILE, body, (zero, zero))
        sum_w = jnp.sum(acc_w, axis=0, keepdims=True)
        sum_u = jnp.sum(acc_u, axis=0, keepdims=True)
        if valid % TILE:
            ww, uu = tile(valid - valid % TILE, valid % TILE)
            sum_w = sum_w + jnp.sum(ww, axis=0, keepdims=True)
            sum_u = sum_u + jnp.sum(uu, axis=0, keepdims=True)
        ns[pl.ds(2 * t, 1), :] = ns[pl.ds(2 * t, 1), :] + sum_w
        ns[pl.ds(2 * t + 1, 1), :] = ns[pl.ds(2 * t + 1, 1), :] + sum_u
        out_m[u].start()
        out_v[u].start()

    def pair(s):
        return (2 * s, 2 * s + 1)

    for s in BOTH:
        for u in pair(s):
            stage_copy(u, False).start()
        if s == 0:
            for cp in state_copy:
                cp.start()
            ns[...] = jnp.zeros_like(ns)
        for u in pair(s):
            stage_copy(u, False).wait()
            pack_send(u)
        if s == 0:
            pl.semaphore_wait(barrier, 10)
        for u in pair(s):
            p_copy[u].start()
        third_stage(third[s])
    for u in pair(0):
        stage_copy(u, True).start()
    for u in pair(0):
        stage_copy(u, True).wait()
        pack_own(u)
        stage_copy(u + 4, False).start()

    for s in range(n_steps + LAG):
        if s < n_steps:
            for u in pair(s):
                core_step(u)
            for u in pair(s):
                q_step(u)
            for at, step in ((THIRD_CORE, third_core_step), (THIRD_X, third_x_step), (THIRD_Y, third_y_step)):
                for i, u in enumerate(third):
                    if at[i] == s:
                        step(u)
            if s + 2 < n_steps:
                for u in pair(s + 2):
                    stage_copy(u, False).wait()
                    p_copy[u - 4].wait_send()
                    pack_send(u)
                    p_copy[u].start()
            if s + 1 < n_steps:
                for u in pair(s + 1):
                    stage_copy(u, True).start()
                for u in pair(s + 1):
                    stage_copy(u, True).wait()
                    pack_own(u)
                    if s + 3 < n_steps:
                        stage_copy(u + 4, False).start()
        if 0 <= s - 1 < n_steps:
            for u in pair(s - 1):
                z_step(u)
        if s >= n_steps:
            for i, u in enumerate(third):
                if THIRD_Y[i] == s:
                    third_y_step(u)
        if 0 <= s - LAG < n_steps:
            for u in pair(s - LAG):
                lamb_step(u)
    for u in third:
        lamb_step(u)

    with jax.named_scope("norms"):
        plane_norm = [remote(ns, nr.at[plane_slot[0]], n_send.at[k], n_recv.at[plane_slot[0]], plane_peer[k - 1]) for k in range(1, 8)]
        for cp in plane_norm:
            cp.start()
        nr[plane_slot[0]] = ns[...]
        for k in range(1, 8):
            remote(ns, nr.at[plane_slot[k]], n_send.at[k], n_recv.at[plane_slot[k]], plane_peer[k - 1]).wait_recv()
        for cp in plane_norm:
            cp.wait_send()
        ns[...] = jnp.sum(nr[0:8], axis=0)
        z_norm = [remote(ns, nr.at[8 + z], n_send.at[7 + k], n_recv.at[8 + z], z_peer[k]) for k in HOPS]
        for cp in z_norm:
            cp.start()
        nr[8 + z] = ns[...]
        for k in HOPS:
            zz = (z + k) % 4
            remote(ns, nr.at[8 + zz], n_send.at[7 + k], n_recv.at[8 + zz], z_peer[k]).wait_recv()
        for cp in z_norm:
            cp.wait_send()
    total = jnp.sum(nr[8:12], axis=0)
    norms = jnp.sqrt(jnp.sum(total, axis=1, keepdims=True))

    def gathered_q(u):
        if colour_of(u) == 2:
            return full.at[z, y, x, c, rows_of(u), :]
        return full.at[:, y, x, c, rows_of(u), :]

    def gathered_p(u):
        if colour_of(u) == 0:
            return full.at[:, :, x, c, rows_of(u), :]
        if colour_of(u) == 2:
            return full.at[z, :, x, c, rows_of(u), :]
        return full.at[:, y, :, c, rows_of(u), :]

    def gathered_c(u):
        return full.at[:, :, :, c, rows_of(u), :]

    def gather_z(u, k):
        src = rx.at[0, 0, 0, rows_of(u), :]
        dst = full.at[z, y, x, c, rows_of(u), :]
        if colour_of(u) == 2:
            src = dst = full.at[z, :, :, c, rows_of(u), :]
        return remote(src, dst, gz_send.at[u, k], gz_recv.at[u, k], z_peer[k])

    gz = [[gather_z(u, k) for k in HOPS] for u in units]
    gq = [remote(gathered_q(u), gathered_q(u), gq_send.at[u], gq_recv.at[u], y_peer if colour_of(u) == 2 else q_peer(u)) for u in units]
    gp = [remote(gathered_p(u), gathered_p(u), gp_send.at[u], gp_recv.at[u], x_peer if colour_of(u) == 2 else p_peer(u)) for u in units]
    gc = [remote(gathered_c(u), gathered_c(u), gc_send.at[u], gc_recv.at[u], core_peer) for u in units]

    def weight_step(u):
        t = tensor(u)
        valid = valid_of(u)
        scale = LEARN_RATE * (norms[2 * t:2 * t + 1] / norms[2 * t + 1:2 * t + 2])

        def tile(r, n):
            rows = pl.ds(base(u) + r, n)
            w = weights[t][:, flat_rows(u, r, n)].reshape(n, LANES)
            nw = w - scale * rz[0, rows, :]
            rz[1, rows, :] = nw
            rx[0, 0, 0, rows, :] = nw.astype(BF16)

        def body(i, carry):
            tile(pl.multiple_of(i * TILE, SUB), TILE)
            return carry

        lax.fori_loop(0, valid // TILE, body, 0)
        if valid % TILE:
            tile(valid - valid % TILE, valid % TILE)
        own_copy[u].start()
        out_w[u].start()
        if colour_of(u) == 2:
            own_copy[u].wait()
            gq[u].start()
        else:
            for cp in gz[u]:
                cp.start()

    def third_gather_z(u):
        with jax.named_scope(f"wait_third_gx#u={u}"):
            gp[u].wait_recv()
        for cp in gz[u]:
            cp.start()

    def third_gather_core(u):
        with jax.named_scope(f"wait_third_gz#u={u}"):
            for cp in gz[u]:
                cp.wait_recv()
        gc[u].start()

    order = list(range(n_steps))[::-1]
    for u in pair(order[0]):
        weight_step(u)
    for u in third:
        weight_step(u)
    for u in pair(order[1]):
        weight_step(u)
    for i in range(n_steps + 3):
        if i < n_steps:
            for u in pair(order[i]):
                own_copy[u].wait()
                with jax.named_scope(f"wait_gz#u={u}"):
                    for cp in gz[u]:
                        cp.wait_recv()
                gq[u].start()
        if i == 0:
            for u in third:
                gq[u].wait_recv()
                gp[u].start()
        if i + 2 < n_steps:
            for u in pair(order[i + 2]):
                weight_step(u)
        for j, u in enumerate(third):
            if GATHER_Z[j] == i:
                third_gather_z(u)
        if 0 <= i - 1 < n_steps:
            for u in pair(order[i - 1]):
                with jax.named_scope(f"wait_gq#u={u}"):
                    gq[u].wait_recv()
                gp[u].start()
        for j, u in enumerate(third):
            if GATHER_CORE[j] == i:
                third_gather_core(u)
        if 0 <= i - 2 < n_steps:
            for u in pair(order[i - 2]):
                with jax.named_scope(f"wait_gp#u={u}"):
                    gp[u].wait_recv()
                gc[u].start()
        if 0 <= i - 3 < n_steps:
            for u in pair(order[i - 3]):
                with jax.named_scope(f"wait_gc#u={u}"):
                    gc[u].wait_recv()
    for u in third:
        gc[u].wait_recv()

    for u in pair_units:
        if u >= n_pair - 4:
            p_copy[u].wait_send()
        if u >= n_pair - 2:
            c_copy[u].wait_send()
        q_copy[u].wait_send()
        for cp in z_copy[u]:
            cp.wait_send()
    for u in third:
        for cp in third_copy[u][0] + list(third_copy[u][1:]):
            cp.wait_send()
    for u in units:
        for cp in gz[u]:
            cp.wait_send()
        gq[u].wait_send()
        gp[u].wait_send()
        gc[u].wait_send()
        out_m[u].wait()
        out_v[u].wait()
        out_w[u].wait()


def comm(grads, state):
    n_units = len(UNITS)
    any_spec = pl.BlockSpec(memory_space=pl.ANY)
    dma = pltpu.SemaphoreType.DMA
    return pl.pallas_call(
        comm_kernel,
        in_specs=[any_spec] * 16,
        out_specs=[any_spec] * 4,
        out_shape=[jax.ShapeDtypeStruct((4, 2, 2, 2, TOTAL, LANES), BF16)] + [jax.ShapeDtypeStruct((TOTAL, LANES), F32)] * 3,
        scratch_shapes=[pltpu.VMEM((1, r * LANES), F32) for r in ROWS] * 3
        + [
            pltpu.VMEM((4, 2, 2, TOTAL, LANES), BF16),
            pltpu.VMEM((4, 2, TOTAL, LANES), F32),
            pltpu.VMEM((4, TOTAL, LANES), F32),
            pltpu.VMEM((3, TOTAL, LANES), F32),
            pltpu.VMEM((2, 4, 2, MAX_ROWS, LANES), F32),
            pltpu.VMEM((2, 4, 2, 2, MAX_ROWS, LANES), BF16),
            pltpu.VMEM((2, 2, 4, 2, 2, MAX_ROWS, LANES), BF16),
            pltpu.VMEM((2, 4, 2, 2, 1, MAX_ROWS * LANES), BF16),
            pltpu.VMEM((2, 2, 2, 2, MAX_ROWS, LANES), BF16),
            pltpu.VMEM((2, 2, 2, MAX_ROWS, LANES), F32),
            pltpu.VMEM((2, 4, 2, 2, 2, MAX_ROWS, LANES), BF16),
            pltpu.VMEM((8, LANES), F32),
            pltpu.VMEM((12, 8, LANES), F32),
            dma((12,)), dma((2,)),
            dma((n_units,)), dma((n_units,)), dma((n_units,)), dma((n_units,)), dma((n_units,)), dma((n_units,)),
            dma((n_units, 4)), dma((n_units, 4)), dma((11,)), dma((12,)), dma((3, n_units)), dma((n_units,)),
            dma((n_units, 4)), dma((n_units, 4)), dma((n_units,)), dma((n_units,)), dma((n_units,)), dma((n_units,)),
            dma((n_units,)), dma((n_units,)),
        ],
        compiler_params=pltpu.CompilerParams(collective_id=0, has_side_effects=True, vmem_limit_bytes=64 * 1024 * 1024 - 128 * 1024),
        name="lamb_comm",
    )(*grads, *state)


def solution(mesh):
    grad_spec = P("data", None, None)
    shard_spec = P(None, "data")
    full_spec = P(None, None)

    def device_step(*blocks):
        grads = [blocks[4 * t].reshape(4, 2, 2, 2, 1, -1) for t in range(4)]
        state = [blocks[4 * t + s] for s in (1, 2, 3) for t in range(4)]
        full, w, m, v = comm(grads, state)
        outs = unpack(full.reshape(32, TOTAL, LANES), w, m, v)
        results = []
        for t in range(4):
            results.extend((outs[t], outs[4 + t], outs[8 + t], outs[12 + t]))
        return tuple(results)

    return jax.shard_map(device_step, mesh=mesh, in_specs=(grad_spec, shard_spec, shard_spec, shard_spec) * 4, out_specs=(full_spec, shard_spec, shard_spec, shard_spec) * 4, check_vma=False)
```

```python
import functools

import jax
import jax.numpy as jnp
from jax import lax
from jax.experimental import pallas as pl
from jax.experimental.pallas import tpu as pltpu
from jax.sharding import PartitionSpec as P

STEP = 10
LEARN_RATE = 0.1
BETA_ONE = 0.9
BETA_TWO = 0.999
EPSILON = 1e-6
WEIGHT_DECAY = 0.01

LANES = 128
SUB = 16
ROWS = (867, 289, 1156, 1156)
PADDED = (880, 304, 1168, 1168)
STARTS = (0, 880, 1184, 2352)
TOTAL = 3520
PLAN = (
    (3, ((3, 4), (6, 5), (14, 14))),
    (2, ((8, 12), (13, 14), (12, 14))),
    (0, ((8, 10), (8, 6), (7, 7), (5, 4))),
    (1, ((3, 4), (3, 3), (3, 3))),
)
THIRD_ROWS = (13, 14)
THIRD_CORE = (3, 6)
THIRD_X = (9, 11)
THIRD_Y = (11, 13)
GATHER_Z = (8, 11)
GATHER_CORE = (11, 14)


def plan_units():
    units, third = [], []
    for t, pairs in PLAN:
        first = 0
        for rows_pair in pairs:
            for colour, rows in enumerate(rows_pair):
                units.append((t, first, rows * SUB, colour))
                first += rows * SUB
        if not third:
            for rows in THIRD_ROWS:
                third.append((t, first, rows * SUB, len(rows_pair)))
                first += rows * SUB
    return tuple(units), tuple(third)


PAIRED, THIRD = plan_units()
UNITS = PAIRED + THIRD
MAX_ROWS = 224
LAG = 4
TILE = 48
SHARDS = 4
HOPS = (1, 2, 3)
BOTH = (0, 1)
MESH = pl.DeviceIdType.MESH
F32 = jnp.float32
BF16 = jnp.bfloat16


def flat(dense, t):
    return dense.reshape(-1)[:ROWS[t] * LANES]


def unpack_kernel(full, w, m, v, *outs):
    spans = [pl.ds(STARTS[t], (ROWS[t] + SUB - 1) // SUB * SUB) for t in range(4)]
    for t, span in enumerate(spans):
        for j in range(SHARDS):
            outs[t][0, pl.ds(j * ROWS[t] * LANES, ROWS[t] * LANES)] = flat(full[j, span, :], t)

    @pl.when(pl.program_id(0) == 0)
    def _():
        for s, src in enumerate((w, m, v)):
            for t, span in enumerate(spans):
                outs[4 * s + 4 + t][0, :] = flat(src[span, :], t)


def unpack(full, w, m, v):
    state = pl.BlockSpec((TOTAL, LANES), lambda i: (0, 0))
    return pl.pallas_call(
        unpack_kernel,
        grid=(32 // SHARDS,),
        in_specs=[pl.BlockSpec((SHARDS, TOTAL, LANES), lambda i: (i, 0, 0)), state, state, state],
        out_specs=[pl.BlockSpec((1, SHARDS * r * LANES), lambda i: (0, i)) for r in ROWS]
        + [pl.BlockSpec((1, r * LANES), lambda i: (0, 0)) for r in ROWS] * 3,
        out_shape=[jax.ShapeDtypeStruct((1, 32 * r * LANES), BF16) for r in ROWS]
        + [jax.ShapeDtypeStruct((1, r * LANES), F32) for r in ROWS] * 3,
        name="unpack",
    )(full, w, m, v)


def comm_kernel(*refs):
    grads = refs[0:4]
    state_in = refs[4:16]
    full, new_w, new_m, new_v = refs[16:20]
    state = refs[20:32]
    weights, first_mom, second_mom = state[:4], state[4:8], state[8:]
    (rx, r2, r3, rz, t2, lx, ps, stage, rx3, t23, ps3, ns, nr, state_sem, stage_sem, p_send, p_recv, c_send, c_recv, q_send, q_recv,
     z_send, z_recv, n_send, n_recv, out_sem, own_sem, gz_send, gz_recv, gq_send, gq_recv, gp_send, gp_recv,
     gc_send, gc_recv) = refs[32:]

    me = lax.axis_index("data")
    c = me % 2
    x = (me // 2) % 2
    y = (me // 4) % 2
    z = me // 8

    def dev(zz, yy, xx, cc):
        return (((zz * 2 + yy) * 2 + xx) * 2 + cc,)

    def flip(value, by):
        return 1 - value if by else value

    core_peer = dev(z, y, x, 1 - c)
    x_peer = dev(z, y, 1 - x, c)
    y_peer = dev(z, 1 - y, x, c)
    z_peer = {k: dev((z + k) % 4, y, x, c) for k in HOPS}
    plane_peer = [dev(z, flip(y, k // 4), flip(x, k // 2 % 2), flip(c, k % 2)) for k in range(1, 8)]
    plane_slot = [flip(y, k // 4) * 4 + flip(x, k // 2 % 2) * 2 + flip(c, k % 2) for k in range(8)]

    barrier = pltpu.get_barrier_semaphore()
    for peer in plane_peer + list(z_peer.values()):
        pl.semaphore_signal(barrier, inc=1, device_id=peer, device_id_type=MESH)

    def remote(src, dst, ssem, rsem, peer):
        return pltpu.make_async_remote_copy(src_ref=src, dst_ref=dst, send_sem=ssem, recv_sem=rsem, device_id=peer, device_id_type=MESH)

    n_units = len(UNITS)
    n_pair = len(PAIRED)
    n_steps = n_pair // 2
    units = range(n_units)

    def sweep(u, body):
        def step(i, carry):
            body(pl.multiple_of(i * SUB, SUB))
            return carry

        lax.fori_loop(0, height(u) // SUB, step, 0)

    def tensor(u):
        return UNITS[u][0]

    def height(u):
        return UNITS[u][2]

    def colour_of(u):
        return UNITS[u][3]

    def base(u):
        return STARTS[tensor(u)] + UNITS[u][1]

    def rows_of(u):
        return pl.ds(base(u), height(u))

    def valid_of(u):
        return min(height(u), ROWS[tensor(u)] - UNITS[u][1])

    def p_peer(u):
        return x_peer if colour_of(u) == 0 else y_peer

    def q_peer(u):
        return y_peer if colour_of(u) == 0 else x_peer

    def q_me(u):
        return y if colour_of(u) == 0 else x

    third = range(n_pair, n_units)
    pair_units = range(n_pair)

    def stage_copy(u, mine):
        t, first, h, colour = UNITS[u]
        lanes = pl.ds(first * LANES, valid_of(u) * LANES)
        if colour == 0:
            src = grads[t].at[:, :, x if mine else 1 - x, :, :, lanes]
        else:
            src = grads[t].at[:, y if mine else 1 - y, :, :, :, lanes]
        return pltpu.make_async_copy(src, stage.at[colour, :, :, :, :, pl.ds(0, valid_of(u) * LANES)], stage_sem.at[colour])

    def pack(u, store):
        h, colour = (height(u), colour_of(u))
        valid = valid_of(u)

        def body(j, carry):
            for cc in BOTH:
                dense = stage[colour, j // 2, j % 2, cc, :, pl.ds(0, valid * LANES)].reshape(valid, LANES)
                if valid < h:
                    dense = jnp.concatenate([dense, jnp.zeros((h - valid, LANES), BF16)], axis=0)
                store(j // 2, j % 2, cc, dense)
            return carry

        lax.fori_loop(0, 8, body, 0)

    def pack_send(u):
        h, colour = (height(u), colour_of(u))

        def store(zz, qq, cc, dense):
            ps[colour, (u // 2) % 2, zz, qq, cc, pl.ds(0, h), :] = dense

        pack(u, store)

    def pack_own(u):
        h, colour = (height(u), colour_of(u))

        def store(zz, qq, cc, dense):
            lx[colour, zz, qq, cc, pl.ds(0, h), :] = dense

        pack(u, store)

    p_copy = [remote(ps.at[u % 2, (u // 2) % 2, :, :, :, pl.ds(0, height(u)), :], rx.at[:, :, :, rows_of(u), :], p_send.at[u], p_recv.at[u], p_peer(u)) for u in pair_units]
    c_copy = [remote(t2.at[u % 2, :, :, pl.ds(0, height(u)), :], r2.at[:, :, rows_of(u), :], c_send.at[u], c_recv.at[u], core_peer) for u in pair_units]
    q_copy = [remote(r2.at[:, 1 - q_me(u), rows_of(u), :], r3.at[:, rows_of(u), :], q_send.at[u], q_recv.at[u], q_peer(u)) for u in pair_units]
    z_copy = [[remote(r3.at[(z + k) % 4, rows_of(u), :], rz.at[k - 1, rows_of(u), :], z_send.at[u, k], z_recv.at[u, k], z_peer[k]) for k in HOPS] for u in pair_units]
    out_m = [pltpu.make_async_copy(r2.at[0, q_me(u), rows_of(u), :], new_m.at[rows_of(u), :], out_sem.at[0, u]) for u in units]
    out_v = [pltpu.make_async_copy(r2.at[1, q_me(u), rows_of(u), :], new_v.at[rows_of(u), :], out_sem.at[1, u]) for u in units]
    out_w = [pltpu.make_async_copy(rz.at[1, rows_of(u), :], new_w.at[rows_of(u), :], out_sem.at[2, u]) for u in units]
    own_copy = [pltpu.make_async_copy(rx.at[0, 0, 0, rows_of(u), :], full.at[z, y, x, c, rows_of(u), :], own_sem.at[u]) for u in units]
    state_copy = [pltpu.make_async_copy(state_in[i], state[i], state_sem.at[i]) for i in range(12)]

    def core_step(u):
        with jax.named_scope(f"wait_p#u={u}"):
            p_copy[u].wait_recv()
        if u >= 2:
            c_copy[u - 2].wait_send()

        def body(r):
            a = lx[u % 2, :, :, 1 - c, pl.ds(r, SUB), :].astype(F32)
            b = rx[:, :, 1 - c, pl.ds(base(u) + r, SUB), :].astype(F32)
            t2[u % 2, :, :, pl.ds(r, SUB), :] = a + b

        sweep(u, body)
        c_copy[u].start()

    def q_step(u):
        with jax.named_scope(f"wait_c#u={u}"):
            c_copy[u].wait_recv()

        def body(r):
            a = lx[u % 2, :, :, c, pl.ds(r, SUB), :].astype(F32)
            b = rx[:, :, c, pl.ds(base(u) + r, SUB), :].astype(F32)
            r2[:, :, pl.ds(base(u) + r, SUB), :] = r2[:, :, pl.ds(base(u) + r, SUB), :] + (a + b)

        sweep(u, body)
        q_copy[u].start()

    def z_step(u):
        with jax.named_scope(f"wait_q#u={u}"):
            q_copy[u].wait_recv()

        def body(r):
            near = pl.ds(base(u) + r, SUB)
            r3[:, near, :] = r3[:, near, :] + r2[:, q_me(u), near, :]

        sweep(u, body)
        for cp in z_copy[u]:
            cp.start()

    def third_parts(u):
        i, h = u - n_pair, height(u)
        rows = rows_of(u)
        short = pl.ds(0, h)
        landing = [rx.at[0:2, :, :, rows, :], rx.at[2:4, :, :, rows, :], rx3.at[i, :, :, :, short, :]]
        first = [remote(ps3.at[i, (z + k) % 4, :, :, :, short, :], landing[k - 1], z_send.at[u, k], z_recv.at[u, k], z_peer[k]) for k in HOPS]
        core = remote(t23.at[i, :, :, short, :], r2.at[0:2, :, rows, :], c_send.at[u], c_recv.at[u], core_peer)
        along_x = remote(r2.at[0:2, 1 - x, rows, :], r3.at[0:2, rows, :], q_send.at[u], q_recv.at[u], x_peer)
        along_y = remote(r3.at[1 - y, rows, :], rz.at[0, rows, :], p_send.at[u], p_recv.at[u], y_peer)
        return first, core, along_x, along_y

    third_copy = {u: third_parts(u) for u in third}

    def third_stage(u):
        t, first, h, colour = UNITS[u]
        valid = valid_of(u)
        lanes = pl.ds(first * LANES, valid * LANES)
        copies = [pltpu.make_async_copy(grads[t].at[:, :, :, cc, :, lanes], stage.at[cc, :, :, :, :, pl.ds(0, valid * LANES)], stage_sem.at[cc]) for cc in BOTH]
        for cp in copies:
            cp.start()
        for cp in copies:
            cp.wait()

        def body(j, carry):
            for xx in BOTH:
                for cc in BOTH:
                    dense = stage[cc, j // 2, j % 2, xx, :, pl.ds(0, valid * LANES)].reshape(valid, LANES)
                    if valid < h:
                        dense = jnp.concatenate([dense, jnp.zeros((h - valid, LANES), BF16)], axis=0)
                    ps3[u - n_pair, j // 2, j % 2, xx, cc, pl.ds(0, h), :] = dense
            return carry

        lax.fori_loop(0, 8, body, 0)
        for cp in third_copy[u][0]:
            cp.start()

    def third_sum(u, r, cc):
        i = u - n_pair
        near = pl.ds(base(u) + r, SUB)
        own = ps3[i, z, :, :, cc, pl.ds(r, SUB), :].astype(F32) + rx[0:2, :, cc, near, :].astype(F32)
        return own + (rx[2:4, :, cc, near, :].astype(F32) + rx3[i, :, :, cc, pl.ds(r, SUB), :].astype(F32))

    def third_core_step(u):
        with jax.named_scope(f"wait_third_z#u={u}"):
            for cp in third_copy[u][0]:
                cp.wait_recv()

        def body(r):
            t23[u - n_pair, :, :, pl.ds(r, SUB), :] = third_sum(u, r, 1 - c)

        sweep(u, body)
        third_copy[u][1].start()

    def third_x_step(u):
        third_copy[u][1].wait_recv()

        def body(r):
            near = pl.ds(base(u) + r, SUB)
            r2[0:2, :, near, :] = r2[0:2, :, near, :] + third_sum(u, r, c)

        sweep(u, body)
        third_copy[u][2].start()

    def third_y_step(u):
        with jax.named_scope(f"wait_third_x#u={u}"):
            third_copy[u][2].wait_recv()

        def body(r):
            near = pl.ds(base(u) + r, SUB)
            r3[0:2, near, :] = r3[0:2, near, :] + r2[0:2, x, near, :]

        sweep(u, body)
        third_copy[u][3].start()

    def flat_rows(u, r, n):
        start = (UNITS[u][1] + r) * LANES
        return pl.ds(start if isinstance(r, int) else pl.multiple_of(start, LANES), n * LANES)

    def lamb_step(u):
        t, first, h, colour = UNITS[u]
        with jax.named_scope(f"wait_z#u={u}"):
            if colour == 2:
                third_copy[u][3].wait_recv()
            else:
                for cp in z_copy[u]:
                    cp.wait_recv()
        if first == 0:
            for i in (t, 4 + t, 8 + t):
                state_copy[i].wait()
        valid = valid_of(u)
        q = q_me(u)

        def tile(r, n):
            rows = pl.ds(base(u) + r, n)
            flat = flat_rows(u, r, n)
            w = weights[t][:, flat].reshape(n, LANES)
            m = first_mom[t][:, flat].reshape(n, LANES)
            v = second_mom[t][:, flat].reshape(n, LANES)
            if colour == 2:
                g = (r3[y, rows, :] + rz[0, rows, :]) / 32.0
            else:
                g = (((r3[z, rows, :] + rz[0, rows, :]) + rz[1, rows, :]) + rz[2, rows, :]) / 32.0
            nm = BETA_ONE * m + (1.0 - BETA_ONE) * g
            nv = BETA_TWO * v + (1.0 - BETA_TWO) * g * g
            u_dir = (nm / (1.0 - BETA_ONE ** STEP)) / (jnp.sqrt(nv / (1.0 - BETA_TWO ** STEP)) + EPSILON) + WEIGHT_DECAY * w
            r2[0, q, rows, :] = nm
            r2[1, q, rows, :] = nv
            rz[0, rows, :] = u_dir
            return w * w, u_dir * u_dir

        def body(i, carry):
            ww, uu = tile(pl.multiple_of(i * TILE, SUB), TILE)
            return (carry[0] + jnp.sum(ww.reshape(TILE // 8, 8, LANES), axis=0), carry[1] + jnp.sum(uu.reshape(TILE // 8, 8, LANES), axis=0))

        zero = jnp.zeros((8, LANES), F32)
        acc_w, acc_u = lax.fori_loop(0, valid // TILE, body, (zero, zero))
        sum_w = jnp.sum(acc_w, axis=0, keepdims=True)
        sum_u = jnp.sum(acc_u, axis=0, keepdims=True)
        if valid % TILE:
            ww, uu = tile(valid - valid % TILE, valid % TILE)
            sum_w = sum_w + jnp.sum(ww, axis=0, keepdims=True)
            sum_u = sum_u + jnp.sum(uu, axis=0, keepdims=True)
        ns[pl.ds(2 * t, 1), :] = ns[pl.ds(2 * t, 1), :] + sum_w
        ns[pl.ds(2 * t + 1, 1), :] = ns[pl.ds(2 * t + 1, 1), :] + sum_u
        out_m[u].start()
        out_v[u].start()

    def pair(s):
        return (2 * s, 2 * s + 1)

    for s in BOTH:
        for u in pair(s):
            stage_copy(u, False).start()
        if s == 0:
            for cp in state_copy:
                cp.start()
            ns[...] = jnp.zeros_like(ns)
        for u in pair(s):
            stage_copy(u, False).wait()
            pack_send(u)
        if s == 0:
            pl.semaphore_wait(barrier, 10)
        for u in pair(s):
            p_copy[u].start()
        third_stage(third[s])
    for u in pair(0):
        stage_copy(u, True).start()
    for u in pair(0):
        stage_copy(u, True).wait()
        pack_own(u)
        stage_copy(u + 4, False).start()

    for s in range(n_steps + LAG):
        if s < n_steps:
            for u in pair(s):
                core_step(u)
            for u in pair(s):
                q_step(u)
            for at, step in ((THIRD_CORE, third_core_step), (THIRD_X, third_x_step), (THIRD_Y, third_y_step)):
                for i, u in enumerate(third):
                    if at[i] == s:
                        step(u)
            if s + 2 < n_steps:
                for u in pair(s + 2):
                    stage_copy(u, False).wait()
                    p_copy[u - 4].wait_send()
                    pack_send(u)
                    p_copy[u].start()
            if s + 1 < n_steps:
                for u in pair(s + 1):
                    stage_copy(u, True).start()
                for u in pair(s + 1):
                    stage_copy(u, True).wait()
                    pack_own(u)
                    if s + 3 < n_steps:
                        stage_copy(u + 4, False).start()
        if 0 <= s - 1 < n_steps:
            for u in pair(s - 1):
                z_step(u)
        if s >= n_steps:
            for i, u in enumerate(third):
                if THIRD_Y[i] == s:
                    third_y_step(u)
        if 0 <= s - LAG < n_steps:
            for u in pair(s - LAG):
                lamb_step(u)
    for u in third:
        lamb_step(u)

    with jax.named_scope("norms"):
        plane_norm = [remote(ns, nr.at[plane_slot[0]], n_send.at[k], n_recv.at[plane_slot[0]], plane_peer[k - 1]) for k in range(1, 8)]
        for cp in plane_norm:
            cp.start()
        nr[plane_slot[0]] = ns[...]
        for k in range(1, 8):
            remote(ns, nr.at[plane_slot[k]], n_send.at[k], n_recv.at[plane_slot[k]], plane_peer[k - 1]).wait_recv()
        for cp in plane_norm:
            cp.wait_send()
        ns[...] = jnp.sum(nr[0:8], axis=0)
        z_norm = [remote(ns, nr.at[8 + z], n_send.at[7 + k], n_recv.at[8 + z], z_peer[k]) for k in HOPS]
        for cp in z_norm:
            cp.start()
        nr[8 + z] = ns[...]
        for k in HOPS:
            zz = (z + k) % 4
            remote(ns, nr.at[8 + zz], n_send.at[7 + k], n_recv.at[8 + zz], z_peer[k]).wait_recv()
        for cp in z_norm:
            cp.wait_send()
    total = jnp.sum(nr[8:12], axis=0)
    norms = jnp.sqrt(jnp.sum(total, axis=1, keepdims=True))

    def gathered_q(u):
        if colour_of(u) == 2:
            return full.at[z, y, x, c, rows_of(u), :]
        return full.at[:, y, x, c, rows_of(u), :]

    def gathered_p(u):
        if colour_of(u) == 0:
            return full.at[:, :, x, c, rows_of(u), :]
        if colour_of(u) == 2:
            return full.at[z, :, x, c, rows_of(u), :]
        return full.at[:, y, :, c, rows_of(u), :]

    def gathered_c(u):
        return full.at[:, :, :, c, rows_of(u), :]

    def gather_z(u, k):
        src = rx.at[0, 0, 0, rows_of(u), :]
        dst = full.at[z, y, x, c, rows_of(u), :]
        if colour_of(u) == 2:
            src = dst = full.at[z, :, :, c, rows_of(u), :]
        return remote(src, dst, gz_send.at[u, k], gz_recv.at[u, k], z_peer[k])

    gz = [[gather_z(u, k) for k in HOPS] for u in units]
    gq = [remote(gathered_q(u), gathered_q(u), gq_send.at[u], gq_recv.at[u], y_peer if colour_of(u) == 2 else q_peer(u)) for u in units]
    gp = [remote(gathered_p(u), gathered_p(u), gp_send.at[u], gp_recv.at[u], x_peer if colour_of(u) == 2 else p_peer(u)) for u in units]
    gc = [remote(gathered_c(u), gathered_c(u), gc_send.at[u], gc_recv.at[u], core_peer) for u in units]

    def weight_step(u):
        t = tensor(u)
        valid = valid_of(u)
        scale = LEARN_RATE * (norms[2 * t:2 * t + 1] / norms[2 * t + 1:2 * t + 2])

        def tile(r, n):
            rows = pl.ds(base(u) + r, n)
            w = weights[t][:, flat_rows(u, r, n)].reshape(n, LANES)
            nw = w - scale * rz[0, rows, :]
            rz[1, rows, :] = nw
            rx[0, 0, 0, rows, :] = nw.astype(BF16)

        def body(i, carry):
            tile(pl.multiple_of(i * TILE, SUB), TILE)
            return carry

        lax.fori_loop(0, valid // TILE, body, 0)
        if valid % TILE:
            tile(valid - valid % TILE, valid % TILE)
        own_copy[u].start()
        out_w[u].start()
        if colour_of(u) == 2:
            own_copy[u].wait()
            gq[u].start()
        else:
            for cp in gz[u]:
                cp.start()

    def third_gather_z(u):
        with jax.named_scope(f"wait_third_gx#u={u}"):
            gp[u].wait_recv()
        for cp in gz[u]:
            cp.start()

    def third_gather_core(u):
        with jax.named_scope(f"wait_third_gz#u={u}"):
            for cp in gz[u]:
                cp.wait_recv()
        gc[u].start()

    def drain_reduce(u):
        if u >= n_pair - 4:
            p_copy[u].wait_send()
        if u >= n_pair - 2:
            c_copy[u].wait_send()
        q_copy[u].wait_send()
        for cp in z_copy[u]:
            cp.wait_send()
        out_m[u].wait()
        out_v[u].wait()

    def drain_gather(u):
        for cp in gz[u]:
            cp.wait_send()
        gq[u].wait_send()
        gp[u].wait_send()
        gc[u].wait_send()
        out_w[u].wait()

    order = list(range(n_steps))[::-1]
    for u in pair(order[0]):
        weight_step(u)
    for u in third:
        weight_step(u)
    for u in pair(order[1]):
        weight_step(u)
    for i in range(n_steps + 3):
        if i < n_steps:
            for u in pair(order[i]):
                own_copy[u].wait()
                with jax.named_scope(f"wait_gz#u={u}"):
                    for cp in gz[u]:
                        cp.wait_recv()
                gq[u].start()
        if i == 0:
            for u in third:
                gq[u].wait_recv()
                gp[u].start()
                for cp in third_copy[u][0] + list(third_copy[u][1:]):
                    cp.wait_send()
                out_m[u].wait()
                out_v[u].wait()
        if i + 2 < n_steps:
            for u in pair(order[i + 2]):
                weight_step(u)
        for j, u in enumerate(third):
            if GATHER_Z[j] == i:
                third_gather_z(u)
        if 0 <= i - 1 < n_steps:
            for u in pair(order[i - 1]):
                with jax.named_scope(f"wait_gq#u={u}"):
                    gq[u].wait_recv()
                gp[u].start()
        for j, u in enumerate(third):
            if GATHER_CORE[j] == i:
                third_gather_core(u)
        if 0 <= i - 2 < n_steps:
            for u in pair(order[i - 2]):
                with jax.named_scope(f"wait_gp#u={u}"):
                    gp[u].wait_recv()
                gc[u].start()
        if 0 <= i - 3 < n_steps:
            for u in pair(order[i - 3]):
                with jax.named_scope(f"wait_gc#u={u}"):
                    gc[u].wait_recv()
        if i < n_steps:
            for u in pair(order[i]):
                drain_reduce(u)
        if 0 <= i - LAG < n_steps:
            for u in pair(order[i - LAG]):
                drain_gather(u)
    for u in third:
        gc[u].wait_recv()
        drain_gather(u)
    for u in pair(order[-1]):
        drain_gather(u)


def comm(grads, state):
    n_units = len(UNITS)
    any_spec = pl.BlockSpec(memory_space=pl.ANY)
    dma = pltpu.SemaphoreType.DMA
    return pl.pallas_call(
        comm_kernel,
        in_specs=[any_spec] * 16,
        out_specs=[any_spec] * 4,
        out_shape=[jax.ShapeDtypeStruct((4, 2, 2, 2, TOTAL, LANES), BF16)] + [jax.ShapeDtypeStruct((TOTAL, LANES), F32)] * 3,
        scratch_shapes=[pltpu.VMEM((1, r * LANES), F32) for r in ROWS] * 3
        + [
            pltpu.VMEM((4, 2, 2, TOTAL, LANES), BF16),
            pltpu.VMEM((4, 2, TOTAL, LANES), F32),
            pltpu.VMEM((4, TOTAL, LANES), F32),
            pltpu.VMEM((3, TOTAL, LANES), F32),
            pltpu.VMEM((2, 4, 2, MAX_ROWS, LANES), F32),
            pltpu.VMEM((2, 4, 2, 2, MAX_ROWS, LANES), BF16),
            pltpu.VMEM((2, 2, 4, 2, 2, MAX_ROWS, LANES), BF16),
            pltpu.VMEM((2, 4, 2, 2, 1, MAX_ROWS * LANES), BF16),
            pltpu.VMEM((2, 2, 2, 2, MAX_ROWS, LANES), BF16),
            pltpu.VMEM((2, 2, 2, MAX_ROWS, LANES), F32),
            pltpu.VMEM((2, 4, 2, 2, 2, MAX_ROWS, LANES), BF16),
            pltpu.VMEM((8, LANES), F32),
            pltpu.VMEM((12, 8, LANES), F32),
            dma((12,)), dma((2,)),
            dma((n_units,)), dma((n_units,)), dma((n_units,)), dma((n_units,)), dma((n_units,)), dma((n_units,)),
            dma((n_units, 4)), dma((n_units, 4)), dma((11,)), dma((12,)), dma((3, n_units)), dma((n_units,)),
            dma((n_units, 4)), dma((n_units, 4)), dma((n_units,)), dma((n_units,)), dma((n_units,)), dma((n_units,)),
            dma((n_units,)), dma((n_units,)),
        ],
        compiler_params=pltpu.CompilerParams(collective_id=0, has_side_effects=True, vmem_limit_bytes=64 * 1024 * 1024 - 128 * 1024),
        name="lamb_comm",
    )(*grads, *state)


def solution(mesh):
    grad_spec = P("data", None, None)
    shard_spec = P(None, "data")
    full_spec = P(None, None)

    def device_step(*blocks):
        grads = [blocks[4 * t].reshape(4, 2, 2, 2, 1, -1) for t in range(4)]
        state = [blocks[4 * t + s] for s in (1, 2, 3) for t in range(4)]
        full, w, m, v = comm(grads, state)
        outs = unpack(full.reshape(32, TOTAL, LANES), w, m, v)
        results = []
        for t in range(4):
            results.extend((outs[t], outs[4 + t], outs[8 + t], outs[12 + t]))
        return tuple(results)

    return jax.shard_map(device_step, mesh=mesh, in_specs=(grad_spec, shard_spec, shard_spec, shard_spec) * 4, out_specs=(full_spec, shard_spec, shard_spec, shard_spec) * 4, check_vma=False)
```

```python
import functools

import jax
import jax.numpy as jnp
from jax import lax
from jax.experimental import pallas as pl
from jax.experimental.pallas import tpu as pltpu
from jax.sharding import PartitionSpec as P

STEP = 10
LEARN_RATE = 0.1
BETA_ONE = 0.9
BETA_TWO = 0.999
EPSILON = 1e-6
WEIGHT_DECAY = 0.01

LANES = 128
SUB = 16
ROWS = (867, 289, 1156, 1156)
PADDED = (880, 304, 1168, 1168)
STARTS = (0, 880, 1184, 2352)
TOTAL = 3520
PLAN = (
    (3, ((3, 4), (6, 5), (14, 14))),
    (2, ((8, 12), (13, 14), (12, 14))),
    (0, ((8, 10), (8, 6), (7, 7), (5, 4))),
    (1, ((3, 4), (3, 3), (3, 3))),
)
THIRD_ROWS = (13, 14)
THIRD_CORE = (3, 6)
THIRD_X = (9, 11)
THIRD_Y = (11, 13)
GATHER_Z = (8, 11)
GATHER_CORE = (11, 14)


def plan_units():
    units, third = [], []
    for t, pairs in PLAN:
        first = 0
        for rows_pair in pairs:
            for colour, rows in enumerate(rows_pair):
                units.append((t, first, rows * SUB, colour))
                first += rows * SUB
        if not third:
            for rows in THIRD_ROWS:
                third.append((t, first, rows * SUB, len(rows_pair)))
                first += rows * SUB
    return tuple(units), tuple(third)


PAIRED, THIRD = plan_units()
UNITS = PAIRED + THIRD
MAX_ROWS = 224
LAG = 4
TILE = 48
SHARDS = 4
HOPS = (1, 2, 3)
BOTH = (0, 1)
MESH = pl.DeviceIdType.MESH
F32 = jnp.float32
BF16 = jnp.bfloat16


def flat(dense, t):
    return dense.reshape(-1)[:ROWS[t] * LANES]


def unpack_kernel(full, w, m, v, *outs):
    spans = [pl.ds(STARTS[t], (ROWS[t] + SUB - 1) // SUB * SUB) for t in range(4)]
    for t, span in enumerate(spans):
        for j in range(SHARDS):
            outs[t][0, pl.ds(j * ROWS[t] * LANES, ROWS[t] * LANES)] = flat(full[j, span, :], t)

    @pl.when(pl.program_id(0) == 0)
    def _():
        for s, src in enumerate((w, m, v)):
            for t, span in enumerate(spans):
                outs[4 * s + 4 + t][0, :] = flat(src[span, :], t)


def unpack(full, w, m, v):
    state = pl.BlockSpec((TOTAL, LANES), lambda i: (0, 0))
    return pl.pallas_call(
        unpack_kernel,
        grid=(32 // SHARDS,),
        in_specs=[pl.BlockSpec((SHARDS, TOTAL, LANES), lambda i: (i, 0, 0)), state, state, state],
        out_specs=[pl.BlockSpec((1, SHARDS * r * LANES), lambda i: (0, i)) for r in ROWS]
        + [pl.BlockSpec((1, r * LANES), lambda i: (0, 0)) for r in ROWS] * 3,
        out_shape=[jax.ShapeDtypeStruct((1, 32 * r * LANES), BF16) for r in ROWS]
        + [jax.ShapeDtypeStruct((1, r * LANES), F32) for r in ROWS] * 3,
        name="unpack",
    )(full, w, m, v)


def comm_kernel(*refs):
    grads = refs[0:4]
    state_in = refs[4:16]
    full, new_w, new_m, new_v = refs[16:20]
    state = refs[20:32]
    weights, first_mom, second_mom = state[:4], state[4:8], state[8:]
    (rx, r2, r3, rz, t2, lx, ps, stage, rx3, t23, ps3, ns, nr, state_sem, stage_sem, p_send, p_recv, c_send, c_recv, q_send, q_recv,
     z_send, z_recv, n_send, n_recv, out_sem) = refs[32:]

    me = lax.axis_index("data")
    c = me % 2
    x = (me // 2) % 2
    y = (me // 4) % 2
    z = me // 8

    def dev(zz, yy, xx, cc):
        return (((zz * 2 + yy) * 2 + xx) * 2 + cc,)

    def flip(value, by):
        return 1 - value if by else value

    core_peer = dev(z, y, x, 1 - c)
    x_peer = dev(z, y, 1 - x, c)
    y_peer = dev(z, 1 - y, x, c)
    z_peer = {k: dev((z + k) % 4, y, x, c) for k in HOPS}
    plane_peer = [dev(z, flip(y, k // 4), flip(x, k // 2 % 2), flip(c, k % 2)) for k in range(1, 8)]
    plane_slot = [flip(y, k // 4) * 4 + flip(x, k // 2 % 2) * 2 + flip(c, k % 2) for k in range(8)]

    barrier = pltpu.get_barrier_semaphore()
    for peer in plane_peer + list(z_peer.values()):
        pl.semaphore_signal(barrier, inc=1, device_id=peer, device_id_type=MESH)

    def remote(src, dst, ssem, rsem, peer):
        return pltpu.make_async_remote_copy(src_ref=src, dst_ref=dst, send_sem=ssem, recv_sem=rsem, device_id=peer, device_id_type=MESH)

    n_units = len(UNITS)
    n_pair = len(PAIRED)
    n_steps = n_pair // 2
    units = range(n_units)

    def sweep(u, body):
        def step(i, carry):
            body(pl.multiple_of(i * SUB, SUB))
            return carry

        lax.fori_loop(0, height(u) // SUB, step, 0)

    def tensor(u):
        return UNITS[u][0]

    def height(u):
        return UNITS[u][2]

    def colour_of(u):
        return UNITS[u][3]

    def base(u):
        return STARTS[tensor(u)] + UNITS[u][1]

    def rows_of(u):
        return pl.ds(base(u), height(u))

    def valid_of(u):
        return min(height(u), ROWS[tensor(u)] - UNITS[u][1])

    def p_peer(u):
        return x_peer if colour_of(u) == 0 else y_peer

    def q_peer(u):
        return y_peer if colour_of(u) == 0 else x_peer

    def q_me(u):
        return y if colour_of(u) == 0 else x

    third = range(n_pair, n_units)
    pair_units = range(n_pair)

    def stage_copy(u, mine):
        t, first, h, colour = UNITS[u]
        lanes = pl.ds(first * LANES, valid_of(u) * LANES)
        if colour == 0:
            src = grads[t].at[:, :, x if mine else 1 - x, :, :, lanes]
        else:
            src = grads[t].at[:, y if mine else 1 - y, :, :, :, lanes]
        return pltpu.make_async_copy(src, stage.at[colour, :, :, :, :, pl.ds(0, valid_of(u) * LANES)], stage_sem.at[colour])

    def pack(u, store):
        h, colour = (height(u), colour_of(u))
        valid = valid_of(u)

        def body(j, carry):
            for cc in BOTH:
                dense = stage[colour, j // 2, j % 2, cc, :, pl.ds(0, valid * LANES)].reshape(valid, LANES)
                if valid < h:
                    dense = jnp.concatenate([dense, jnp.zeros((h - valid, LANES), BF16)], axis=0)
                store(j // 2, j % 2, cc, dense)
            return carry

        lax.fori_loop(0, 8, body, 0)

    def pack_send(u):
        h, colour = (height(u), colour_of(u))

        def store(zz, qq, cc, dense):
            ps[colour, (u // 2) % 2, zz, qq, cc, pl.ds(0, h), :] = dense

        pack(u, store)

    def pack_own(u):
        h, colour = (height(u), colour_of(u))

        def store(zz, qq, cc, dense):
            lx[colour, zz, qq, cc, pl.ds(0, h), :] = dense

        pack(u, store)

    p_copy = [remote(ps.at[u % 2, (u // 2) % 2, :, :, :, pl.ds(0, height(u)), :], rx.at[:, :, :, rows_of(u), :], p_send.at[u], p_recv.at[u], p_peer(u)) for u in pair_units]
    c_copy = [remote(t2.at[u % 2, :, :, pl.ds(0, height(u)), :], r2.at[:, :, rows_of(u), :], c_send.at[u], c_recv.at[u], core_peer) for u in pair_units]
    q_copy = [remote(r2.at[:, 1 - q_me(u), rows_of(u), :], r3.at[:, rows_of(u), :], q_send.at[u], q_recv.at[u], q_peer(u)) for u in pair_units]
    z_copy = [[remote(r3.at[(z + k) % 4, rows_of(u), :], rz.at[k - 1, rows_of(u), :], z_send.at[u, k - 1], z_recv.at[u, k - 1], z_peer[k]) for k in HOPS] for u in pair_units]
    out_m = [pltpu.make_async_copy(r2.at[0, q_me(u), rows_of(u), :], new_m.at[rows_of(u), :], out_sem.at[0, u]) for u in units]
    out_v = [pltpu.make_async_copy(r2.at[1, q_me(u), rows_of(u), :], new_v.at[rows_of(u), :], out_sem.at[1, u]) for u in units]
    out_w = [pltpu.make_async_copy(rz.at[1, rows_of(u), :], new_w.at[rows_of(u), :], out_sem.at[0, u]) for u in units]
    own_copy = [pltpu.make_async_copy(rx.at[0, 0, 0, rows_of(u), :], full.at[z, y, x, c, rows_of(u), :], out_sem.at[1, u]) for u in units]
    state_copy = [pltpu.make_async_copy(state_in[i], state[i], state_sem.at[i]) for i in range(12)]

    def core_step(u):
        with jax.named_scope(f"wait_p#u={u}"):
            p_copy[u].wait_recv()
        if u >= 2:
            c_copy[u - 2].wait_send()

        def body(r):
            a = lx[u % 2, :, :, 1 - c, pl.ds(r, SUB), :].astype(F32)
            b = rx[:, :, 1 - c, pl.ds(base(u) + r, SUB), :].astype(F32)
            t2[u % 2, :, :, pl.ds(r, SUB), :] = a + b

        sweep(u, body)
        c_copy[u].start()

    def q_step(u):
        with jax.named_scope(f"wait_c#u={u}"):
            c_copy[u].wait_recv()

        def body(r):
            a = lx[u % 2, :, :, c, pl.ds(r, SUB), :].astype(F32)
            b = rx[:, :, c, pl.ds(base(u) + r, SUB), :].astype(F32)
            r2[:, :, pl.ds(base(u) + r, SUB), :] = r2[:, :, pl.ds(base(u) + r, SUB), :] + (a + b)

        sweep(u, body)
        q_copy[u].start()

    def z_step(u):
        with jax.named_scope(f"wait_q#u={u}"):
            q_copy[u].wait_recv()

        def body(r):
            near = pl.ds(base(u) + r, SUB)
            r3[:, near, :] = r3[:, near, :] + r2[:, q_me(u), near, :]

        sweep(u, body)
        for cp in z_copy[u]:
            cp.start()

    def third_parts(u):
        i, h = u - n_pair, height(u)
        rows = rows_of(u)
        short = pl.ds(0, h)
        landing = [rx.at[0:2, :, :, rows, :], rx.at[2:4, :, :, rows, :], rx3.at[i, :, :, :, short, :]]
        first = [remote(ps3.at[i, (z + k) % 4, :, :, :, short, :], landing[k - 1], z_send.at[u, k - 1], z_recv.at[u, k - 1], z_peer[k]) for k in HOPS]
        core = remote(t23.at[i, :, :, short, :], r2.at[0:2, :, rows, :], c_send.at[u], c_recv.at[u], core_peer)
        along_x = remote(r2.at[0:2, 1 - x, rows, :], r3.at[0:2, rows, :], q_send.at[u], q_recv.at[u], x_peer)
        along_y = remote(r3.at[1 - y, rows, :], rz.at[0, rows, :], p_send.at[u], p_recv.at[u], y_peer)
        return first, core, along_x, along_y

    third_copy = {u: third_parts(u) for u in third}

    def third_stage(u):
        t, first, h, colour = UNITS[u]
        valid = valid_of(u)
        lanes = pl.ds(first * LANES, valid * LANES)
        copies = [pltpu.make_async_copy(grads[t].at[:, :, :, cc, :, lanes], stage.at[cc, :, :, :, :, pl.ds(0, valid * LANES)], stage_sem.at[cc]) for cc in BOTH]
        for cp in copies:
            cp.start()
        for cp in copies:
            cp.wait()

        def body(j, carry):
            for xx in BOTH:
                for cc in BOTH:
                    dense = stage[cc, j // 2, j % 2, xx, :, pl.ds(0, valid * LANES)].reshape(valid, LANES)
                    if valid < h:
                        dense = jnp.concatenate([dense, jnp.zeros((h - valid, LANES), BF16)], axis=0)
                    ps3[u - n_pair, j // 2, j % 2, xx, cc, pl.ds(0, h), :] = dense
            return carry

        lax.fori_loop(0, 8, body, 0)
        for cp in third_copy[u][0]:
            cp.start()

    def third_sum(u, r, cc):
        i = u - n_pair
        near = pl.ds(base(u) + r, SUB)
        own = ps3[i, z, :, :, cc, pl.ds(r, SUB), :].astype(F32) + rx[0:2, :, cc, near, :].astype(F32)
        return own + (rx[2:4, :, cc, near, :].astype(F32) + rx3[i, :, :, cc, pl.ds(r, SUB), :].astype(F32))

    def third_core_step(u):
        with jax.named_scope(f"wait_third_z#u={u}"):
            for cp in third_copy[u][0]:
                cp.wait_recv()

        def body(r):
            t23[u - n_pair, :, :, pl.ds(r, SUB), :] = third_sum(u, r, 1 - c)

        sweep(u, body)
        third_copy[u][1].start()

    def third_x_step(u):
        third_copy[u][1].wait_recv()

        def body(r):
            near = pl.ds(base(u) + r, SUB)
            r2[0:2, :, near, :] = r2[0:2, :, near, :] + third_sum(u, r, c)

        sweep(u, body)
        third_copy[u][2].start()

    def third_y_step(u):
        with jax.named_scope(f"wait_third_x#u={u}"):
            third_copy[u][2].wait_recv()

        def body(r):
            near = pl.ds(base(u) + r, SUB)
            r3[0:2, near, :] = r3[0:2, near, :] + r2[0:2, x, near, :]

        sweep(u, body)
        third_copy[u][3].start()

    def flat_rows(u, r, n):
        start = (UNITS[u][1] + r) * LANES
        return pl.ds(start if isinstance(r, int) else pl.multiple_of(start, LANES), n * LANES)

    def lamb_step(u):
        t, first, h, colour = UNITS[u]
        with jax.named_scope(f"wait_z#u={u}"):
            if colour == 2:
                third_copy[u][3].wait_recv()
            else:
                for cp in z_copy[u]:
                    cp.wait_recv()
        if first == 0:
            for i in (t, 4 + t, 8 + t):
                state_copy[i].wait()
        valid = valid_of(u)
        q = q_me(u)

        def tile(r, n):
            rows = pl.ds(base(u) + r, n)
            flat = flat_rows(u, r, n)
            w = weights[t][:, flat].reshape(n, LANES)
            m = first_mom[t][:, flat].reshape(n, LANES)
            v = second_mom[t][:, flat].reshape(n, LANES)
            if colour == 2:
                g = (r3[y, rows, :] + rz[0, rows, :]) / 32.0
            else:
                g = (((r3[z, rows, :] + rz[0, rows, :]) + rz[1, rows, :]) + rz[2, rows, :]) / 32.0
            nm = BETA_ONE * m + (1.0 - BETA_ONE) * g
            nv = BETA_TWO * v + (1.0 - BETA_TWO) * g * g
            u_dir = (nm / (1.0 - BETA_ONE ** STEP)) / (jnp.sqrt(nv / (1.0 - BETA_TWO ** STEP)) + EPSILON) + WEIGHT_DECAY * w
            r2[0, q, rows, :] = nm
            r2[1, q, rows, :] = nv
            rz[0, rows, :] = u_dir
            return w * w, u_dir * u_dir

        def body(i, carry):
            ww, uu = tile(pl.multiple_of(i * TILE, SUB), TILE)
            return (carry[0] + jnp.sum(ww.reshape(TILE // 8, 8, LANES), axis=0), carry[1] + jnp.sum(uu.reshape(TILE // 8, 8, LANES), axis=0))

        zero = jnp.zeros((8, LANES), F32)
        acc_w, acc_u = lax.fori_loop(0, valid // TILE, body, (zero, zero))
        sum_w = jnp.sum(acc_w, axis=0, keepdims=True)
        sum_u = jnp.sum(acc_u, axis=0, keepdims=True)
        if valid % TILE:
            ww, uu = tile(valid - valid % TILE, valid % TILE)
            sum_w = sum_w + jnp.sum(ww, axis=0, keepdims=True)
            sum_u = sum_u + jnp.sum(uu, axis=0, keepdims=True)
        ns[pl.ds(2 * t, 1), :] = ns[pl.ds(2 * t, 1), :] + sum_w
        ns[pl.ds(2 * t + 1, 1), :] = ns[pl.ds(2 * t + 1, 1), :] + sum_u
        out_m[u].start()
        out_v[u].start()

    def pair(s):
        return (2 * s, 2 * s + 1)

    for s in BOTH:
        for u in pair(s):
            stage_copy(u, False).start()
        if s == 0:
            for cp in state_copy:
                cp.start()
            ns[...] = jnp.zeros_like(ns)
        for u in pair(s):
            stage_copy(u, False).wait()
            pack_send(u)
        if s == 0:
            pl.semaphore_wait(barrier, 10)
        for u in pair(s):
            p_copy[u].start()
        third_stage(third[s])
    for u in pair(0):
        stage_copy(u, True).start()
    for u in pair(0):
        stage_copy(u, True).wait()
        pack_own(u)
        stage_copy(u + 4, False).start()

    for s in range(n_steps + LAG):
        if s < n_steps:
            for u in pair(s):
                core_step(u)
            for u in pair(s):
                q_step(u)
            for at, step in ((THIRD_CORE, third_core_step), (THIRD_X, third_x_step), (THIRD_Y, third_y_step)):
                for i, u in enumerate(third):
                    if at[i] == s:
                        step(u)
            if s + 2 < n_steps:
                for u in pair(s + 2):
                    stage_copy(u, False).wait()
                    p_copy[u - 4].wait_send()
                    pack_send(u)
                    p_copy[u].start()
            if s + 1 < n_steps:
                for u in pair(s + 1):
                    stage_copy(u, True).start()
                for u in pair(s + 1):
                    stage_copy(u, True).wait()
                    pack_own(u)
                    if s + 3 < n_steps:
                        stage_copy(u + 4, False).start()
        if 0 <= s - 1 < n_steps:
            for u in pair(s - 1):
                z_step(u)
        if s >= n_steps:
            for i, u in enumerate(third):
                if THIRD_Y[i] == s:
                    third_y_step(u)
        if 0 <= s - LAG < n_steps:
            for u in pair(s - LAG):
                lamb_step(u)
    for u in third:
        lamb_step(u)

    with jax.named_scope("norms"):
        plane_norm = [remote(ns, nr.at[plane_slot[0]], n_send.at[k], n_recv.at[plane_slot[0]], plane_peer[k - 1]) for k in range(1, 8)]
        for cp in plane_norm:
            cp.start()
        nr[plane_slot[0]] = ns[...]
        for k in range(1, 8):
            remote(ns, nr.at[plane_slot[k]], n_send.at[k], n_recv.at[plane_slot[k]], plane_peer[k - 1]).wait_recv()
        for cp in plane_norm:
            cp.wait_send()
        ns[...] = jnp.sum(nr[0:8], axis=0)
        z_norm = [remote(ns, nr.at[8 + z], n_send.at[7 + k], n_recv.at[8 + z], z_peer[k]) for k in HOPS]
        for cp in z_norm:
            cp.start()
        nr[8 + z] = ns[...]
        for k in HOPS:
            zz = (z + k) % 4
            remote(ns, nr.at[8 + zz], n_send.at[7 + k], n_recv.at[8 + zz], z_peer[k]).wait_recv()
        for cp in z_norm:
            cp.wait_send()
    total = jnp.sum(nr[8:12], axis=0)
    norms = jnp.sqrt(jnp.sum(total, axis=1, keepdims=True))

    def gathered_q(u):
        if colour_of(u) == 2:
            return full.at[z, y, x, c, rows_of(u), :]
        return full.at[:, y, x, c, rows_of(u), :]

    def gathered_p(u):
        if colour_of(u) == 0:
            return full.at[:, :, x, c, rows_of(u), :]
        if colour_of(u) == 2:
            return full.at[z, :, x, c, rows_of(u), :]
        return full.at[:, y, :, c, rows_of(u), :]

    def gathered_c(u):
        return full.at[:, :, :, c, rows_of(u), :]

    def gather_z(u, k):
        src = rx.at[0, 0, 0, rows_of(u), :]
        dst = full.at[z, y, x, c, rows_of(u), :]
        if colour_of(u) == 2:
            src = dst = full.at[z, :, :, c, rows_of(u), :]
        return remote(src, dst, z_send.at[u, k - 1], z_recv.at[u, k - 1], z_peer[k])

    gz = [[gather_z(u, k) for k in HOPS] for u in units]
    gq = [remote(gathered_q(u), gathered_q(u), q_send.at[u], q_recv.at[u], y_peer if colour_of(u) == 2 else q_peer(u)) for u in units]
    gp = [remote(gathered_p(u), gathered_p(u), p_send.at[u], p_recv.at[u], x_peer if colour_of(u) == 2 else p_peer(u)) for u in units]
    gc = [remote(gathered_c(u), gathered_c(u), c_send.at[u], c_recv.at[u], core_peer) for u in units]

    def drain_reduce(u):
        if colour_of(u) == 2:
            for cp in third_copy[u][0] + list(third_copy[u][1:]):
                cp.wait_send()
        else:
            if u >= n_pair - 4:
                p_copy[u].wait_send()
            if u >= n_pair - 2:
                c_copy[u].wait_send()
            q_copy[u].wait_send()
            for cp in z_copy[u]:
                cp.wait_send()
        out_m[u].wait()
        out_v[u].wait()

    def weight_step(u):
        drain_reduce(u)
        t = tensor(u)
        valid = valid_of(u)
        scale = LEARN_RATE * (norms[2 * t:2 * t + 1] / norms[2 * t + 1:2 * t + 2])

        def tile(r, n):
            rows = pl.ds(base(u) + r, n)
            w = weights[t][:, flat_rows(u, r, n)].reshape(n, LANES)
            nw = w - scale * rz[0, rows, :]
            rz[1, rows, :] = nw
            rx[0, 0, 0, rows, :] = nw.astype(BF16)

        def body(i, carry):
            tile(pl.multiple_of(i * TILE, SUB), TILE)
            return carry

        lax.fori_loop(0, valid // TILE, body, 0)
        if valid % TILE:
            tile(valid - valid % TILE, valid % TILE)
        own_copy[u].start()
        out_w[u].start()
        if colour_of(u) == 2:
            own_copy[u].wait()
            gq[u].start()
        else:
            for cp in gz[u]:
                cp.start()

    def third_gather_z(u):
        with jax.named_scope(f"wait_third_gx#u={u}"):
            gp[u].wait_recv()
        for cp in gz[u]:
            cp.start()

    def third_gather_core(u):
        with jax.named_scope(f"wait_third_gz#u={u}"):
            for cp in gz[u]:
                cp.wait_recv()
        gc[u].start()

    def drain_gather(u):
        for cp in gz[u]:
            cp.wait_send()
        gq[u].wait_send()
        gp[u].wait_send()
        gc[u].wait_send()
        out_w[u].wait()

    order = list(range(n_steps))[::-1]
    for u in pair(order[0]):
        weight_step(u)
    for u in third:
        weight_step(u)
    for u in pair(order[1]):
        weight_step(u)
    for i in range(n_steps + 3):
        if i < n_steps:
            for u in pair(order[i]):
                own_copy[u].wait()
                with jax.named_scope(f"wait_gz#u={u}"):
                    for cp in gz[u]:
                        cp.wait_recv()
                gq[u].start()
        if i == 0:
            for u in third:
                gq[u].wait_recv()
                gp[u].start()
        if i + 2 < n_steps:
            for u in pair(order[i + 2]):
                weight_step(u)
        for j, u in enumerate(third):
            if GATHER_Z[j] == i:
                third_gather_z(u)
        if 0 <= i - 1 < n_steps:
            for u in pair(order[i - 1]):
                with jax.named_scope(f"wait_gq#u={u}"):
                    gq[u].wait_recv()
                gp[u].start()
        for j, u in enumerate(third):
            if GATHER_CORE[j] == i:
                third_gather_core(u)
        if 0 <= i - 2 < n_steps:
            for u in pair(order[i - 2]):
                with jax.named_scope(f"wait_gp#u={u}"):
                    gp[u].wait_recv()
                gc[u].start()
        if 0 <= i - 3 < n_steps:
            for u in pair(order[i - 3]):
                with jax.named_scope(f"wait_gc#u={u}"):
                    gc[u].wait_recv()
        if 0 <= i - LAG < n_steps:
            for u in pair(order[i - LAG]):
                drain_gather(u)
    for u in third:
        gc[u].wait_recv()
        drain_gather(u)
    for u in pair(order[-1]):
        drain_gather(u)


def comm(grads, state):
    n_units = len(UNITS)
    any_spec = pl.BlockSpec(memory_space=pl.ANY)
    dma = pltpu.SemaphoreType.DMA
    return pl.pallas_call(
        comm_kernel,
        in_specs=[any_spec] * 16,
        out_specs=[any_spec] * 4,
        out_shape=[jax.ShapeDtypeStruct((4, 2, 2, 2, TOTAL, LANES), BF16)] + [jax.ShapeDtypeStruct((TOTAL, LANES), F32)] * 3,
        scratch_shapes=[pltpu.VMEM((1, r * LANES), F32) for r in ROWS] * 3
        + [
            pltpu.VMEM((4, 2, 2, TOTAL, LANES), BF16),
            pltpu.VMEM((4, 2, TOTAL, LANES), F32),
            pltpu.VMEM((4, TOTAL, LANES), F32),
            pltpu.VMEM((3, TOTAL, LANES), F32),
            pltpu.VMEM((2, 4, 2, MAX_ROWS, LANES), F32),
            pltpu.VMEM((2, 4, 2, 2, MAX_ROWS, LANES), BF16),
            pltpu.VMEM((2, 2, 4, 2, 2, MAX_ROWS, LANES), BF16),
            pltpu.VMEM((2, 4, 2, 2, 1, MAX_ROWS * LANES), BF16),
            pltpu.VMEM((2, 2, 2, 2, MAX_ROWS, LANES), BF16),
            pltpu.VMEM((2, 2, 2, MAX_ROWS, LANES), F32),
            pltpu.VMEM((2, 4, 2, 2, 2, MAX_ROWS, LANES), BF16),
            pltpu.VMEM((8, LANES), F32),
            pltpu.VMEM((12, 8, LANES), F32),
            dma((12,)), dma((2,)),
            dma((n_units,)), dma((n_units,)), dma((n_units,)), dma((n_units,)), dma((n_units,)), dma((n_units,)),
            dma((n_units, 3)), dma((n_units, 3)), dma((11,)), dma((12,)), dma((2, n_units)),
        ],
        compiler_params=pltpu.CompilerParams(collective_id=0, has_side_effects=True, vmem_limit_bytes=64 * 1024 * 1024 - 128 * 1024),
        name="lamb_comm",
    )(*grads, *state)


def solution(mesh):
    grad_spec = P("data", None, None)
    shard_spec = P(None, "data")
    full_spec = P(None, None)

    def device_step(*blocks):
        grads = [blocks[4 * t].reshape(4, 2, 2, 2, 1, -1) for t in range(4)]
        state = [blocks[4 * t + s] for s in (1, 2, 3) for t in range(4)]
        full, w, m, v = comm(grads, state)
        outs = unpack(full.reshape(32, TOTAL, LANES), w, m, v)
        results = []
        for t in range(4):
            results.extend((outs[t], outs[4 + t], outs[8 + t], outs[12 + t]))
        return tuple(results)

    return jax.shard_map(device_step, mesh=mesh, in_specs=(grad_spec, shard_spec, shard_spec, shard_spec) * 4, out_specs=(full_spec, shard_spec, shard_spec, shard_spec) * 4, check_vma=False)
```

```python
import functools

import jax
import jax.numpy as jnp
from jax import lax
from jax.experimental import pallas as pl
from jax.experimental.pallas import tpu as pltpu
from jax.sharding import PartitionSpec as P

STEP = 10
LEARN_RATE = 0.1
BETA_ONE = 0.9
BETA_TWO = 0.999
EPSILON = 1e-6
WEIGHT_DECAY = 0.01

LANES = 128
SUB = 16
ROWS = (867, 289, 1156, 1156)
PADDED = (880, 304, 1168, 1168)
STARTS = (0, 880, 1184, 2352)
TOTAL = 3520
PLAN = (
    (3, ((3, 4), (6, 5), (14, 14))),
    (2, ((8, 12), (13, 14), (12, 14))),
    (0, ((8, 10), (8, 6), (7, 7), (5, 4))),
    (1, ((3, 4), (3, 3), (3, 3))),
)
THIRD_ROWS = (13, 14)
THIRD_CORE = (3, 6)
THIRD_X = (9, 11)
THIRD_Y = (11, 13)
GATHER_Z = (8, 11)
GATHER_CORE = (11, 14)


def plan_units():
    units, third = [], []
    for t, pairs in PLAN:
        first = 0
        for rows_pair in pairs:
            for colour, rows in enumerate(rows_pair):
                units.append((t, first, rows * SUB, colour))
                first += rows * SUB
        if not third:
            for rows in THIRD_ROWS:
                third.append((t, first, rows * SUB, len(rows_pair)))
                first += rows * SUB
    return tuple(units), tuple(third)


PAIRED, THIRD = plan_units()
UNITS = PAIRED + THIRD
MAX_ROWS = 224
LAG = 4
TILE = 48
SHARDS = 4
HOPS = (1, 2, 3)
BOTH = (0, 1)
MESH = pl.DeviceIdType.MESH
F32 = jnp.float32
BF16 = jnp.bfloat16


def flat(dense, t):
    return dense.reshape(-1)[:ROWS[t] * LANES]


def unpack_kernel(full, w, m, v, *outs):
    spans = [pl.ds(STARTS[t], (ROWS[t] + SUB - 1) // SUB * SUB) for t in range(4)]
    for t, span in enumerate(spans):
        for j in range(SHARDS):
            outs[t][0, pl.ds(j * ROWS[t] * LANES, ROWS[t] * LANES)] = flat(full[j, span, :], t)

    @pl.when(pl.program_id(0) == 0)
    def _():
        for s, src in enumerate((w, m, v)):
            for t, span in enumerate(spans):
                outs[4 * s + 4 + t][0, :] = flat(src[span, :], t)


def unpack(full, w, m, v):
    state = pl.BlockSpec((TOTAL, LANES), lambda i: (0, 0))
    return pl.pallas_call(
        unpack_kernel,
        grid=(32 // SHARDS,),
        in_specs=[pl.BlockSpec((SHARDS, TOTAL, LANES), lambda i: (i, 0, 0)), state, state, state],
        out_specs=[pl.BlockSpec((1, SHARDS * r * LANES), lambda i: (0, i)) for r in ROWS]
        + [pl.BlockSpec((1, r * LANES), lambda i: (0, 0)) for r in ROWS] * 3,
        out_shape=[jax.ShapeDtypeStruct((1, 32 * r * LANES), BF16) for r in ROWS]
        + [jax.ShapeDtypeStruct((1, r * LANES), F32) for r in ROWS] * 3,
        name="unpack",
    )(full, w, m, v)


def comm_kernel(*refs):
    grads = refs[0:4]
    state_in = refs[4:16]
    full, new_w, new_m, new_v = refs[16:20]
    state = refs[20:32]
    weights, first_mom, second_mom = state[:4], state[4:8], state[8:]
    (rx, r2, r3, rz, t2, lx, ps, stage, rx3, t23, ps3, ns, nr, state_sem, stage_sem, p_send, p_recv, c_send, c_recv, q_send, q_recv,
     z_send, z_recv, n_send, n_recv, out_sem) = refs[32:]

    me = lax.axis_index("data")
    c = me % 2
    x = (me // 2) % 2
    y = (me // 4) % 2
    z = me // 8

    def dev(zz, yy, xx, cc):
        return (((zz * 2 + yy) * 2 + xx) * 2 + cc,)

    core_peer = dev(z, y, x, 1 - c)
    x_peer = dev(z, y, 1 - x, c)
    y_peer = dev(z, 1 - y, x, c)
    z_peer = {k: dev((z + k) % 4, y, x, c) for k in HOPS}
    others = [((me + k) % 32,) for k in range(1, 32)]

    barrier = pltpu.get_barrier_semaphore()
    for peer in others:
        pl.semaphore_signal(barrier, inc=1, device_id=peer, device_id_type=MESH)

    def remote(src, dst, ssem, rsem, peer):
        return pltpu.make_async_remote_copy(src_ref=src, dst_ref=dst, send_sem=ssem, recv_sem=rsem, device_id=peer, device_id_type=MESH)

    n_units = len(UNITS)
    n_pair = len(PAIRED)
    n_steps = n_pair // 2
    units = range(n_units)

    def wait_all(like, sem):
        pltpu.make_async_copy(like, like, sem).wait()

    def z_bytes(u):
        if colour_of(u) == 2:
            return ps3.at[u - n_pair, 0:3, :, :, :, pl.ds(0, height(u)), :]
        return rz.at[:, rows_of(u), :]

    def gather_z_bytes(u):
        if colour_of(u) == 2:
            return full.at[0:3, :, :, c, rows_of(u), :]
        return rx.at[0:3, 0, 0, rows_of(u), :]

    def sweep(u, body):
        def step(i, carry):
            body(pl.multiple_of(i * SUB, SUB))
            return carry

        lax.fori_loop(0, height(u) // SUB, step, 0)

    def tensor(u):
        return UNITS[u][0]

    def height(u):
        return UNITS[u][2]

    def colour_of(u):
        return UNITS[u][3]

    def base(u):
        return STARTS[tensor(u)] + UNITS[u][1]

    def rows_of(u):
        return pl.ds(base(u), height(u))

    def valid_of(u):
        return min(height(u), ROWS[tensor(u)] - UNITS[u][1])

    def p_peer(u):
        return x_peer if colour_of(u) == 0 else y_peer

    def q_peer(u):
        return y_peer if colour_of(u) == 0 else x_peer

    def q_me(u):
        return y if colour_of(u) == 0 else x

    third = range(n_pair, n_units)
    pair_units = range(n_pair)

    def stage_copy(u, mine):
        t, first, h, colour = UNITS[u]
        lanes = pl.ds(first * LANES, valid_of(u) * LANES)
        if colour == 0:
            src = grads[t].at[:, :, x if mine else 1 - x, :, :, lanes]
        else:
            src = grads[t].at[:, y if mine else 1 - y, :, :, :, lanes]
        return pltpu.make_async_copy(src, stage.at[colour, :, :, :, :, pl.ds(0, valid_of(u) * LANES)], stage_sem.at[colour])

    def pack(u, store):
        h, colour = (height(u), colour_of(u))
        valid = valid_of(u)

        def body(j, carry):
            for cc in BOTH:
                dense = stage[colour, j // 2, j % 2, cc, :, pl.ds(0, valid * LANES)].reshape(valid, LANES)
                if valid < h:
                    dense = jnp.concatenate([dense, jnp.zeros((h - valid, LANES), BF16)], axis=0)
                store(j // 2, j % 2, cc, dense)
            return carry

        lax.fori_loop(0, 8, body, 0)

    def pack_send(u):
        h, colour = (height(u), colour_of(u))

        def store(zz, qq, cc, dense):
            ps[colour, (u // 2) % 2, zz, qq, cc, pl.ds(0, h), :] = dense

        pack(u, store)

    def pack_own(u):
        h, colour = (height(u), colour_of(u))

        def store(zz, qq, cc, dense):
            lx[colour, zz, qq, cc, pl.ds(0, h), :] = dense

        pack(u, store)

    p_copy = [remote(ps.at[u % 2, (u // 2) % 2, :, :, :, pl.ds(0, height(u)), :], rx.at[:, :, :, rows_of(u), :], p_send.at[u], p_recv.at[u], p_peer(u)) for u in pair_units]
    c_copy = [remote(t2.at[u % 2, :, :, pl.ds(0, height(u)), :], r2.at[:, :, rows_of(u), :], c_send.at[u], c_recv.at[u], core_peer) for u in pair_units]
    q_copy = [remote(r2.at[:, 1 - q_me(u), rows_of(u), :], r3.at[:, rows_of(u), :], q_send.at[u], q_recv.at[u], q_peer(u)) for u in pair_units]
    z_copy = [[remote(r3.at[(z + k) % 4, rows_of(u), :], rz.at[k - 1, rows_of(u), :], z_send.at[u], z_recv.at[u], z_peer[k]) for k in HOPS] for u in pair_units]
    out_m = [pltpu.make_async_copy(r2.at[0, q_me(u), rows_of(u), :], new_m.at[rows_of(u), :], out_sem.at[0, u]) for u in units]
    out_v = [pltpu.make_async_copy(r2.at[1, q_me(u), rows_of(u), :], new_v.at[rows_of(u), :], out_sem.at[1, u]) for u in units]
    out_w = [pltpu.make_async_copy(rz.at[1, rows_of(u), :], new_w.at[rows_of(u), :], out_sem.at[0, u]) for u in units]
    own_copy = [pltpu.make_async_copy(rx.at[0, 0, 0, rows_of(u), :], full.at[z, y, x, c, rows_of(u), :], out_sem.at[1, u]) for u in units]
    state_copy = [pltpu.make_async_copy(state_in[i], state[i], state_sem.at[i]) for i in range(12)]

    def core_step(u):
        with jax.named_scope(f"wait_p#u={u}"):
            p_copy[u].wait_recv()
        if u >= 2:
            c_copy[u - 2].wait_send()

        def body(r):
            a = lx[u % 2, :, :, 1 - c, pl.ds(r, SUB), :].astype(F32)
            b = rx[:, :, 1 - c, pl.ds(base(u) + r, SUB), :].astype(F32)
            t2[u % 2, :, :, pl.ds(r, SUB), :] = a + b

        sweep(u, body)
        c_copy[u].start()

    def q_step(u):
        with jax.named_scope(f"wait_c#u={u}"):
            c_copy[u].wait_recv()

        def body(r):
            a = lx[u % 2, :, :, c, pl.ds(r, SUB), :].astype(F32)
            b = rx[:, :, c, pl.ds(base(u) + r, SUB), :].astype(F32)
            r2[:, :, pl.ds(base(u) + r, SUB), :] = r2[:, :, pl.ds(base(u) + r, SUB), :] + (a + b)

        sweep(u, body)
        q_copy[u].start()

    def z_step(u):
        with jax.named_scope(f"wait_q#u={u}"):
            q_copy[u].wait_recv()

        def body(r):
            near = pl.ds(base(u) + r, SUB)
            r3[:, near, :] = r3[:, near, :] + r2[:, q_me(u), near, :]

        sweep(u, body)
        for cp in z_copy[u]:
            cp.start()

    def third_parts(u):
        i, h = u - n_pair, height(u)
        rows = rows_of(u)
        short = pl.ds(0, h)
        landing = [rx.at[0:2, :, :, rows, :], rx.at[2:4, :, :, rows, :], rx3.at[i, :, :, :, short, :]]
        first = [remote(ps3.at[i, (z + k) % 4, :, :, :, short, :], landing[k - 1], z_send.at[u], z_recv.at[u], z_peer[k]) for k in HOPS]
        core = remote(t23.at[i, :, :, short, :], r2.at[0:2, :, rows, :], c_send.at[u], c_recv.at[u], core_peer)
        along_x = remote(r2.at[0:2, 1 - x, rows, :], r3.at[0:2, rows, :], q_send.at[u], q_recv.at[u], x_peer)
        along_y = remote(r3.at[1 - y, rows, :], rz.at[0, rows, :], p_send.at[u], p_recv.at[u], y_peer)
        return first, core, along_x, along_y

    third_copy = {u: third_parts(u) for u in third}

    def third_stage(u):
        t, first, h, colour = UNITS[u]
        valid = valid_of(u)
        lanes = pl.ds(first * LANES, valid * LANES)
        copies = [pltpu.make_async_copy(grads[t].at[:, :, :, cc, :, lanes], stage.at[cc, :, :, :, :, pl.ds(0, valid * LANES)], stage_sem.at[cc]) for cc in BOTH]
        for cp in copies:
            cp.start()
        for cp in copies:
            cp.wait()

        def body(j, carry):
            for xx in BOTH:
                for cc in BOTH:
                    dense = stage[cc, j // 2, j % 2, xx, :, pl.ds(0, valid * LANES)].reshape(valid, LANES)
                    if valid < h:
                        dense = jnp.concatenate([dense, jnp.zeros((h - valid, LANES), BF16)], axis=0)
                    ps3[u - n_pair, j // 2, j % 2, xx, cc, pl.ds(0, h), :] = dense
            return carry

        lax.fori_loop(0, 8, body, 0)
        for cp in third_copy[u][0]:
            cp.start()

    def third_sum(u, r, cc):
        i = u - n_pair
        near = pl.ds(base(u) + r, SUB)
        own = ps3[i, z, :, :, cc, pl.ds(r, SUB), :].astype(F32) + rx[0:2, :, cc, near, :].astype(F32)
        return own + (rx[2:4, :, cc, near, :].astype(F32) + rx3[i, :, :, cc, pl.ds(r, SUB), :].astype(F32))

    def third_core_step(u):
        with jax.named_scope(f"wait_third_z#u={u}"):
            wait_all(z_bytes(u), z_recv.at[u])

        def body(r):
            t23[u - n_pair, :, :, pl.ds(r, SUB), :] = third_sum(u, r, 1 - c)

        sweep(u, body)
        third_copy[u][1].start()

    def third_x_step(u):
        third_copy[u][1].wait_recv()

        def body(r):
            near = pl.ds(base(u) + r, SUB)
            r2[0:2, :, near, :] = r2[0:2, :, near, :] + third_sum(u, r, c)

        sweep(u, body)
        third_copy[u][2].start()

    def third_y_step(u):
        with jax.named_scope(f"wait_third_x#u={u}"):
            third_copy[u][2].wait_recv()

        def body(r):
            near = pl.ds(base(u) + r, SUB)
            r3[0:2, near, :] = r3[0:2, near, :] + r2[0:2, x, near, :]

        sweep(u, body)
        third_copy[u][3].start()

    def flat_rows(u, r, n):
        start = (UNITS[u][1] + r) * LANES
        return pl.ds(start if isinstance(r, int) else pl.multiple_of(start, LANES), n * LANES)

    def lamb_step(u):
        t, first, h, colour = UNITS[u]
        with jax.named_scope(f"wait_z#u={u}"):
            if colour == 2:
                third_copy[u][3].wait_recv()
            else:
                wait_all(z_bytes(u), z_recv.at[u])
        if first == 0:
            for i in (t, 4 + t, 8 + t):
                state_copy[i].wait()
        valid = valid_of(u)
        q = q_me(u)

        def tile(r, n):
            rows = pl.ds(base(u) + r, n)
            flat = flat_rows(u, r, n)
            w = weights[t][:, flat].reshape(n, LANES)
            m = first_mom[t][:, flat].reshape(n, LANES)
            v = second_mom[t][:, flat].reshape(n, LANES)
            if colour == 2:
                g = (r3[y, rows, :] + rz[0, rows, :]) / 32.0
            else:
                g = (((r3[z, rows, :] + rz[0, rows, :]) + rz[1, rows, :]) + rz[2, rows, :]) / 32.0
            nm = BETA_ONE * m + (1.0 - BETA_ONE) * g
            nv = BETA_TWO * v + (1.0 - BETA_TWO) * g * g
            u_dir = (nm / (1.0 - BETA_ONE ** STEP)) / (jnp.sqrt(nv / (1.0 - BETA_TWO ** STEP)) + EPSILON) + WEIGHT_DECAY * w
            r2[0, q, rows, :] = nm
            r2[1, q, rows, :] = nv
            rz[0, rows, :] = u_dir
            return w * w, u_dir * u_dir

        def body(i, carry):
            ww, uu = tile(pl.multiple_of(i * TILE, SUB), TILE)
            return (carry[0] + jnp.sum(ww.reshape(TILE // 8, 8, LANES), axis=0), carry[1] + jnp.sum(uu.reshape(TILE // 8, 8, LANES), axis=0))

        zero = jnp.zeros((8, LANES), F32)
        acc_w, acc_u = lax.fori_loop(0, valid // TILE, body, (zero, zero))
        sum_w = jnp.sum(acc_w, axis=0, keepdims=True)
        sum_u = jnp.sum(acc_u, axis=0, keepdims=True)
        if valid % TILE:
            ww, uu = tile(valid - valid % TILE, valid % TILE)
            sum_w = sum_w + jnp.sum(ww, axis=0, keepdims=True)
            sum_u = sum_u + jnp.sum(uu, axis=0, keepdims=True)
        ns[pl.ds(2 * t, 1), :] = ns[pl.ds(2 * t, 1), :] + sum_w
        ns[pl.ds(2 * t + 1, 1), :] = ns[pl.ds(2 * t + 1, 1), :] + sum_u
        out_m[u].start()
        out_v[u].start()

    def pair(s):
        return (2 * s, 2 * s + 1)

    for s in BOTH:
        for u in pair(s):
            stage_copy(u, False).start()
        if s == 0:
            for cp in state_copy:
                cp.start()
            ns[...] = jnp.zeros_like(ns)
        for u in pair(s):
            stage_copy(u, False).wait()
            pack_send(u)
        if s == 0:
            pl.semaphore_wait(barrier, 31)
        for u in pair(s):
            p_copy[u].start()
        third_stage(third[s])
    for u in pair(0):
        stage_copy(u, True).start()
    for u in pair(0):
        stage_copy(u, True).wait()
        pack_own(u)
        stage_copy(u + 4, False).start()

    for s in range(n_steps + LAG):
        if s < n_steps:
            for u in pair(s):
                core_step(u)
            for u in pair(s):
                q_step(u)
            for at, step in ((THIRD_CORE, third_core_step), (THIRD_X, third_x_step), (THIRD_Y, third_y_step)):
                for i, u in enumerate(third):
                    if at[i] == s:
                        step(u)
            if s + 2 < n_steps:
                for u in pair(s + 2):
                    stage_copy(u, False).wait()
                    p_copy[u - 4].wait_send()
                    pack_send(u)
                    p_copy[u].start()
            if s + 1 < n_steps:
                for u in pair(s + 1):
                    stage_copy(u, True).start()
                for u in pair(s + 1):
                    stage_copy(u, True).wait()
                    pack_own(u)
                    if s + 3 < n_steps:
                        stage_copy(u + 4, False).start()
        if 0 <= s - 1 < n_steps:
            for u in pair(s - 1):
                z_step(u)
        if s >= n_steps:
            for i, u in enumerate(third):
                if THIRD_Y[i] == s:
                    third_y_step(u)
        if 0 <= s - LAG < n_steps:
            for u in pair(s - LAG):
                lamb_step(u)
    for u in third:
        lamb_step(u)

    with jax.named_scope("norms"):
        shares = [remote(ns, nr.at[me], n_send.at[k], n_recv.at[me], peer) for k, peer in enumerate(others)]
        for cp in shares:
            cp.start()
        nr[me] = ns[...]
        for k, (sender,) in enumerate(others):
            remote(ns, nr.at[sender], n_send.at[k], n_recv.at[sender], others[k]).wait_recv()
        for cp in shares:
            cp.wait_send()
    total = jnp.sum(nr[...], axis=0)
    norms = jnp.sqrt(jnp.sum(total, axis=1, keepdims=True))

    def gathered_q(u):
        if colour_of(u) == 2:
            return full.at[z, y, x, c, rows_of(u), :]
        return full.at[:, y, x, c, rows_of(u), :]

    def gathered_p(u):
        if colour_of(u) == 0:
            return full.at[:, :, x, c, rows_of(u), :]
        if colour_of(u) == 2:
            return full.at[z, :, x, c, rows_of(u), :]
        return full.at[:, y, :, c, rows_of(u), :]

    def gathered_c(u):
        return full.at[:, :, :, c, rows_of(u), :]

    def gather_z(u, k):
        src = rx.at[0, 0, 0, rows_of(u), :]
        dst = full.at[z, y, x, c, rows_of(u), :]
        if colour_of(u) == 2:
            src = dst = full.at[z, :, :, c, rows_of(u), :]
        return remote(src, dst, z_send.at[u], z_recv.at[u], z_peer[k])

    gz = [[gather_z(u, k) for k in HOPS] for u in units]
    gq = [remote(gathered_q(u), gathered_q(u), q_send.at[u], q_recv.at[u], y_peer if colour_of(u) == 2 else q_peer(u)) for u in units]
    gp = [remote(gathered_p(u), gathered_p(u), p_send.at[u], p_recv.at[u], x_peer if colour_of(u) == 2 else p_peer(u)) for u in units]
    gc = [remote(gathered_c(u), gathered_c(u), c_send.at[u], c_recv.at[u], core_peer) for u in units]

    def drain_reduce(u):
        if colour_of(u) == 2:
            for cp in third_copy[u][1:]:
                cp.wait_send()
        else:
            if u >= n_pair - 4:
                p_copy[u].wait_send()
            if u >= n_pair - 2:
                c_copy[u].wait_send()
            q_copy[u].wait_send()
        wait_all(z_bytes(u), z_send.at[u])
        out_m[u].wait()
        out_v[u].wait()

    def weight_step(u):
        drain_reduce(u)
        t = tensor(u)
        valid = valid_of(u)
        scale = LEARN_RATE * (norms[2 * t:2 * t + 1] / norms[2 * t + 1:2 * t + 2])

        def tile(r, n):
            rows = pl.ds(base(u) + r, n)
            w = weights[t][:, flat_rows(u, r, n)].reshape(n, LANES)
            nw = w - scale * rz[0, rows, :]
            rz[1, rows, :] = nw
            rx[0, 0, 0, rows, :] = nw.astype(BF16)

        def body(i, carry):
            tile(pl.multiple_of(i * TILE, SUB), TILE)
            return carry

        lax.fori_loop(0, valid // TILE, body, 0)
        if valid % TILE:
            tile(valid - valid % TILE, valid % TILE)
        own_copy[u].start()
        out_w[u].start()
        if colour_of(u) == 2:
            own_copy[u].wait()
            gq[u].start()
        else:
            for cp in gz[u]:
                cp.start()

    def third_gather_z(u):
        with jax.named_scope(f"wait_third_gx#u={u}"):
            gp[u].wait_recv()
        for cp in gz[u]:
            cp.start()

    def third_gather_core(u):
        with jax.named_scope(f"wait_third_gz#u={u}"):
            wait_all(gather_z_bytes(u), z_recv.at[u])
        gc[u].start()

    def drain_gather(u):
        wait_all(gather_z_bytes(u), z_send.at[u])
        gq[u].wait_send()
        gp[u].wait_send()
        gc[u].wait_send()
        out_w[u].wait()

    order = list(range(n_steps))[::-1]
    for u in pair(order[0]):
        weight_step(u)
    for u in third:
        weight_step(u)
    for u in pair(order[1]):
        weight_step(u)
    for i in range(n_steps + 3):
        if i < n_steps:
            for u in pair(order[i]):
                own_copy[u].wait()
                with jax.named_scope(f"wait_gz#u={u}"):
                    wait_all(gather_z_bytes(u), z_recv.at[u])
                gq[u].start()
        if i == 0:
            for u in third:
                gq[u].wait_recv()
                gp[u].start()
        if i + 2 < n_steps:
            for u in pair(order[i + 2]):
                weight_step(u)
        for j, u in enumerate(third):
            if GATHER_Z[j] == i:
                third_gather_z(u)
        if 0 <= i - 1 < n_steps:
            for u in pair(order[i - 1]):
                with jax.named_scope(f"wait_gq#u={u}"):
                    gq[u].wait_recv()
                gp[u].start()
        for j, u in enumerate(third):
            if GATHER_CORE[j] == i:
                third_gather_core(u)
        if 0 <= i - 2 < n_steps:
            for u in pair(order[i - 2]):
                with jax.named_scope(f"wait_gp#u={u}"):
                    gp[u].wait_recv()
                gc[u].start()
        if 0 <= i - 3 < n_steps:
            for u in pair(order[i - 3]):
                with jax.named_scope(f"wait_gc#u={u}"):
                    gc[u].wait_recv()
        if 0 <= i - LAG < n_steps:
            for u in pair(order[i - LAG]):
                drain_gather(u)
    for u in third:
        gc[u].wait_recv()
        drain_gather(u)
    for u in pair(order[-1]):
        drain_gather(u)


def comm(grads, state):
    n_units = len(UNITS)
    any_spec = pl.BlockSpec(memory_space=pl.ANY)
    dma = pltpu.SemaphoreType.DMA
    return pl.pallas_call(
        comm_kernel,
        in_specs=[any_spec] * 16,
        out_specs=[any_spec] * 4,
        out_shape=[jax.ShapeDtypeStruct((4, 2, 2, 2, TOTAL, LANES), BF16)] + [jax.ShapeDtypeStruct((TOTAL, LANES), F32)] * 3,
        scratch_shapes=[pltpu.VMEM((1, r * LANES), F32) for r in ROWS] * 3
        + [
            pltpu.VMEM((4, 2, 2, TOTAL, LANES), BF16),
            pltpu.VMEM((4, 2, TOTAL, LANES), F32),
            pltpu.VMEM((4, TOTAL, LANES), F32),
            pltpu.VMEM((3, TOTAL, LANES), F32),
            pltpu.VMEM((2, 4, 2, MAX_ROWS, LANES), F32),
            pltpu.VMEM((2, 4, 2, 2, MAX_ROWS, LANES), BF16),
            pltpu.VMEM((2, 2, 4, 2, 2, MAX_ROWS, LANES), BF16),
            pltpu.VMEM((2, 4, 2, 2, 1, MAX_ROWS * LANES), BF16),
            pltpu.VMEM((2, 2, 2, 2, MAX_ROWS, LANES), BF16),
            pltpu.VMEM((2, 2, 2, MAX_ROWS, LANES), F32),
            pltpu.VMEM((2, 4, 2, 2, 2, MAX_ROWS, LANES), BF16),
            pltpu.VMEM((8, LANES), F32),
            pltpu.VMEM((32, 8, LANES), F32),
            dma((12,)), dma((2,)),
            dma((n_units,)), dma((n_units,)), dma((n_units,)), dma((n_units,)), dma((n_units,)), dma((n_units,)),
            dma((n_units,)), dma((n_units,)), dma((31,)), dma((32,)), dma((2, n_units)),
        ],
        compiler_params=pltpu.CompilerParams(collective_id=0, has_side_effects=True, vmem_limit_bytes=64 * 1024 * 1024 - 128 * 1024),
        name="lamb_comm",
    )(*grads, *state)


def solution(mesh):
    grad_spec = P("data", None, None)
    shard_spec = P(None, "data")
    full_spec = P(None, None)

    def device_step(*blocks):
        grads = [blocks[4 * t].reshape(4, 2, 2, 2, 1, -1) for t in range(4)]
        state = [blocks[4 * t + s] for s in (1, 2, 3) for t in range(4)]
        full, w, m, v = comm(grads, state)
        outs = unpack(full.reshape(32, TOTAL, LANES), w, m, v)
        results = []
        for t in range(4):
            results.extend((outs[t], outs[4 + t], outs[8 + t], outs[12 + t]))
        return tuple(results)

    return jax.shard_map(device_step, mesh=mesh, in_specs=(grad_spec, shard_spec, shard_spec, shard_spec) * 4, out_specs=(full_spec, shard_spec, shard_spec, shard_spec) * 4, check_vma=False)
```

```python
import functools

import jax
import jax.numpy as jnp
from jax import lax
from jax.experimental import pallas as pl
from jax.experimental.pallas import tpu as pltpu
from jax.sharding import PartitionSpec as P

STEP = 10
LEARN_RATE = 0.1
BETA_ONE = 0.9
BETA_TWO = 0.999
EPSILON = 1e-6
WEIGHT_DECAY = 0.01

LANES = 128
SUB = 16
ROWS = (867, 289, 1156, 1156)
PADDED = (880, 304, 1168, 1168)
STARTS = (0, 880, 1184, 2352)
TOTAL = 3520
PLAN = (
    (3, ((3, 4), (6, 5), (14, 14))),
    (2, ((8, 12), (13, 14), (12, 14))),
    (0, ((8, 10), (8, 6), (7, 7), (5, 4))),
    (1, ((3, 4), (3, 3), (3, 3))),
)
THIRD_ROWS = (13, 14)
THIRD_CORE = (3, 6)
THIRD_X = (9, 11)
THIRD_Y = (11, 13)
GATHER_Z = (8, 11)
GATHER_CORE = (11, 14)


def plan_units():
    units, third = [], []
    for t, pairs in PLAN:
        first = 0
        for rows_pair in pairs:
            for colour, rows in enumerate(rows_pair):
                units.append((t, first, rows * SUB, colour))
                first += rows * SUB
        if not third:
            for rows in THIRD_ROWS:
                third.append((t, first, rows * SUB, len(rows_pair)))
                first += rows * SUB
    return tuple(units), tuple(third)


PAIRED, THIRD = plan_units()
UNITS = PAIRED + THIRD
MAX_ROWS = 224
LAG = 4
TILE = 48
SHARDS = 4
HOPS = (1, 2, 3)
BOTH = (0, 1)
MESH = pl.DeviceIdType.MESH
F32 = jnp.float32
BF16 = jnp.bfloat16


def flat(dense, t):
    return dense.reshape(-1)[:ROWS[t] * LANES]


def unpack_kernel(full, w, m, v, *outs):
    spans = [pl.ds(STARTS[t], (ROWS[t] + SUB - 1) // SUB * SUB) for t in range(4)]
    for t, span in enumerate(spans):
        for j in range(SHARDS):
            outs[t][0, pl.ds(j * ROWS[t] * LANES, ROWS[t] * LANES)] = flat(full[j, span, :], t)

    @pl.when(pl.program_id(0) == 0)
    def _():
        for s, src in enumerate((w, m, v)):
            for t, span in enumerate(spans):
                outs[4 * s + 4 + t][0, :] = flat(src[span, :], t)


def unpack(full, w, m, v):
    state = pl.BlockSpec((TOTAL, LANES), lambda i: (0, 0))
    return pl.pallas_call(
        unpack_kernel,
        grid=(32 // SHARDS,),
        in_specs=[pl.BlockSpec((SHARDS, TOTAL, LANES), lambda i: (i, 0, 0)), state, state, state],
        out_specs=[pl.BlockSpec((1, SHARDS * r * LANES), lambda i: (0, i)) for r in ROWS]
        + [pl.BlockSpec((1, r * LANES), lambda i: (0, 0)) for r in ROWS] * 3,
        out_shape=[jax.ShapeDtypeStruct((1, 32 * r * LANES), BF16) for r in ROWS]
        + [jax.ShapeDtypeStruct((1, r * LANES), F32) for r in ROWS] * 3,
        name="unpack",
    )(full, w, m, v)


def comm_kernel(*refs):
    grads = refs[0:4]
    state_in = refs[4:16]
    full, new_w, new_m, new_v = refs[16:20]
    state = refs[20:32]
    weights, first_mom, second_mom = state[:4], state[4:8], state[8:]
    (rx, r2, r3, rz, t2, lx, ps, stage, rx3, t23, ps3, ns, nr, state_sem, stage_sem, p_send, p_recv, c_send, c_recv, q_send, q_recv,
     z_send, z_recv, n_send, n_recv, out_sem) = refs[32:]

    me = lax.axis_index("data")
    c = me % 2
    x = (me // 2) % 2
    y = (me // 4) % 2
    z = me // 8

    def dev(zz, yy, xx, cc):
        return (((zz * 2 + yy) * 2 + xx) * 2 + cc,)

    def flip(value, by):
        return 1 - value if by else value

    core_peer = dev(z, y, x, 1 - c)
    x_peer = dev(z, y, 1 - x, c)
    y_peer = dev(z, 1 - y, x, c)
    z_peer = {k: dev((z + k) % 4, y, x, c) for k in HOPS}
    plane_peer = [dev(z, flip(y, k // 4), flip(x, k // 2 % 2), flip(c, k % 2)) for k in range(1, 8)]
    plane_slot = [flip(y, k // 4) * 4 + flip(x, k // 2 % 2) * 2 + flip(c, k % 2) for k in range(8)]

    barrier = pltpu.get_barrier_semaphore()
    for peer in plane_peer + list(z_peer.values()):
        pl.semaphore_signal(barrier, inc=1, device_id=peer, device_id_type=MESH)

    def remote(src, dst, ssem, rsem, peer):
        return pltpu.make_async_remote_copy(src_ref=src, dst_ref=dst, send_sem=ssem, recv_sem=rsem, device_id=peer, device_id_type=MESH)

    n_units = len(UNITS)
    n_pair = len(PAIRED)
    n_steps = n_pair // 2
    units = range(n_units)

    def wait_all(like, sem):
        pltpu.make_async_copy(like, like, sem).wait()

    def z_bytes(u):
        if colour_of(u) == 2:
            return ps3.at[u - n_pair, 0:3, :, :, :, pl.ds(0, height(u)), :]
        return rz.at[:, rows_of(u), :]

    def gather_z_bytes(u):
        if colour_of(u) == 2:
            return full.at[0:3, :, :, c, rows_of(u), :]
        return rx.at[0:3, 0, 0, rows_of(u), :]

    def sweep(u, body):
        def step(i, carry):
            body(pl.multiple_of(i * SUB, SUB))
            return carry

        lax.fori_loop(0, height(u) // SUB, step, 0)

    def tensor(u):
        return UNITS[u][0]

    def height(u):
        return UNITS[u][2]

    def colour_of(u):
        return UNITS[u][3]

    def base(u):
        return STARTS[tensor(u)] + UNITS[u][1]

    def rows_of(u):
        return pl.ds(base(u), height(u))

    def valid_of(u):
        return min(height(u), ROWS[tensor(u)] - UNITS[u][1])

    def p_peer(u):
        return x_peer if colour_of(u) == 0 else y_peer

    def q_peer(u):
        return y_peer if colour_of(u) == 0 else x_peer

    def q_me(u):
        return y if colour_of(u) == 0 else x

    third = range(n_pair, n_units)
    pair_units = range(n_pair)

    def stage_copy(u, mine):
        t, first, h, colour = UNITS[u]
        lanes = pl.ds(first * LANES, valid_of(u) * LANES)
        if colour == 0:
            src = grads[t].at[:, :, x if mine else 1 - x, :, :, lanes]
        else:
            src = grads[t].at[:, y if mine else 1 - y, :, :, :, lanes]
        return pltpu.make_async_copy(src, stage.at[colour, :, :, :, :, pl.ds(0, valid_of(u) * LANES)], stage_sem.at[colour])

    def pack(u, store):
        h, colour = (height(u), colour_of(u))
        valid = valid_of(u)

        def body(j, carry):
            for cc in BOTH:
                dense = stage[colour, j // 2, j % 2, cc, :, pl.ds(0, valid * LANES)].reshape(valid, LANES)
                if valid < h:
                    dense = jnp.concatenate([dense, jnp.zeros((h - valid, LANES), BF16)], axis=0)
                store(j // 2, j % 2, cc, dense)
            return carry

        lax.fori_loop(0, 8, body, 0)

    def pack_send(u):
        h, colour = (height(u), colour_of(u))

        def store(zz, qq, cc, dense):
            ps[colour, (u // 2) % 2, zz, qq, cc, pl.ds(0, h), :] = dense

        pack(u, store)

    def pack_own(u):
        h, colour = (height(u), colour_of(u))

        def store(zz, qq, cc, dense):
            lx[colour, zz, qq, cc, pl.ds(0, h), :] = dense

        pack(u, store)

    p_copy = [remote(ps.at[u % 2, (u // 2) % 2, :, :, :, pl.ds(0, height(u)), :], rx.at[:, :, :, rows_of(u), :], p_send.at[u], p_recv.at[u], p_peer(u)) for u in pair_units]
    c_copy = [remote(t2.at[u % 2, :, :, pl.ds(0, height(u)), :], r2.at[:, :, rows_of(u), :], c_send.at[u], c_recv.at[u], core_peer) for u in pair_units]
    q_copy = [remote(r2.at[:, 1 - q_me(u), rows_of(u), :], r3.at[:, rows_of(u), :], q_send.at[u], q_recv.at[u], q_peer(u)) for u in pair_units]
    z_copy = [[remote(r3.at[(z + k) % 4, rows_of(u), :], rz.at[k - 1, rows_of(u), :], z_send.at[u], z_recv.at[u], z_peer[k]) for k in HOPS] for u in pair_units]
    out_m = [pltpu.make_async_copy(r2.at[0, q_me(u), rows_of(u), :], new_m.at[rows_of(u), :], out_sem.at[0, u]) for u in units]
    out_v = [pltpu.make_async_copy(r2.at[1, q_me(u), rows_of(u), :], new_v.at[rows_of(u), :], out_sem.at[1, u]) for u in units]
    out_w = [pltpu.make_async_copy(rz.at[1, rows_of(u), :], new_w.at[rows_of(u), :], out_sem.at[0, u]) for u in units]
    own_copy = [pltpu.make_async_copy(rx.at[0, 0, 0, rows_of(u), :], full.at[z, y, x, c, rows_of(u), :], out_sem.at[1, u]) for u in units]
    state_copy = [pltpu.make_async_copy(state_in[i], state[i], state_sem.at[i]) for i in range(12)]

    def core_step(u):
        with jax.named_scope(f"wait_p#u={u}"):
            p_copy[u].wait_recv()
        if u >= 2:
            c_copy[u - 2].wait_send()

        def body(r):
            a = lx[u % 2, :, :, 1 - c, pl.ds(r, SUB), :].astype(F32)
            b = rx[:, :, 1 - c, pl.ds(base(u) + r, SUB), :].astype(F32)
            t2[u % 2, :, :, pl.ds(r, SUB), :] = a + b

        sweep(u, body)
        c_copy[u].start()

    def q_step(u):
        with jax.named_scope(f"wait_c#u={u}"):
            c_copy[u].wait_recv()

        def body(r):
            a = lx[u % 2, :, :, c, pl.ds(r, SUB), :].astype(F32)
            b = rx[:, :, c, pl.ds(base(u) + r, SUB), :].astype(F32)
            r2[:, :, pl.ds(base(u) + r, SUB), :] = r2[:, :, pl.ds(base(u) + r, SUB), :] + (a + b)

        sweep(u, body)
        q_copy[u].start()

    def z_step(u):
        with jax.named_scope(f"wait_q#u={u}"):
            q_copy[u].wait_recv()

        def body(r):
            near = pl.ds(base(u) + r, SUB)
            r3[:, near, :] = r3[:, near, :] + r2[:, q_me(u), near, :]

        sweep(u, body)
        for cp in z_copy[u]:
            cp.start()

    def third_parts(u):
        i, h = u - n_pair, height(u)
        rows = rows_of(u)
        short = pl.ds(0, h)
        landing = [rx.at[0:2, :, :, rows, :], rx.at[2:4, :, :, rows, :], rx3.at[i, :, :, :, short, :]]
        first = [remote(ps3.at[i, (z + k) % 4, :, :, :, short, :], landing[k - 1], z_send.at[u], z_recv.at[u], z_peer[k]) for k in HOPS]
        core = remote(t23.at[i, :, :, short, :], r2.at[0:2, :, rows, :], c_send.at[u], c_recv.at[u], core_peer)
        along_x = remote(r2.at[0:2, 1 - x, rows, :], r3.at[0:2, rows, :], q_send.at[u], q_recv.at[u], x_peer)
        along_y = remote(r3.at[1 - y, rows, :], rz.at[0, rows, :], p_send.at[u], p_recv.at[u], y_peer)
        return first, core, along_x, along_y

    third_copy = {u: third_parts(u) for u in third}

    def third_stage(u):
        t, first, h, colour = UNITS[u]
        valid = valid_of(u)
        lanes = pl.ds(first * LANES, valid * LANES)
        copies = [pltpu.make_async_copy(grads[t].at[:, :, :, cc, :, lanes], stage.at[cc, :, :, :, :, pl.ds(0, valid * LANES)], stage_sem.at[cc]) for cc in BOTH]
        for cp in copies:
            cp.start()
        for cp in copies:
            cp.wait()

        def body(j, carry):
            for xx in BOTH:
                for cc in BOTH:
                    dense = stage[cc, j // 2, j % 2, xx, :, pl.ds(0, valid * LANES)].reshape(valid, LANES)
                    if valid < h:
                        dense = jnp.concatenate([dense, jnp.zeros((h - valid, LANES), BF16)], axis=0)
                    ps3[u - n_pair, j // 2, j % 2, xx, cc, pl.ds(0, h), :] = dense
            return carry

        lax.fori_loop(0, 8, body, 0)
        for cp in third_copy[u][0]:
            cp.start()

    def third_sum(u, r, cc):
        i = u - n_pair
        near = pl.ds(base(u) + r, SUB)
        own = ps3[i, z, :, :, cc, pl.ds(r, SUB), :].astype(F32) + rx[0:2, :, cc, near, :].astype(F32)
        return own + (rx[2:4, :, cc, near, :].astype(F32) + rx3[i, :, :, cc, pl.ds(r, SUB), :].astype(F32))

    def third_core_step(u):
        with jax.named_scope(f"wait_third_z#u={u}"):
            wait_all(z_bytes(u), z_recv.at[u])

        def body(r):
            t23[u - n_pair, :, :, pl.ds(r, SUB), :] = third_sum(u, r, 1 - c)

        sweep(u, body)
        third_copy[u][1].start()

    def third_x_step(u):
        third_copy[u][1].wait_recv()

        def body(r):
            near = pl.ds(base(u) + r, SUB)
            r2[0:2, :, near, :] = r2[0:2, :, near, :] + third_sum(u, r, c)

        sweep(u, body)
        third_copy[u][2].start()

    def third_y_step(u):
        with jax.named_scope(f"wait_third_x#u={u}"):
            third_copy[u][2].wait_recv()

        def body(r):
            near = pl.ds(base(u) + r, SUB)
            r3[0:2, near, :] = r3[0:2, near, :] + r2[0:2, x, near, :]

        sweep(u, body)
        third_copy[u][3].start()

    def flat_rows(u, r, n):
        start = (UNITS[u][1] + r) * LANES
        return pl.ds(start if isinstance(r, int) else pl.multiple_of(start, LANES), n * LANES)

    def lamb_step(u):
        t, first, h, colour = UNITS[u]
        with jax.named_scope(f"wait_z#u={u}"):
            if colour == 2:
                third_copy[u][3].wait_recv()
            else:
                wait_all(z_bytes(u), z_recv.at[u])
        if first == 0:
            for i in (t, 4 + t, 8 + t):
                state_copy[i].wait()
        valid = valid_of(u)
        q = q_me(u)

        def tile(r, n):
            rows = pl.ds(base(u) + r, n)
            flat = flat_rows(u, r, n)
            w = weights[t][:, flat].reshape(n, LANES)
            m = first_mom[t][:, flat].reshape(n, LANES)
            v = second_mom[t][:, flat].reshape(n, LANES)
            if colour == 2:
                g = (r3[y, rows, :] + rz[0, rows, :]) / 32.0
            else:
                g = (((r3[z, rows, :] + rz[0, rows, :]) + rz[1, rows, :]) + rz[2, rows, :]) / 32.0
            nm = BETA_ONE * m + (1.0 - BETA_ONE) * g
            nv = BETA_TWO * v + (1.0 - BETA_TWO) * g * g
            u_dir = (nm / (1.0 - BETA_ONE ** STEP)) / (jnp.sqrt(nv / (1.0 - BETA_TWO ** STEP)) + EPSILON) + WEIGHT_DECAY * w
            r2[0, q, rows, :] = nm
            r2[1, q, rows, :] = nv
            rz[0, rows, :] = u_dir
            return w * w, u_dir * u_dir

        def body(i, carry):
            ww, uu = tile(pl.multiple_of(i * TILE, SUB), TILE)
            return (carry[0] + jnp.sum(ww.reshape(TILE // 8, 8, LANES), axis=0), carry[1] + jnp.sum(uu.reshape(TILE // 8, 8, LANES), axis=0))

        zero = jnp.zeros((8, LANES), F32)
        acc_w, acc_u = lax.fori_loop(0, valid // TILE, body, (zero, zero))
        sum_w = jnp.sum(acc_w, axis=0, keepdims=True)
        sum_u = jnp.sum(acc_u, axis=0, keepdims=True)
        if valid % TILE:
            ww, uu = tile(valid - valid % TILE, valid % TILE)
            sum_w = sum_w + jnp.sum(ww, axis=0, keepdims=True)
            sum_u = sum_u + jnp.sum(uu, axis=0, keepdims=True)
        ns[pl.ds(2 * t, 1), :] = ns[pl.ds(2 * t, 1), :] + sum_w
        ns[pl.ds(2 * t + 1, 1), :] = ns[pl.ds(2 * t + 1, 1), :] + sum_u
        out_m[u].start()
        out_v[u].start()

    def pair(s):
        return (2 * s, 2 * s + 1)

    for s in BOTH:
        for u in pair(s):
            stage_copy(u, False).start()
        if s == 0:
            for cp in state_copy:
                cp.start()
            ns[...] = jnp.zeros_like(ns)
        for u in pair(s):
            stage_copy(u, False).wait()
            pack_send(u)
        if s == 0:
            pl.semaphore_wait(barrier, 10)
        for u in pair(s):
            p_copy[u].start()
        third_stage(third[s])
    for u in pair(0):
        stage_copy(u, True).start()
    for u in pair(0):
        stage_copy(u, True).wait()
        pack_own(u)
        stage_copy(u + 4, False).start()

    for s in range(n_steps + LAG):
        if s < n_steps:
            for u in pair(s):
                core_step(u)
            for u in pair(s):
                q_step(u)
            for at, step in ((THIRD_CORE, third_core_step), (THIRD_X, third_x_step), (THIRD_Y, third_y_step)):
                for i, u in enumerate(third):
                    if at[i] == s:
                        step(u)
            if s + 2 < n_steps:
                for u in pair(s + 2):
                    stage_copy(u, False).wait()
                    p_copy[u - 4].wait_send()
                    pack_send(u)
                    p_copy[u].start()
            if s + 1 < n_steps:
                for u in pair(s + 1):
                    stage_copy(u, True).start()
                for u in pair(s + 1):
                    stage_copy(u, True).wait()
                    pack_own(u)
                    if s + 3 < n_steps:
                        stage_copy(u + 4, False).start()
        if 0 <= s - 1 < n_steps:
            for u in pair(s - 1):
                z_step(u)
        if s >= n_steps:
            for i, u in enumerate(third):
                if THIRD_Y[i] == s:
                    third_y_step(u)
        if 0 <= s - LAG < n_steps:
            for u in pair(s - LAG):
                lamb_step(u)
    for u in third:
        lamb_step(u)

    with jax.named_scope("norms"):
        plane_norm = [remote(ns, nr.at[plane_slot[0]], n_send.at[k], n_recv.at[plane_slot[0]], plane_peer[k - 1]) for k in range(1, 8)]
        for cp in plane_norm:
            cp.start()
        nr[plane_slot[0]] = ns[...]
        for k in range(1, 8):
            remote(ns, nr.at[plane_slot[k]], n_send.at[k], n_recv.at[plane_slot[k]], plane_peer[k - 1]).wait_recv()
        for cp in plane_norm:
            cp.wait_send()
        ns[...] = jnp.sum(nr[0:8], axis=0)
        z_norm = [remote(ns, nr.at[8 + z], n_send.at[7 + k], n_recv.at[8 + z], z_peer[k]) for k in HOPS]
        for cp in z_norm:
            cp.start()
        nr[8 + z] = ns[...]
        for k in HOPS:
            zz = (z + k) % 4
            remote(ns, nr.at[8 + zz], n_send.at[7 + k], n_recv.at[8 + zz], z_peer[k]).wait_recv()
        for cp in z_norm:
            cp.wait_send()
    total = jnp.sum(nr[8:12], axis=0)
    norms = jnp.sqrt(jnp.sum(total, axis=1, keepdims=True))

    def gathered_q(u):
        if colour_of(u) == 2:
            return full.at[z, y, x, c, rows_of(u), :]
        return full.at[:, y, x, c, rows_of(u), :]

    def gathered_p(u):
        if colour_of(u) == 0:
            return full.at[:, :, x, c, rows_of(u), :]
        if colour_of(u) == 2:
            return full.at[z, :, x, c, rows_of(u), :]
        return full.at[:, y, :, c, rows_of(u), :]

    def gathered_c(u):
        return full.at[:, :, :, c, rows_of(u), :]

    def gather_z(u, k):
        src = rx.at[0, 0, 0, rows_of(u), :]
        dst = full.at[z, y, x, c, rows_of(u), :]
        if colour_of(u) == 2:
            src = dst = full.at[z, :, :, c, rows_of(u), :]
        return remote(src, dst, z_send.at[u], z_recv.at[u], z_peer[k])

    gz = [[gather_z(u, k) for k in HOPS] for u in units]
    gq = [remote(gathered_q(u), gathered_q(u), q_send.at[u], q_recv.at[u], y_peer if colour_of(u) == 2 else q_peer(u)) for u in units]
    gp = [remote(gathered_p(u), gathered_p(u), p_send.at[u], p_recv.at[u], x_peer if colour_of(u) == 2 else p_peer(u)) for u in units]
    gc = [remote(gathered_c(u), gathered_c(u), c_send.at[u], c_recv.at[u], core_peer) for u in units]

    def drain_reduce(u):
        if colour_of(u) == 2:
            for cp in third_copy[u][1:]:
                cp.wait_send()
        else:
            if u >= n_pair - 4:
                p_copy[u].wait_send()
            if u >= n_pair - 2:
                c_copy[u].wait_send()
            q_copy[u].wait_send()
        wait_all(z_bytes(u), z_send.at[u])
        out_m[u].wait()
        out_v[u].wait()

    def weight_step(u):
        drain_reduce(u)
        t = tensor(u)
        valid = valid_of(u)
        scale = LEARN_RATE * (norms[2 * t:2 * t + 1] / norms[2 * t + 1:2 * t + 2])

        def tile(r, n):
            rows = pl.ds(base(u) + r, n)
            w = weights[t][:, flat_rows(u, r, n)].reshape(n, LANES)
            nw = w - scale * rz[0, rows, :]
            rz[1, rows, :] = nw
            rx[0, 0, 0, rows, :] = nw.astype(BF16)

        def body(i, carry):
            tile(pl.multiple_of(i * TILE, SUB), TILE)
            return carry

        lax.fori_loop(0, valid // TILE, body, 0)
        if valid % TILE:
            tile(valid - valid % TILE, valid % TILE)
        own_copy[u].start()
        out_w[u].start()
        if colour_of(u) == 2:
            own_copy[u].wait()
            gq[u].start()
        else:
            for cp in gz[u]:
                cp.start()

    def third_gather_z(u):
        with jax.named_scope(f"wait_third_gx#u={u}"):
            gp[u].wait_recv()
        for cp in gz[u]:
            cp.start()

    def third_gather_core(u):
        with jax.named_scope(f"wait_third_gz#u={u}"):
            wait_all(gather_z_bytes(u), z_recv.at[u])
        gc[u].start()

    def drain_gather(u):
        wait_all(gather_z_bytes(u), z_send.at[u])
        gq[u].wait_send()
        gp[u].wait_send()
        gc[u].wait_send()
        out_w[u].wait()

    order = list(range(n_steps))[::-1]
    for u in pair(order[0]):
        weight_step(u)
    for u in third:
        weight_step(u)
    for u in pair(order[1]):
        weight_step(u)
    for i in range(n_steps + 3):
        if i < n_steps:
            for u in pair(order[i]):
                own_copy[u].wait()
                with jax.named_scope(f"wait_gz#u={u}"):
                    wait_all(gather_z_bytes(u), z_recv.at[u])
                gq[u].start()
        if i == 0:
            for u in third:
                gq[u].wait_recv()
                gp[u].start()
        if i + 2 < n_steps:
            for u in pair(order[i + 2]):
                weight_step(u)
        for j, u in enumerate(third):
            if GATHER_Z[j] == i:
                third_gather_z(u)
        if 0 <= i - 1 < n_steps:
            for u in pair(order[i - 1]):
                with jax.named_scope(f"wait_gq#u={u}"):
                    gq[u].wait_recv()
                gp[u].start()
        for j, u in enumerate(third):
            if GATHER_CORE[j] == i:
                third_gather_core(u)
        if 0 <= i - 2 < n_steps:
            for u in pair(order[i - 2]):
                with jax.named_scope(f"wait_gp#u={u}"):
                    gp[u].wait_recv()
                gc[u].start()
        if 0 <= i - 3 < n_steps:
            for u in pair(order[i - 3]):
                with jax.named_scope(f"wait_gc#u={u}"):
                    gc[u].wait_recv()
        if 0 <= i - LAG < n_steps:
            for u in pair(order[i - LAG]):
                drain_gather(u)
    for u in third:
        gc[u].wait_recv()
        drain_gather(u)
    for u in pair(order[-1]):
        drain_gather(u)


def comm(grads, state):
    n_units = len(UNITS)
    any_spec = pl.BlockSpec(memory_space=pl.ANY)
    dma = pltpu.SemaphoreType.DMA
    return pl.pallas_call(
        comm_kernel,
        in_specs=[any_spec] * 16,
        out_specs=[any_spec] * 4,
        out_shape=[jax.ShapeDtypeStruct((4, 2, 2, 2, TOTAL, LANES), BF16)] + [jax.ShapeDtypeStruct((TOTAL, LANES), F32)] * 3,
        scratch_shapes=[pltpu.VMEM((1, r * LANES), F32) for r in ROWS] * 3
        + [
            pltpu.VMEM((4, 2, 2, TOTAL, LANES), BF16),
            pltpu.VMEM((4, 2, TOTAL, LANES), F32),
            pltpu.VMEM((4, TOTAL, LANES), F32),
            pltpu.VMEM((3, TOTAL, LANES), F32),
            pltpu.VMEM((2, 4, 2, MAX_ROWS, LANES), F32),
            pltpu.VMEM((2, 4, 2, 2, MAX_ROWS, LANES), BF16),
            pltpu.VMEM((2, 2, 4, 2, 2, MAX_ROWS, LANES), BF16),
            pltpu.VMEM((2, 4, 2, 2, 1, MAX_ROWS * LANES), BF16),
            pltpu.VMEM((2, 2, 2, 2, MAX_ROWS, LANES), BF16),
            pltpu.VMEM((2, 2, 2, MAX_ROWS, LANES), F32),
            pltpu.VMEM((2, 4, 2, 2, 2, MAX_ROWS, LANES), BF16),
            pltpu.VMEM((8, LANES), F32),
            pltpu.VMEM((12, 8, LANES), F32),
            dma((12,)), dma((2,)),
            dma((n_units,)), dma((n_units,)), dma((n_units,)), dma((n_units,)), dma((n_units,)), dma((n_units,)),
            dma((n_units,)), dma((n_units,)), dma((11,)), dma((12,)), dma((2, n_units)),
        ],
        compiler_params=pltpu.CompilerParams(collective_id=0, has_side_effects=True, vmem_limit_bytes=64 * 1024 * 1024 - 128 * 1024),
        name="lamb_comm",
    )(*grads, *state)


def solution(mesh):
    grad_spec = P("data", None, None)
    shard_spec = P(None, "data")
    full_spec = P(None, None)

    def device_step(*blocks):
        grads = [blocks[4 * t].reshape(4, 2, 2, 2, 1, -1) for t in range(4)]
        state = [blocks[4 * t + s] for s in (1, 2, 3) for t in range(4)]
        full, w, m, v = comm(grads, state)
        outs = unpack(full.reshape(32, TOTAL, LANES), w, m, v)
        results = []
        for t in range(4):
            results.extend((outs[t], outs[4 + t], outs[8 + t], outs[12 + t]))
        return tuple(results)

    return jax.shard_map(device_step, mesh=mesh, in_specs=(grad_spec, shard_spec, shard_spec, shard_spec) * 4, out_specs=(full_spec, shard_spec, shard_spec, shard_spec) * 4, check_vma=False)
```
